32 devices in a mesh: fsdp: 4 (over y, core), heads: 2 (over x), tensor: 4 (over z).
Axes of the slice: x: 2, y: 2, z: 4, core: 2. Of those that a mesh axis runs over, the one named last changes fastest.
Arguments:
- tokens: bfloat16 [64, 197, 512], P(('fsdp', 'tensor')), may hold values from -6 to 6
- cotangent: bfloat16 [64, 197, 512], P(('fsdp', 'tensor')), may hold values from -6 to 6
- w_qkv: bfloat16 [3, 512, 512], P(None, ('fsdp', 'tensor'), 'heads'), may hold values from -0.25 to 0.25
- w_out: bfloat16 [512, 512], P('heads', ('fsdp', 'tensor')), may hold values from -0.75 to 0.75
- w_router: bfloat16 [512, 32], P(('fsdp', 'tensor')), may hold values from -0.25 to 0.25
- norm_one: bfloat16 [512], P(('fsdp', 'tensor')), may hold values from 0.099609375 to 1.8984375
- norm_two: bfloat16 [512], P(('fsdp', 'tensor')), may hold values from 0.099609375 to 1.8984375
- w_in: bfloat16 [32, 512, 2048], P('heads', 'fsdp', 'tensor'), may hold values from -0.25 to 0.25
- w_back: bfloat16 [32, 2048, 512], P('heads', 'tensor', 'fsdp'), may hold values from -4 to 4
- routes: int32 [64, 197, 2], P(('fsdp', 'tensor')), may hold values from 0 to 31, all different within a row; in each aligned block of 788 rows (0 to 787, 788 to 1575, ..., all dimensions but the last counted through in order) at most 64 rows name the same one
Outputs:
- output: bfloat16 [64, 197, 512], P(('fsdp', 'tensor'))
- token_grad: float32 [64, 197, 512], P(('fsdp', 'tensor'))
- qkv_grad: float32 [3, 512, 512], P(None, ('fsdp', 'tensor'), 'heads')
- out_grad: float32 [512, 512], P('heads', ('fsdp', 'tensor'))
- router_grad: float32 [512, 32], P(('fsdp', 'tensor'))
- norm_one_grad: float32 [512], P(('fsdp', 'tensor'))
- norm_two_grad: float32 [512], P(('fsdp', 'tensor'))
- in_grad: float32 [32, 512, 2048], P('heads', 'fsdp', 'tensor')
- back_grad: float32 [32, 2048, 512], P('heads', 'tensor', 'fsdp')
The draws below stay inside these ranges and needn't reach their ends.
Inputs may be any that keep to these rules, and one draw needn't show every extreme that they name: Each token names two different experts. Within the 788 tokens of one group (aligned blocks of rows), no expert is named by more than 64 routes, a bound that some block reaches.
All inputs are finite; a program needn't handle non-finite values.
Results may differ from the reference program's by a relative error of at most 0.02.
Values may be sent and summed in bfloat16 or wider, within the bound.
A program may use at most 192 MiB of HBM per device.

```python
import math
import jax
import jax.numpy as jnp
import numpy as np
from jax import lax

D = 512
HEADS = 8
HD = 64
FF = 2048
EXPERTS = 32
SEQ = 197
IMG_DEV = 4
TOK_DEV = 788
CAP = 64
IMAGES = 64
N_FSDP = 4
N_TENSOR = 4


def levels(stream_key, shape, pieces, smallest, high):
    loudness = 1.0
    for axis_at, shards_of in pieces:
        steps = jax.random.uniform(jax.random.fold_in(jax.random.fold_in(stream_key, 6), axis_at), (shards_of,), jnp.float32, smallest / len(pieces), high / len(pieces))
        loudness = loudness * jnp.repeat(jnp.exp(steps), shape[axis_at] // shards_of).reshape((-1,) + (1,) * (len(shape) - 1 - axis_at))
    return loudness


def shared_out(own_key, own, number, rows, amount, top, bound, skew):
    order = jax.random.permutation(own_key, amount)
    heavy_load, usual = portions_of(amount, rows * top, bound, skew, True), portions_of(amount, rows * top, bound, skew, False)
    places = jnp.arange(amount)

    def named(lengths, offset_by):
        used = int((lengths > 0).sum())
        fixed = max(1, used // 4)
        passed = fixed + (places - fixed + offset_by * (used - fixed)) % max(1, amount - fixed)
        return jnp.zeros((amount,), jnp.int32).at[order[jnp.where(places < fixed, places, passed)]].set(jnp.asarray(lengths, jnp.int32))

    lengths = jnp.where(number % 4 == 0, named(heavy_load, number // 4), named(usual, number - number // 4 - 1))
    mixed = jax.random.permutation(jax.random.fold_in(own, 3), amount)
    source_of, taker = mixed[0:amount // 2 * 2:2], mixed[1:amount // 2 * 2:2]
    margin = jnp.minimum(lengths[source_of] - 1, bound - lengths[taker]) // 2
    margin = jnp.where((source_of == order[0]) | (taker == order[0]) | (lengths[taker] == 0), 0, jnp.maximum(margin, 0))
    passed = jax.random.randint(jax.random.fold_in(own, 4), (amount // 2,), 0, 1 << 20) % (margin + 1)
    lengths = lengths.at[source_of].add(-passed).at[taker].add(passed)
    members = jnp.searchsorted(jnp.cumsum(lengths), jnp.arange(rows * top), side="right").astype(jnp.int32)
    listing = members.reshape(top, rows).T
    listing = listing[jax.random.permutation(jax.random.fold_in(own, 1), rows)]
    offset_by = jax.random.randint(jax.random.fold_in(own, 2), (rows, 1), 0, top)
    return jnp.take_along_axis(listing, (jnp.arange(top)[None, :] + offset_by) % top, axis=1)


def portions_of(count, total, bound, lean, full):
    portions = [(1 << 20) // math.isqrt(rank ** lean) + 1 for rank in range(1, count + 1)]
    largest = bound if full else min(bound, max(-(-total // count), total * portions[0] // sum(portions)))
    least = 1 if total - largest >= count - 1 else 0
    given, spare = [largest] + [least] * (count - 1), total - largest - least * (count - 1)
    while spare > 0:
        movable = [i for i in range(1, count) if given[i] < largest] or [i for i in range(1, count) if given[i] < bound]
        whole, remaining = sum([portions[i] for i in movable]), spare
        for i in movable:
            addition = min(bound - given[i], max(1, remaining * portions[i] // whole), spare)
            given[i] = given[i] + addition
            spare = spare - addition
    return np.array(given)


def noise(stream_key, shape, width, limit, split=(), kind=jnp.bfloat16):
    drawn = jax.random.normal(stream_key, shape, jnp.float32) * width
    if len(split) > 0:
        drawn = levels(stream_key, shape, split, -0.22, 0.18) * drawn
    return jnp.clip(drawn, min=-limit, max=limit).astype(kind)


def setup_inputs(seed: int = 0) -> dict:
    seeds = jax.random.split(jax.random.key(seed), 11)
    tokens = noise(seeds[0], (IMAGES, SEQ, D), 1.0, 6.0, ((0, 16),))
    cotangent = noise(seeds[1], (IMAGES, SEQ, D), 1.0, 6.0, ((0, 16),))
    w_qkv = noise(seeds[2], (3, D, D), D ** -0.5, 0.25, ((1, 16), (2, 2)))
    w_out = noise(seeds[3], (D, D), (D // 8) ** -0.5, 0.75, ((0, 2), (1, 16)))
    w_router = noise(seeds[4], (D, EXPERTS), D ** -0.5, 0.25, ((0, 16),))
    norm_one = jnp.clip(1.0 + 0.18 * jax.random.normal(seeds[5], (D,), jnp.float32), 0.099609375, 1.8984375).astype(jnp.bfloat16)
    norm_two = jnp.clip(1.0 + 0.18 * jax.random.normal(seeds[6], (D,), jnp.float32), 0.099609375, 1.8984375).astype(jnp.bfloat16)
    w_in = noise(seeds[7], (EXPERTS, D, FF), D ** -0.5, 0.25, ((0, 2), (1, 4), (2, 4)))
    w_back = noise(seeds[8], (EXPERTS, FF, D), (max(FF // 1024, 1)) ** -0.5, 4.0, ((0, 2), (1, 4), (2, 4)))
    routes_keys = jax.random.split(jax.random.fold_in(seeds[9], 1), IMAGES * SEQ // TOK_DEV)
    routes_turns = jax.random.permutation(jax.random.fold_in(seeds[9], 3), IMAGES * SEQ // TOK_DEV)
    routes = jax.vmap(lambda own, number: shared_out(jax.random.fold_in(seeds[9], 2), own, number, TOK_DEV, EXPERTS, 2, CAP, 1))(routes_keys, routes_turns).reshape((IMAGES, SEQ, 2))
    return dict(tokens=tokens, cotangent=cotangent, w_qkv=w_qkv, w_out=w_out, w_router=w_router, norm_one=norm_one, norm_two=norm_two, w_in=w_in, w_back=w_back, routes=routes)


@jax.custom_vjp
def low(v):
    return lax.optimization_barrier(v.astype(jnp.bfloat16)).astype(jnp.float32)

@jax.custom_vjp
def low_back(v):
    return v

def low_keep(v):
    return (low(v), None)

def low_pass(kept, grad):
    return (grad,)

def back_keep(v):
    return (v, None)

def back_low(kept, grad):
    return (low(grad),)
low.defvjp(low_keep, low_pass)
low_back.defvjp(back_keep, back_low)
highest_precision = lax.Precision.HIGHEST

def layer_norm(values, gain):
    centre = values - lax.optimization_barrier(jnp.mean(values, axis=-1, keepdims=True))
    spread = lax.rsqrt(lax.optimization_barrier(jnp.mean(centre * centre, axis=-1, keepdims=True)) + 1e-06)
    return centre * spread * gain

def slot_ids(route_rows):
    picked_flat = route_rows.reshape(-1)
    one_hot = (picked_flat[:, None] == jnp.arange(EXPERTS, dtype=jnp.int32)[None, :]).astype(jnp.int32)
    earlier = jnp.cumsum(one_hot, axis=0) - one_hot
    position = lax.optimization_barrier(jnp.sum(earlier * one_hot, axis=1))
    return (picked_flat * CAP + position).astype(jnp.int32).reshape(route_rows.shape)

def group_forward(params, image_block, route_rows):
    w_qkv, w_out, w_router, norm_one, norm_two, w_in, w_back = params
    first_in = low(layer_norm(image_block, norm_one))
    projected = low_back(low(jnp.einsum('bsd,jde->jbse', first_in, w_qkv, precision=highest_precision)))
    heads_view = projected.reshape(3, IMG_DEV, SEQ, HEADS, HD)
    query_rows, key_rows, value_rows = (heads_view[0], heads_view[1], heads_view[2])
    scores = low_back(jnp.einsum('bshd,bthd->bhst', query_rows, key_rows, precision=highest_precision) * HD ** (-0.5))
    weights = jax.nn.softmax(scores, axis=-1)
    mixed_rows = low_back(low(jnp.einsum('bhst,bthd->bshd', low(weights), value_rows, precision=highest_precision)))
    mixed_rows = mixed_rows.reshape(IMG_DEV, SEQ, D)
    attention = low_back(jnp.einsum('bse,ed->bsd', mixed_rows, w_out, precision=highest_precision))
    residual = image_block + attention
    second_in = low(layer_norm(residual, norm_two)).reshape(TOK_DEV, D)
    logits = low_back(jnp.dot(second_in, w_router, precision=highest_precision))
    router_probs = jax.nn.softmax(logits, axis=-1)
    gate_values = jnp.take_along_axis(router_probs, route_rows, axis=1)
    slot_index = slot_ids(route_rows)
    buffer_rows = jnp.zeros((EXPERTS * CAP, D), jnp.float32).at[slot_index.reshape(-1)].add(jnp.repeat(second_in, route_rows.shape[1], axis=0))
    inner_act = low_back(jnp.einsum('ecd,edf->ecf', buffer_rows.reshape(EXPERTS, CAP, D), w_in, precision=highest_precision))
    hidden = low(jax.nn.gelu(inner_act, approximate=False))
    expert_out = low_back(low(jnp.einsum('ecf,efd->ecd', hidden, w_back, precision=highest_precision))).reshape(EXPERTS * CAP, D)
    returned = expert_out[slot_index]
    moe_sum = lax.optimization_barrier(jnp.sum(gate_values[:, :, None] * returned, axis=1))
    return residual + moe_sum.reshape(IMG_DEV, SEQ, D)

def reference(tokens, cotangent, w_qkv, w_out, w_router, norm_one, norm_two, w_in, w_back, routes):
    groups = N_FSDP * N_TENSOR
    blocks = tokens.astype(jnp.float32).reshape(groups, IMG_DEV, SEQ, D)
    route_groups = routes.reshape(groups, TOK_DEV, routes.shape[2])
    params = (w_qkv.astype(jnp.float32), w_out.astype(jnp.float32), w_router.astype(jnp.float32), norm_one.astype(jnp.float32), norm_two.astype(jnp.float32), w_in.astype(jnp.float32), w_back.astype(jnp.float32))

    def whole(weight_set, inputs):

        def one_group(pair):
            return group_forward(weight_set, pair[0], pair[1])
        return lax.map(jax.checkpoint(one_group), (inputs, route_groups))
    output, pullback = jax.vjp(whole, params, blocks)
    weight_grads, input_grads = pullback(cotangent.astype(jnp.float32).reshape(output.shape))
    return (output.reshape(IMAGES, SEQ, D).astype(jnp.bfloat16), input_grads.reshape(IMAGES, SEQ, D), weight_grads[0], weight_grads[1], weight_grads[2], weight_grads[3], weight_grads[4], weight_grads[5], weight_grads[6])
```

```python
import functools

import jax
import jax.numpy as jnp
from jax import lax
from jax.experimental import pallas as pl
from jax.experimental.pallas import tpu as pltpu
from jax.sharding import PartitionSpec as P

HD = 64
EXPERTS = 32
CAP = 64
PAIR = 2
LANES = 128
MESH = pl.DeviceIdType.MESH
F32 = jnp.float32
BF16 = jnp.bfloat16


def mm(a, b):
    return lax.dot_general(a, b, (((1,), (0,)), ((), ())), preferred_element_type=F32)


def mm_nt(a, b):
    return lax.dot_general(a, b, (((1,), (1,)), ((), ())), preferred_element_type=F32)


def mm_tn(a, b):
    return lax.dot_general(a, b, (((0,), (0,)), ((), ())), preferred_element_type=F32)


def iota(shape, dim):
    return lax.broadcasted_iota(jnp.int32, shape, dim).astype(F32)


def norm_of(x):
    centre = x - jnp.mean(x, axis=-1, keepdims=True)
    spread = lax.rsqrt(jnp.mean(centre * centre, axis=-1, keepdims=True) + 1e-06)
    return centre * spread, spread


def norm_back(scaled, normed, spread):
    middle = jnp.mean(scaled, axis=-1, keepdims=True)
    along = jnp.mean(scaled * normed, axis=-1, keepdims=True)
    return spread * (scaled - middle - normed * along)


class Sizes:
    def __init__(self, mesh_shape, images, length, width, home, ff_shard):
        self.tensor = mesh_shape["tensor"]
        self.heads = mesh_shape["heads"]
        self.pair = PAIR if self.tensor % PAIR == 0 else 1
        self.halves = self.tensor // self.pair
        self.team_i = min(mesh_shape["fsdp"], max(1, home // self.tensor))
        self.reps = mesh_shape["fsdp"] // self.team_i
        self.team = self.team_i * self.tensor
        self.home = home
        self.own_e = home // (self.team_i * self.pair)
        self.images = images
        self.length = length
        self.width = width
        self.pad = -(-length // 16) * 16
        self.own_img = images // self.heads
        self.own = self.own_img * self.pad
        self.all = images * self.pad
        self.rows = -(-self.all // LANES) * LANES
        self.ffs = ff_shard
        self.ff = ff_shard * self.pair
        self.slots = home * CAP
        self.dq = width // self.team_i
        self.wrow = self.dq // self.tensor
        self.ecols = width // self.heads
        self.lw = self.own_e * CAP
        self.nh = width // HD


def kernel(z, names, *refs):
    ref = dict(zip(names, refs))
    tok, cot, rt, wpack, spack = ref["tok"], ref["cot"], ref["rt"], ref["wpack"], ref["spack"]
    win, wback = ref["win"], ref["wback"]
    T, I, R = z.tensor, z.team_i, z.reps
    D, L, RP = z.width, z.length, z.pad
    OWN, ALL, ROWS = z.own, z.all, z.rows
    PR, A, ED = z.pair, z.halves, z.own_e
    FS, DQ, WR, EC = z.ffs, z.dq, z.wrow, z.ecols

    fs, h, t = lax.axis_index("fsdp"), lax.axis_index("heads"), lax.axis_index("tensor")
    i, r = fs // R, lax.rem(fs, R)
    oh = 1 - h
    pos, half = lax.rem(t, PR), t // PR
    e0 = (i * PR + pos) * ED
    i_core = i + 1 - 2 * lax.rem(i, 2)
    i_far = lax.rem(i + 2, I)
    i_diag = lax.rem(i_core + 2, I)
    mine = i * T + t

    def dev(ii, tt, hh=None):
        return {"fsdp": ii * R + r, "heads": h if hh is None else hh, "tensor": tt}

    def rcopy(src, dst, ssem, rsem, target):
        return pltpu.make_async_remote_copy(
            src_ref=src, dst_ref=dst, send_sem=ssem, recv_sem=rsem, device_id=target, device_id_type=MESH
        )

    def lcopy(src, dst, sem):
        return pltpu.make_async_copy(src, dst, sem)

    def al(v, m):
        return pl.multiple_of(v, m)

    bar = pltpu.get_barrier_semaphore()
    for di in range(I):
        for dt in range(T):
            if di or dt:
                pl.semaphore_signal(
                    bar, inc=1, device_id=dev(lax.rem(i + di, I), lax.rem(t + dt, T)), device_id_type=MESH
                )
    pl.semaphore_signal(bar, inc=1, device_id=dev(i, t, oh), device_id_type=MESH)
    pl.semaphore_wait(bar, I * T)

    wall, sall = ref["wall"], ref["sall"]
    ws, wr, wl = ref["ws"], ref["wr"], ref["wl"]

    def shard_of(buf):
        return buf.at[:, pl.ds(al(mine * WR, WR), WR), pl.ds(al(h * EC, LANES), EC)]

    def block(buf, ii, hh):
        return buf.at[:, pl.ds(al(ii * DQ, DQ), DQ), pl.ds(al(hh * EC, LANES), EC)]

    def srows(ii):
        return sall.at[pl.ds(al(ii * DQ, DQ), DQ)]

    s_mine = sall.at[pl.ds(al(mine * WR, WR), WR)]
    first = []
    for dt in range(1, T):
        to = dev(i, lax.rem(t + dt, T))
        first.append(rcopy(wpack, shard_of(wall), ws.at[0, dt], wr.at[0, dt], to))
        first.append(rcopy(spack, s_mine, ws.at[1, dt], wr.at[1, dt], to))
    for c in first:
        c.start()
    own_w = [lcopy(wpack, shard_of(wall), wl.at[0]), lcopy(spack, s_mine, wl.at[1])]
    for c in own_w:
        c.start()

    xn2a, cota, rp = ref["xn2a"], ref["cota"], ref["rp"]
    xn2a[...] = jnp.zeros_like(xn2a)
    cota[...] = jnp.zeros_like(cota)
    rp[...] = jnp.full_like(rp, -1.0)
    xs = ref["xs"]
    xs[...] = jnp.zeros_like(xs)
    for m in range(z.images):
        cota[pl.ds(m * RP, L), :] = cot[m]
        rp[pl.ds(m * RP, L), 0:2] = rt[m].astype(F32)
    for m in range(z.own_img):
        xs[pl.ds(m * RP, L), :] = tok[h * z.own_img + m].astype(F32)

    lane_all = iota((ROWS, LANES), 1)
    r0, r1 = rp[:, 0:1], rp[:, 1:2]
    oh0 = jnp.where(r0 == lane_all, 1.0, 0.0)
    oh1 = jnp.where(r1 == lane_all, 1.0, 0.0)
    both = ref["both"]
    both[...] = (oh0 + oh1).astype(BF16)
    idc = ref["idc"]

    def count(c, _):
        at = pl.ds(al(c * LANES, LANES), LANES)
        before = iota((LANES, ROWS), 1) < iota((LANES, ROWS), 0) + (c * LANES).astype(F32)
        counted = mm(jnp.where(before, 1.0, 0.0).astype(BF16), both[...])
        lane = iota((LANES, LANES), 1)
        q0, q1 = rp[at, 0:1], rp[at, 1:2]
        number = counted + lane * CAP
        n0 = jnp.sum(jnp.where(q0 == lane, number, 0.0), axis=1, keepdims=True)
        n1 = jnp.sum(jnp.where(q1 == lane, number, 0.0), axis=1, keepdims=True)
        n0 = jnp.where(q0 < 0.0, -1.0, n0)
        n1 = jnp.where(q1 < 0.0, -1.0, n1)
        idc[at, :] = jnp.where(lane == 0.0, n0, jnp.where(lane == 1.0, n1, -1.0))
        return 0

    lax.fori_loop(0, ROWS // LANES, count, 0)
    idr = ref["idr"]
    idr[...] = jnp.transpose(idc[...])

    gs, xsl = ref["gs"], ref["xsl"]

    def dispatch(source, target):
        def one(c, _):
            slot = iota((LANES, ROWS), 0) + (c * LANES + h * z.slots).astype(F32)
            pick = jnp.where(idr[0:1, :] == slot, 1.0, 0.0) + jnp.where(idr[1:2, :] == slot, 1.0, 0.0)
            got = mm(pick.astype(BF16), source[...]).astype(BF16)
            per = LANES // CAP
            target[pl.ds(c * per, per)] = got.reshape(per, CAP, D)
            return 0

        lax.fori_loop(0, z.slots // LANES, one, 0)

    dispatch(cota, gs)

    for c in first:
        c.wait_recv()
    for c in own_w:
        c.wait()
    b_x = rcopy(block(wall, i, h), block(wall, i, h), ws.at[2, 0], wr.at[2, 0], dev(i, t, oh))
    b_y = rcopy(block(wall, i, h), block(wall, i, h), ws.at[2, 1], wr.at[2, 1], dev(i_far, t))
    b_ys = rcopy(srows(i), srows(i), ws.at[2, 2], wr.at[2, 2], dev(i_far, t))
    b_c = rcopy(block(wall, i, h), block(wall, i, h), ws.at[2, 3], wr.at[2, 3], dev(i_core, t))
    b_cs = rcopy(srows(i), srows(i), ws.at[3, 0], wr.at[3, 0], dev(i_core, t))
    for c in (b_y, b_x, b_ys, b_c, b_cs):
        c.start()
    b_y.wait_recv()
    f_x = rcopy(block(wall, i_far, h), block(wall, i_far, h), ws.at[3, 1], wr.at[3, 1], dev(i, t, oh))
    f_x.start()
    f_c = rcopy(block(wall, i_far, h), block(wall, i_far, h), ws.at[3, 2], wr.at[3, 2], dev(i_core, t))
    f_c.start()
    b_ys.wait_recv()
    f_cs = rcopy(srows(i_far), srows(i_far), ws.at[3, 3], wr.at[3, 3], dev(i_core, t))
    f_cs.start()
    b_x.wait_recv()
    f_c2 = rcopy(block(wall, i, oh), block(wall, i, oh), ws.at[4, 0], wr.at[4, 0], dev(i_core, t))
    f_c2.start()

    vin, vback = ref["vin"], ref["vback"]
    es, er = ref["es"], ref["er"]
    moved = []
    k = 0
    for dp in range(PR):
        for di in range(I):
            ii, pp = lax.rem(i + di, I), lax.rem(pos + dp, PR)
            them = pl.ds((ii * PR + pp) * ED, ED)
            to_in = vin.at[:, pl.ds(al(i * DQ, DQ), DQ), pl.ds(al(pos * FS, FS), FS)]
            to_back = vback.at[:, pl.ds(al(pos * FS, FS), FS), pl.ds(al(i * DQ, DQ), DQ)]
            if di == 0 and dp == 0:
                moved.append(lcopy(win.at[them], to_in, er.at[0, 0]))
                moved.append(lcopy(wback.at[them], to_back, er.at[1, 0]))
            else:
                to = dev(ii, half * PR + pp)
                moved.append(rcopy(win.at[them], to_in, es.at[0, k], er.at[0, k], to))
                moved.append(rcopy(wback.at[them], to_back, es.at[1, k], er.at[1, k], to))
            k += 1
    for c in moved:
        c.start()

    xr, gr, gater = ref["xr"], ref["gr"], ref["gater"]
    ds, dr = ref["ds"], ref["dr"]

    def spread(src, dst, row, whole):
        made = []
        for di in range(I):
            for dt in range(T):
                kk = di * T + dt
                ii, tt = lax.rem(i + di, I), lax.rem(t + dt, T)
                pp = lax.rem(tt, PR)
                if whole:
                    s, d = src.at[ii * PR + pp], dst.at[mine]
                else:
                    s, d = src.at[pl.ds((ii * PR + pp) * ED, ED)], dst.at[:, mine]
                if kk == 0:
                    made.append(lcopy(s, d, dr.at[row, 0]))
                else:
                    made.append(rcopy(s, d, ds.at[row, kk], dr.at[row, kk], dev(ii, tt)))
        for c in made:
            c.start()
        return made

    g_moved = spread(gs, gr, 0, False)

    f_x.wait_recv()
    f_c3 = rcopy(block(wall, i_far, oh), block(wall, i_far, oh), ws.at[4, 1], wr.at[4, 1], dev(i_core, t))
    f_c3.start()
    for c in (b_c, b_cs, f_c, f_cs, f_c2, f_c3):
        c.wait_recv()

    sall_t = jnp.transpose(sall[...].astype(F32))
    gains = ref["gains"]
    gains[...] = sall_t[EXPERTS : EXPERTS + 8, :]
    xn1, qkv, mixed, probs = ref["xn1"], ref["qkv"], ref["mixed"], ref["probs"]
    normed, _ = norm_of(xs[...])
    xn1[...] = (normed * gains[0:1, :]).astype(BF16)

    def project(j, _):
        qkv[j] = mm(xn1[...], wall[j]).astype(BF16)
        return 0

    lax.fori_loop(0, 3, project, 0)
    groups = D // LANES
    scale = HD ** (-0.5)

    def attend(n, _):
        rows = pl.ds(al((n // groups) * RP, 16), RP)
        cols = pl.ds(al(lax.rem(n, groups) * LANES, LANES), LANES)
        q, kk, v = qkv[0, rows, cols], qkv[1, rows, cols], qkv[2, rows, cols]
        low = iota((RP, LANES), 1) < HD
        key = iota((RP, RP), 1)
        outs = []
        for s in range(2):
            sel = low if s == 0 else jnp.logical_not(low)
            score = mm_nt(jnp.where(sel, q, jnp.zeros_like(q)), kk) * scale
            score = jnp.where(key < L, score, -1e30)
            e = jnp.exp(score - jnp.max(score, axis=-1, keepdims=True))
            p = e / jnp.sum(e, axis=-1, keepdims=True)
            p = p.astype(BF16)
            probs[n * 2 + s] = p
            outs.append(mm(p, v))
        mixed[rows, cols] = jnp.where(low, outs[0], outs[1]).astype(BF16)
        return 0

    lax.fori_loop(0, z.own_img * groups, attend, 0)
    resid = ref["resid"]
    resid[...] = xs[...] + mm_nt(mixed[...], wall[3])
    normed, _ = norm_of(resid[...])
    mine_rows = pl.ds(al(h * OWN, 16), OWN)
    other_rows = pl.ds(al(oh * OWN, 16), OWN)
    xn2a[mine_rows, :] = (normed * gains[1:2, :]).astype(BF16)

    xsm, xrm = ref["xsm"], ref["xrm"]
    x_swap = rcopy(xn2a.at[mine_rows], xn2a.at[mine_rows], xsm.at[0], xrm.at[0], dev(i, t, oh))
    x_swap.start()
    x_swap.wait_recv()
    logits = mm(xn2a[...], sall[...])
    logits = jnp.where(lane_all < EXPERTS, logits, -1e30)
    e = jnp.exp(logits - jnp.max(logits, axis=-1, keepdims=True))
    router = ref["router"]
    router[...] = e / jnp.sum(e, axis=-1, keepdims=True)
    gcol = ref["gcol"]
    g0 = jnp.sum(jnp.where(rp[:, 0:1] == lane_all, router[...], 0.0), axis=1, keepdims=True)
    g1 = jnp.sum(jnp.where(rp[:, 1:2] == lane_all, router[...], 0.0), axis=1, keepdims=True)
    gcol[...] = jnp.where(lane_all == 0.0, g0, g1)
    dispatch(xn2a, xsl)
    x_moved = spread(xsl, xr, 1, False)
    gsend = ref["gsend"]

    def gate_row(c, _):
        lane = lane_all + (c * z.lw + h * z.slots).astype(F32)
        keep = lane_all < z.lw
        w = jnp.where(jnp.logical_and(keep, idc[:, 0:1] == lane), gcol[:, 0:1], 0.0)
        w = w + jnp.where(jnp.logical_and(keep, idc[:, 1:2] == lane), gcol[:, 1:2], 0.0)
        gsend[c] = jnp.broadcast_to(jnp.sum(w, axis=0, keepdims=True), (8, LANES))
        return 0

    lax.fori_loop(0, z.home // ED, gate_row, 0)
    gate_moved = spread(gsend, gater, 2, True)

    hid, igs, gtile = ref["hid"], ref["igs"], ref["gtile"]
    eoa, sia = ref["eoa"], ref["sia"]
    eos, sis, ggs = ref["eos"], ref["sis"], ref["ggs"]
    eor, sir, ggr = ref["eor"], ref["sir"], ref["ggr"]
    rs, rr = ref["rs"], ref["rr"]
    gcols = ref["gcols"]
    ggs[...] = jnp.zeros_like(ggs)
    for c in moved:
        c.wait()
    TR = T * CAP
    eye = iota((LANES, LANES), 0) == iota((LANES, LANES), 1)

    def wait_role(row, kk, dst):
        pltpu.make_async_copy(dst, dst, dr.at[row, kk]).wait()

    def tile(n, _):
        gi = lax.rem(i - n + I, I)
        grp = pl.ds(gi * T, T)
        for dt in range(T):
            src = gi * T + lax.rem(t - dt + T, T)
            wait_role(0, n * T + dt, gr.at[:, src])
            wait_role(1, n * T + dt, xr.at[:, src])
            wait_role(2, n * T + dt, gater.at[src])
        for dt in range(T):
            row = gater[gi * T + dt][0:1, :]
            col = jnp.sum(jnp.where(eye, jnp.broadcast_to(row, (LANES, LANES)), 0.0), axis=1, keepdims=True)
            gcols[dt] = jnp.broadcast_to(col, (LANES, LANES))

        def part(ep, _):
            e, p = ep // PR, lax.rem(ep, PR)
            cols = pl.ds(al(p * FS, FS), FS)
            trow = pl.ds(al(gi * TR, TR), TR)
            x = xr[e, grp].reshape(TR, D)

            @pl.when(p == 0)
            def _():
                g = gr[e, grp].reshape(TR, D)
                gtile[...] = g
                gate = gcols[:, pl.ds(al(e * CAP, CAP), CAP), :].reshape(TR, LANES)[:, 0:1]
                gr[e, grp] = (g.astype(F32) * gate).astype(BF16).reshape(T, CAP, D)
                eoa[...] = jnp.zeros_like(eoa)
                sia[...] = jnp.zeros_like(sia)

            inner = mm(x, vin[e, :, cols])
            erf = lax.erf(inner * (0.5**0.5))
            cdf = 0.5 * (1.0 + erf)
            hidden = (inner * cdf).astype(BF16)
            slope = cdf + inner * (jnp.exp(-0.5 * inner * inner) * 0.3989422804014327)
            hid[e, trow, cols] = hidden
            eoa[...] += mm(hidden, vback[e, cols, :])
            back = mm_nt(gr[e, grp].reshape(TR, D), vback[e, cols, :])
            inner_grad = (back * slope).astype(BF16)
            igs[e, trow, cols] = inner_grad
            sia[...] += mm_nt(inner_grad, vin[e, :, cols])

            @pl.when(p == PR - 1)
            def _():
                eo = eoa[...]
                eos[e, grp] = eo.astype(BF16).reshape(T, CAP, D)
                sis[e, grp] = sia[...].astype(BF16).reshape(T, CAP, D)
                gg = jnp.sum(eo * gtile[...].astype(F32), axis=1, keepdims=True)
                there = iota((CAP, LANES), 1) == iota((CAP, LANES), 0) + (e * CAP).astype(F32)
                for dt in range(T):
                    piece = jnp.broadcast_to(gg[dt * CAP : (dt + 1) * CAP], (CAP, LANES))
                    line = jnp.sum(jnp.where(there, piece, 0.0), axis=0, keepdims=True)
                    ggs[gi * T + dt] = ggs[gi * T + dt] + jnp.broadcast_to(line, (8, LANES))

            return 0

        lax.fori_loop(0, ED * PR, part, 0)
        give_back(n, 0, sis, sir, False)
        give_back(n, 2, ggs, ggr, True)
        return 0

    def give_back(n, row, src, dst, whole):
        gi = lax.rem(i - n + I, I)
        for dt in range(T):
            tt = lax.rem(t + dt, T)
            kk = n * T + dt
            if whole:
                s, d = src.at[gi * T + tt], dst.at[mine]
            else:
                s, d = src.at[:, gi * T + tt], dst.at[half, pl.ds(e0, ED)]
            if dt == 0:

                @pl.when(n == 0)
                def _():
                    lcopy(s, d, rr.at[row, kk]).start()

                @pl.when(n > 0)
                def _():
                    rcopy(s, d, rs.at[row, kk], rr.at[row, kk], dev(gi, tt)).start()

            else:
                rcopy(s, d, rs.at[row, kk], rr.at[row, kk], dev(gi, tt)).start()

    lax.fori_loop(0, I, tile, 0)

    def give_eo(n, _):
        give_back(n, 1, eos, eor, False)
        return 0

    lax.fori_loop(0, I, give_eo, 0)

    ing, backg = ref["ing"], ref["backg"]
    vs, vr = ref["vs"], ref["vr"]

    def weight_grad(ep, _):
        e, p = ep // PR, lax.rem(ep, PR)
        cols = pl.ds(al(p * FS, FS), FS)
        vin[e, :, cols] = mm_tn(xr[e].reshape(z.team * CAP, D), igs[e, :, cols]).astype(BF16)
        vback[e, cols, :] = mm_tn(hid[e, :, cols], gr[e].reshape(z.team * CAP, D)).astype(BF16)
        for di in range(I):
            ii = lax.rem(i + di, I)
            part_in = vin.at[e, pl.ds(al(ii * DQ, DQ), DQ), cols]
            part_back = vback.at[e, cols, pl.ds(al(ii * DQ, DQ), DQ)]
            to_in, to_back = ing.at[e0 + e], backg.at[e0 + e]
            if di == 0:

                @pl.when(p == pos)
                def _():
                    lcopy(part_in, to_in, vr.at[0, e0 + e]).start()
                    lcopy(part_back, to_back, vr.at[1, e0 + e]).start()

                @pl.when(p != pos)
                def _():
                    rcopy(part_in, to_in, vs.at[0, ep * I], vr.at[0, e0 + e], dev(ii, half * PR + p)).start()
                    rcopy(part_back, to_back, vs.at[1, ep * I], vr.at[1, e0 + e], dev(ii, half * PR + p)).start()

            else:
                to = dev(ii, half * PR + p)
                rcopy(part_in, to_in, vs.at[0, ep * I + di], vr.at[0, e0 + e], to).start()
                rcopy(part_back, to_back, vs.at[1, ep * I + di], vr.at[1, e0 + e], to).start()
        return 0

    lax.fori_loop(0, ED * PR, weight_grad, 0)

    ggx = ref["ggx"]
    cacc = ref["cacc"]

    def from_of(n, dt):
        return lax.rem(i + n, I), lax.rem(t - dt + T, T)

    def wait_home(row, view):
        def one(n, _):
            for dt in range(T):
                fi, ft = from_of(n, dt)
                d = view(fi, ft)
                pltpu.make_async_copy(d, d, rr.at[row, n * T + dt]).wait()
            return 0

        lax.fori_loop(0, I, one, 0)

    def slot_view(buf):
        return lambda fi, ft: buf.at[ft // PR, pl.ds((fi * PR + lax.rem(ft, PR)) * ED, ED)]

    wait_home(2, lambda fi, ft: ggr.at[fi * T + ft])
    gg_swap = rcopy(ggr, ggx, xsm.at[1], xrm.at[1], dev(i, t, oh))
    gg_swap.start()
    wait_home(0, slot_view(sir))

    CH = 256

    def combine(rows, src, weighted):
        c0, c1 = idc[rows, 0:1], idc[rows, 1:2]
        w0 = gcol[rows, 0:1] if weighted else 1.0
        w1 = gcol[rows, 1:2] if weighted else 1.0
        cacc[...] = jnp.zeros_like(cacc)

        def one(c, _):
            lane = iota((OWN, CH), 1) + (c * CH + h * z.slots).astype(F32)
            w = jnp.where(c0 == lane, w0, 0.0) + jnp.where(c1 == lane, w1, 0.0)
            w = w.astype(BF16)
            for a in range(A):
                cacc[...] += mm(w, src[a, pl.ds(c * (CH // CAP), CH // CAP)].reshape(CH, D))
            return 0

        lax.fori_loop(0, z.slots // CH, one, 0)

    dbs, dbr = ref["dbs"], ref["dbr"]
    combine(other_rows, sir, False)
    dbs[...] = cacc[...].astype(BF16)
    db_swap = rcopy(dbs, dbr, xsm.at[2], xrm.at[2], dev(i, t, oh))
    db_swap.start()
    combine(mine_rows, sir, False)

    lane_own = iota((OWN, LANES), 1)
    m0, m1 = rp[mine_rows, 0:1], rp[mine_rows, 1:2]
    gg_swap.wait_recv()
    ggacc = ref["ggacc"]
    ggacc[...] = jnp.zeros_like(ggacc)

    def gate_back(q, _):
        fi, pp = q // PR, lax.rem(q, PR)
        k0, k1 = idc[mine_rows, 0:1], idc[mine_rows, 1:2]
        for buf, hh in ((ggr, h), (ggx, oh)):
            line = buf[fi * T + pp][0:1, :]
            for a in range(1, A):
                line = line + buf[fi * T + a * PR + pp][0:1, :]
            lane = lane_own + (q * z.lw + hh * z.slots).astype(F32)
            keep = lane_own < z.lw
            ggacc[0] += jnp.where(jnp.logical_and(keep, k0 == lane), line, 0.0)
            ggacc[1] += jnp.where(jnp.logical_and(keep, k1 == lane), line, 0.0)
        return 0

    lax.fori_loop(0, z.home // ED, gate_back, 0)
    gg0 = jnp.sum(ggacc[0], axis=1, keepdims=True)
    gg1 = jnp.sum(ggacc[1], axis=1, keepdims=True)
    mrouter = router[mine_rows, :]
    pgrad = jnp.where(m0 == lane_own, gg0, 0.0) + jnp.where(m1 == lane_own, gg1, 0.0)
    lgrad = (mrouter * (pgrad - jnp.sum(pgrad * mrouter, axis=1, keepdims=True))).astype(BF16)
    xn2 = xn2a[mine_rows, :]
    small = ref["small"]
    small[...] = jnp.where(iota((D, LANES), 1) < EXPERTS, mm_tn(xn2, lgrad), 0.0)
    through = mm_nt(lgrad, sall[...])
    db_swap.wait_recv()
    xgrad = cacc[...] + dbr[...].astype(F32) + through
    normed, spread_two = norm_of(resid[...])
    nrows = ref["nrows"]
    nrows[...] = jnp.zeros_like(nrows)
    nrows[EXPERTS + 1 : EXPERTS + 2, :] = jnp.sum(xgrad * normed, axis=0, keepdims=True)
    rgrad = ref["rgrad"]
    rgrad[...] = cota[mine_rows, :].astype(F32) + norm_back(xgrad * gains[1:2, :], normed, spread_two)

    agrad = rgrad[...].astype(BF16)

    def gw(j, row, count):
        return (0, pl.ds(al((j // 2) * D + row, LANES), count), pl.ds(al(lax.rem(j, 2) * D, LANES), D))

    hid[gw(jnp.int32(3), 0, D)] = mm_tn(agrad, mixed[...]).astype(BF16)
    mg = ref["mg"]
    mg[...] = mm(agrad, wall[3]).astype(BF16)
    pg = ref["pg"]

    def attend_back(n, _):
        rows = pl.ds(al((n // groups) * RP, 16), RP)
        cols = pl.ds(al(lax.rem(n, groups) * LANES, LANES), LANES)
        q, kk, v = qkv[0, rows, cols], qkv[1, rows, cols], qkv[2, rows, cols]
        m = mg[rows, cols]
        low = iota((RP, LANES), 1) < HD
        dq, dk, dv = [], [], []
        for s in range(2):
            sel = low if s == 0 else jnp.logical_not(low)
            low_p = probs[n * 2 + s]
            p = low_p.astype(F32)
            dp = mm_nt(jnp.where(sel, m, jnp.zeros_like(m)), v)
            dv.append(mm_tn(low_p, m))
            sg = (p * (dp - jnp.sum(dp * p, axis=-1, keepdims=True))).astype(BF16)
            dq.append(mm(sg, kk))
            dk.append(mm_tn(sg, q))
        pg[0, rows, cols] = (jnp.where(low, dq[0], dq[1]) * scale).astype(BF16)
        pg[1, rows, cols] = (jnp.where(low, dk[0], dk[1]) * scale).astype(BF16)
        pg[2, rows, cols] = jnp.where(low, dv[0], dv[1]).astype(BF16)
        return 0

    lax.fori_loop(0, z.own_img * groups, attend_back, 0)
    cacc[...] = jnp.zeros_like(cacc)

    def project_back(j, _):
        hid[gw(j, 0, D)] = mm_tn(xn1[...], pg[j]).astype(BF16)
        cacc[...] += mm_nt(pg[j], wall[j])
        return 0

    lax.fori_loop(0, 3, project_back, 0)

    s1r, s2s, s2r, s3s, s3r, s4s, s4r = (ref[n] for n in ("s1r", "s2s", "s2r", "s3s", "s3r", "s4s", "s4r"))
    u1s, u1r, u3s, u3r, u4s, u4r, u5s, u5r = (ref[n] for n in ("u1s", "u1r", "u3s", "u3r", "u4s", "u4r", "u5s", "u5r"))
    qs, qr = ref["qs"], ref["qr"]

    def quarter(ii):
        return pl.ds(al(ii * DQ, DQ), DQ)

    sw1 = []
    for b, ii in enumerate((i_core, i_diag)):
        for jr in range(2):
            src = hid.at[0, pl.ds(al(jr * D + ii * DQ, LANES), DQ), pl.ds(0, 2 * D)]
            sw1.append(rcopy(src, s1r.at[jr, b], qs.at[13 + 2 * b + jr], qr.at[13 + 2 * b + jr], dev(i_core, t)))
    for c in sw1:
        c.start()

    normed, spread_one = norm_of(xs[...])
    nrows[EXPERTS : EXPERTS + 1, :] = jnp.sum(cacc[...] * normed, axis=0, keepdims=True)
    tgrad = rgrad[...] + norm_back(cacc[...] * gains[0:1, :], normed, spread_one)
    tgs, tgr = ref["tgs"], ref["tgr"]
    tgs[...] = tgrad.astype(BF16)
    t_swap = rcopy(tgs, tgr, xsm.at[3], xrm.at[3], dev(i, t, oh))
    t_swap.start()
    small[...] = small[...] + jnp.transpose(nrows[...])
    for b, ii in enumerate((i_core, i_diag)):
        u1s[b] = small[quarter(ii), :]
    sv1 = rcopy(u1s, u1r, qs.at[1], qr.at[1], dev(i_core, t))
    sv1.start()
    for c in sw1:
        c.wait_recv()
    sv1.wait_recv()
    accu, acc2 = ref["accu"], ref["acc2"]
    for b, ii in enumerate((i, i_far)):
        for j in range(4):
            for hh, keep in ((oh, False), (h, True)):
                cols = pl.ds(al((j % 2) * D + hh * EC, LANES), EC)
                here = hid[0, pl.ds(al((j // 2) * D + ii * DQ, LANES), DQ), cols].astype(F32)
                here = here + s1r[j // 2, b, :, cols].astype(F32)
                if keep:
                    acc2[j, b] = here
                else:
                    s2s[j, b] = here.astype(BF16)
        accu[b] = small[quarter(ii), :] + u1r[b]
    sw2 = rcopy(s2s, s2r, qs.at[2], qr.at[2], dev(i, t, oh))
    sw2.start()
    u3s[...] = accu[1]
    sv3 = rcopy(u3s, u3r, qs.at[3], qr.at[3], dev(i_far, t))
    sv3.start()

    out_o, tg_o = ref["out_o"], ref["tg_o"]
    mos, mor, outs, outr = ref["mos"], ref["mor"], ref["outs"], ref["outr"]
    wait_home(1, slot_view(eor))
    combine(other_rows, eor, True)
    mos[...] = cacc[...].astype(BF16)
    m_swap = rcopy(mos, mor, xsm.at[4], xrm.at[4], dev(i, t, oh))
    m_swap.start()

    sw2.wait_recv()
    acc2[...] = acc2[...] + s2r[...].astype(F32)
    s3s[...] = acc2[:, 1].astype(BF16)
    sw3 = rcopy(s3s, s3r, qs.at[4], qr.at[4], dev(i_far, t))
    sw3.start()
    sv3.wait_recv()
    accu[0] = accu[0] + u3r[...]
    u4s[...] = accu[0]

    combine(mine_rows, eor, True)
    m_swap.wait_recv()
    outs[...] = (resid[...] + cacc[...] + mor[...].astype(F32)).astype(BF16)
    o_swap = rcopy(outs, outr, xsm.at[5], xrm.at[5], dev(i, t, oh))
    o_swap.start()
    for m in range(z.own_img):
        out_o[h * z.own_img + m] = outs[pl.ds(m * RP, L), :]
        tg_o[h * z.own_img + m] = tgs[pl.ds(m * RP, L), :]

    sw3.wait_recv()
    acc2[:, 0] = acc2[:, 0] + s3r[...].astype(F32)
    s4s[...] = acc2[:, 0].astype(BF16)
    last = []
    for dt in range(1, T):
        tt = lax.rem(t + dt, T)
        rows = pl.ds(al(tt * WR, WR), WR)
        last.append(rcopy(s4s.at[:, rows, :], s4r.at[dt], qs.at[4 + 2 * dt], qr.at[4 + 2 * dt], dev(i, tt)))
        last.append(rcopy(u4s.at[rows, :], u4r.at[dt], qs.at[5 + 2 * dt], qr.at[5 + 2 * dt], dev(i, tt)))
    for c in last:
        c.start()
    for c in last:
        c.wait_recv()
    wfin, sfin = ref["wfin"], ref["sfin"]
    my_rows = pl.ds(al(t * WR, WR), WR)
    total = acc2[:, 0, my_rows, :]
    part = accu[0, my_rows, :]
    for dt in range(1, T):
        total = total + s4r[dt].astype(F32)
        part = part + u4r[dt]
    wfin[...] = total
    u5s[...] = part
    sv5 = rcopy(u5s, u5r, qs.at[12], qr.at[12], dev(i, t, oh))
    sv5.start()
    t_swap.wait_recv()
    o_swap.wait_recv()
    for m in range(z.own_img):
        out_o[oh * z.own_img + m] = outr[pl.ds(m * RP, L), :]
        tg_o[oh * z.own_img + m] = tgr[pl.ds(m * RP, L), :]
    sv5.wait_recv()
    sfin[...] = u5s[...] + u5r[...]

    def grads_in(e, _):
        pltpu.make_async_copy(ing.at[e], ing.at[e], vr.at[0, e]).wait()
        pltpu.make_async_copy(backg.at[e], backg.at[e], vr.at[1, e]).wait()
        return 0

    lax.fori_loop(0, z.home, grads_in, 0)

    def grads_out(ep, _):
        p = lax.rem(ep, PR)
        for di in range(I):
            a_in = vin.at[0, pl.ds(0, DQ), pl.ds(0, FS)]
            a_back = vback.at[0, pl.ds(0, FS), pl.ds(0, DQ)]
            if di == 0:

                @pl.when(p != pos)
                def _():
                    pltpu.make_async_copy(a_in, a_in, vs.at[0, ep * I]).wait()
                    pltpu.make_async_copy(a_back, a_back, vs.at[1, ep * I]).wait()

            else:
                pltpu.make_async_copy(a_in, a_in, vs.at[0, ep * I + di]).wait()
                pltpu.make_async_copy(a_back, a_back, vs.at[1, ep * I + di]).wait()
        return 0

    lax.fori_loop(0, ED * PR, grads_out, 0)

    def back_out(n, _):
        for dt in range(T):

            def one():
                for row, buf in ((0, sis), (1, eos)):
                    d = buf.at[:, 0]
                    pltpu.make_async_copy(d, d, rs.at[row, n * T + dt]).wait()
                pltpu.make_async_copy(ggs.at[0], ggs.at[0], rs.at[2, n * T + dt]).wait()

            if dt == 0:
                pl.when(n > 0)(one)
            else:
                one()
        return 0

    lax.fori_loop(0, I, back_out, 0)
    for c in g_moved[1:] + x_moved[1:] + gate_moved[1:]:
        c.wait_send()
    for c in first + [b_x, b_y, b_ys, b_c, b_cs, f_x, f_c, f_cs, f_c2, f_c3]:
        c.wait_send()
    for c in (x_swap, gg_swap, db_swap, t_swap, m_swap, o_swap, *sw1, sv1, sw2, sv3, sw3, sv5, *last):
        c.wait_send()


def call(z, tok, cot, rt, wpack, spack, win, wback):
    T, I, PR, A, ED, D = z.tensor, z.team_i, z.pair, z.halves, z.own_e, z.width
    OWN, ROWS, EC, DQ, WR = z.own, z.rows, z.ecols, z.dq, z.wrow
    team = z.team
    V, S = pltpu.VMEM, pltpu.SemaphoreType.DMA
    ins = ["tok", "cot", "rt", "wpack", "spack", "win", "wback"]
    outs = {
        "out_o": jax.ShapeDtypeStruct(tok.shape, BF16),
        "tg_o": jax.ShapeDtypeStruct(tok.shape, BF16),
        "wfin": jax.ShapeDtypeStruct((4, WR, EC), F32),
        "sfin": jax.ShapeDtypeStruct((WR, LANES), F32),
        "ing": jax.ShapeDtypeStruct(win.shape, BF16),
        "backg": jax.ShapeDtypeStruct(wback.shape, BF16),
    }
    heads_own = z.own_img * z.nh
    scratch = {
        "wall": V((4, D, D), BF16), "sall": V((D, LANES), BF16), "gains": V((8, D), F32),
        "xn2a": V((ROWS, D), BF16), "cota": V((ROWS, D), BF16), "rp": V((ROWS, LANES), F32),
        "xs": V((OWN, D), F32), "both": V((ROWS, LANES), BF16), "idc": V((ROWS, LANES), F32),
        "idr": V((LANES, ROWS), F32), "gs": V((z.home, CAP, D), BF16), "xsl": V((z.home, CAP, D), BF16),
        "vin": V((ED, D, z.ff), BF16), "vback": V((ED, z.ff, D), BF16),
        "xr": V((ED, team, CAP, D), BF16), "gr": V((ED, team, CAP, D), BF16), "gater": V((team, 8, LANES), F32),
        "xn1": V((OWN, D), BF16), "qkv": V((3, OWN, D), BF16), "mixed": V((OWN, D), BF16),
        "probs": V((heads_own, z.pad, z.pad), BF16), "resid": V((OWN, D), F32), "router": V((ROWS, LANES), F32),
        "gcol": V((ROWS, LANES), F32), "gsend": V((z.home // ED, 8, LANES), F32),
        "hid": V((ED, team * CAP, z.ff), BF16), "igs": V((ED, team * CAP, z.ff), BF16),
        "eoa": V((T * CAP, D), F32), "sia": V((T * CAP, D), F32),
        "eos": V((ED, team, CAP, D), BF16), "sis": V((ED, team, CAP, D), BF16), "ggs": V((team, 8, LANES), F32),
        "eor": V((A, z.home, CAP, D), BF16), "sir": V((A, z.home, CAP, D), BF16), "ggr": V((team, 8, LANES), F32),
        "gcols": V((T, LANES, LANES), F32), "gtile": V((T * CAP, D), BF16),
        "ggx": V((team, 8, LANES), F32), "cacc": V((OWN, D), F32), "dbs": V((OWN, D), BF16), "dbr": V((OWN, D), BF16),
        "ggacc": V((2, OWN, LANES), F32), "small": V((D, LANES), F32), "nrows": V((LANES, D), F32),
        "rgrad": V((OWN, D), F32), "mg": V((OWN, D), BF16), "pg": V((3, OWN, D), BF16),
        "s1r": V((2, 2, DQ, 2 * D), BF16),
        "s2s": V((4, 2, DQ, EC), BF16), "s2r": V((4, 2, DQ, EC), BF16),
        "s3s": V((4, DQ, EC), BF16), "s3r": V((4, DQ, EC), BF16),
        "s4s": V((4, DQ, EC), BF16), "s4r": V((T, 4, WR, EC), BF16),
        "u1s": V((2, DQ, LANES), F32), "u1r": V((2, DQ, LANES), F32),
        "u3s": V((DQ, LANES), F32), "u3r": V((DQ, LANES), F32),
        "u4s": V((DQ, LANES), F32), "u4r": V((T, WR, LANES), F32),
        "u5s": V((WR, LANES), F32), "u5r": V((WR, LANES), F32),
        "accu": V((2, DQ, LANES), F32), "acc2": V((4, 2, DQ, EC), F32),
        "tgs": V((OWN, D), BF16), "tgr": V((OWN, D), BF16), "mos": V((OWN, D), BF16), "mor": V((OWN, D), BF16),
        "outs": V((OWN, D), BF16), "outr": V((OWN, D), BF16),
        "ws": S((5, 4)), "wr": S((5, 4)), "wl": S((2,)), "es": S((2, I * PR)), "er": S((2, I * PR)),
        "ds": S((3, team)), "dr": S((3, team)), "rs": S((3, team)), "rr": S((3, team)),
        "vs": S((2, ED * PR * I)), "vr": S((2, z.home)), "xsm": S((6,)), "xrm": S((6,)), "qs": S((20,)), "qr": S((20,)),
    }
    vmem = pl.BlockSpec(memory_space=pltpu.VMEM)
    anyw = pl.BlockSpec(memory_space=pl.ANY)
    names = ins + list(outs) + list(scratch)
    return pl.pallas_call(
        functools.partial(kernel, z, names),
        out_shape=tuple(outs.values()),
        in_specs=[vmem] * 5 + [anyw] * 2,
        out_specs=(vmem,) * 4 + (anyw,) * 2,
        scratch_shapes=list(scratch.values()),
        compiler_params=pltpu.CompilerParams(collective_id=0, has_side_effects=True, vmem_limit_bytes=64 * 1024 * 1024 - 65536),
        name="block",
    )(tok, cot, rt, wpack, spack, win, wback)


def solution(mesh):
    def local(tokens, cotangent, w_qkv, w_out, w_router, norm_one, norm_two, w_in, w_back, routes):
        images, length, width = tokens.shape
        z = Sizes(mesh.shape, images, length, width, w_in.shape[0], w_in.shape[2])
        R = z.reps
        wpack = jnp.concatenate([w_qkv, jnp.transpose(w_out)[None]], axis=0)
        fill = jnp.zeros((w_router.shape[0], LANES - EXPERTS - 2), BF16)
        spack = jnp.concatenate([w_router, norm_one[:, None], norm_two[:, None], fill], axis=1)
        sets = None
        if R > 1:
            sets = [[a * R + b for b in range(R)] for a in range(z.team_i)]
            w_in = lax.all_gather(w_in, "fsdp", axis=1, tiled=True, axis_index_groups=sets)
            w_back = lax.all_gather(w_back, "fsdp", axis=2, tiled=True, axis_index_groups=sets)
            place = lax.axis_index("tensor") * z.wrow

            def quarter(w, axis):
                w = lax.all_gather(w, "tensor", axis=axis, tiled=True)
                w = lax.all_gather(w, "fsdp", axis=axis, tiled=True, axis_index_groups=sets)
                return lax.dynamic_slice_in_dim(w, place, z.wrow, axis)

            wpack, spack = quarter(wpack, 1), quarter(spack, 0)
        out, tgrad, wfin, sfin, ing, backg = call(z, tokens, cotangent, routes, wpack, spack, w_in, w_back)
        if R > 1:
            ing = lax.psum_scatter(ing, "fsdp", scatter_dimension=1, tiled=True, axis_index_groups=sets)
            backg = lax.psum_scatter(backg, "fsdp", scatter_dimension=2, tiled=True, axis_index_groups=sets)

            def shard(w, axis):
                w = lax.all_gather(w, "tensor", axis=axis, tiled=True)
                w = lax.psum_scatter(w, "fsdp", scatter_dimension=axis, tiled=True, axis_index_groups=sets)
                rows = w.shape[axis] // z.tensor
                return lax.dynamic_slice_in_dim(w, lax.axis_index("tensor") * rows, rows, axis)

            wfin, sfin = shard(wfin, 1), shard(sfin, 0)
        return (
            out,
            tgrad.astype(F32),
            wfin[:3],
            jnp.transpose(wfin[3]),
            sfin[:, :EXPERTS],
            sfin[:, EXPERTS],
            sfin[:, EXPERTS + 1],
            ing.astype(F32),
            backg.astype(F32),
        )

    rows = P(("fsdp", "tensor"), None, None)
    qkv = P(None, ("fsdp", "tensor"), "heads")
    proj = P("heads", ("fsdp", "tensor"))
    table = P(("fsdp", "tensor"), None)
    gain = P(("fsdp", "tensor"))
    first = P("heads", "fsdp", "tensor")
    second = P("heads", "tensor", "fsdp")
    return jax.shard_map(
        local,
        mesh=mesh,
        in_specs=(rows, rows, qkv, proj, table, gain, gain, first, second, rows),
        out_specs=(rows, rows, qkv, proj, table, gain, gain, first, second),
        check_vma=False,
    )
```

```python
import functools

import jax
import jax.numpy as jnp
from jax import lax
from jax.experimental import pallas as pl
from jax.experimental.pallas import tpu as pltpu
from jax.sharding import PartitionSpec as P

HD = 64
EXPERTS = 32
CAP = 64
PAIR = 2
EARLY = 2
LANES = 128
MESH = pl.DeviceIdType.MESH
F32 = jnp.float32
BF16 = jnp.bfloat16


def mm(a, b):
    return lax.dot_general(a, b, (((1,), (0,)), ((), ())), preferred_element_type=F32)


def mm_nt(a, b):
    return lax.dot_general(a, b, (((1,), (1,)), ((), ())), preferred_element_type=F32)


def mm_tn(a, b):
    return lax.dot_general(a, b, (((0,), (0,)), ((), ())), preferred_element_type=F32)


def iota(shape, dim):
    return lax.broadcasted_iota(jnp.int32, shape, dim).astype(F32)


def norm_of(x):
    centre = x - jnp.mean(x, axis=-1, keepdims=True)
    spread = lax.rsqrt(jnp.mean(centre * centre, axis=-1, keepdims=True) + 1e-06)
    return centre * spread, spread


def norm_back(scaled, normed, spread):
    middle = jnp.mean(scaled, axis=-1, keepdims=True)
    along = jnp.mean(scaled * normed, axis=-1, keepdims=True)
    return spread * (scaled - middle - normed * along)


class Sizes:
    def __init__(self, mesh_shape, images, length, width, home, ff_shard):
        self.tensor = mesh_shape["tensor"]
        self.heads = mesh_shape["heads"]
        self.pair = PAIR if self.tensor % PAIR == 0 else 1
        self.halves = self.tensor // self.pair
        self.team_i = min(mesh_shape["fsdp"], max(1, home // self.tensor))
        self.reps = mesh_shape["fsdp"] // self.team_i
        self.team = self.team_i * self.tensor
        self.home = home
        self.own_e = home // (self.team_i * self.pair)
        self.images = images
        self.length = length
        self.width = width
        self.pad = -(-length // 16) * 16
        self.own_img = images // self.heads
        self.own = self.own_img * self.pad
        self.all = images * self.pad
        self.rows = -(-self.all // LANES) * LANES
        self.ffs = ff_shard
        self.ff = ff_shard * self.pair
        self.slots = home * CAP
        self.dq = width // self.team_i
        self.wrow = self.dq // self.tensor
        self.ecols = width // self.heads
        self.lw = self.own_e * CAP
        self.nh = width // HD


def kernel(z, names, *refs):
    ref = dict(zip(names, refs))
    tok, cot, rt, wpack, spack = ref["tok"], ref["cot"], ref["rt"], ref["wpack"], ref["spack"]
    win, wback = ref["win"], ref["wback"]
    T, I, R = z.tensor, z.team_i, z.reps
    D, L, RP = z.width, z.length, z.pad
    OWN, ALL, ROWS = z.own, z.all, z.rows
    PR, A, ED = z.pair, z.halves, z.own_e
    FS, DQ, WR, EC = z.ffs, z.dq, z.wrow, z.ecols

    fs, h, t = lax.axis_index("fsdp"), lax.axis_index("heads"), lax.axis_index("tensor")
    i, r = fs // R, lax.rem(fs, R)
    oh = 1 - h
    pos, half = lax.rem(t, PR), t // PR
    e0 = (i * PR + pos) * ED
    i_core = i + 1 - 2 * lax.rem(i, 2)
    i_far = lax.rem(i + 2, I)
    i_diag = lax.rem(i_core + 2, I)
    mine = i * T + t

    def dev(ii, tt, hh=None):
        return {"fsdp": ii * R + r, "heads": h if hh is None else hh, "tensor": tt}

    def rcopy(src, dst, ssem, rsem, target):
        return pltpu.make_async_remote_copy(
            src_ref=src, dst_ref=dst, send_sem=ssem, recv_sem=rsem, device_id=target, device_id_type=MESH
        )

    def lcopy(src, dst, sem):
        return pltpu.make_async_copy(src, dst, sem)

    def al(v, m):
        return pl.multiple_of(v, m)

    bar = pltpu.get_barrier_semaphore()
    for di in range(I):
        for dt in range(T):
            if di or dt:
                pl.semaphore_signal(
                    bar, inc=1, device_id=dev(lax.rem(i + di, I), lax.rem(t + dt, T)), device_id_type=MESH
                )
    pl.semaphore_signal(bar, inc=1, device_id=dev(i, t, oh), device_id_type=MESH)
    pl.semaphore_wait(bar, I * T)

    wall, sall = ref["wall"], ref["sall"]
    ws, wr, wl = ref["ws"], ref["wr"], ref["wl"]

    def shard_of(buf):
        return buf.at[:, pl.ds(al(mine * WR, WR), WR), pl.ds(al(h * EC, LANES), EC)]

    def block(buf, ii, hh):
        return buf.at[:, pl.ds(al(ii * DQ, DQ), DQ), pl.ds(al(hh * EC, LANES), EC)]

    def srows(ii):
        return sall.at[pl.ds(al(ii * DQ, DQ), DQ)]

    s_mine = sall.at[pl.ds(al(mine * WR, WR), WR)]
    first = []
    for dt in range(1, T):
        to = dev(i, lax.rem(t + dt, T))
        first.append(rcopy(wpack, shard_of(wall), ws.at[0, dt], wr.at[0, dt], to))
        first.append(rcopy(spack, s_mine, ws.at[1, dt], wr.at[1, dt], to))
    for c in first:
        c.start()
    own_w = [lcopy(wpack, shard_of(wall), wl.at[0]), lcopy(spack, s_mine, wl.at[1])]
    for c in own_w:
        c.start()

    vin, vback = ref["vin"], ref["vback"]
    es, er = ref["es"], ref["er"]
    moved = []
    for di in range(I):
        for dp in range(PR):
            k = di * PR + dp
            ii, pp = lax.rem(i + di, I), lax.rem(pos + dp, PR)
            them = pl.ds((ii * PR + pp) * ED, ED)
            to_in = vin.at[:, pl.ds(al(i * DQ, DQ), DQ), pl.ds(al(pos * FS, FS), FS)]
            to_back = vback.at[:, pl.ds(al(pos * FS, FS), FS), pl.ds(al(i * DQ, DQ), DQ)]
            if k == 0:
                moved.append(lcopy(win.at[them], to_in, er.at[0, 0]))
                moved.append(lcopy(wback.at[them], to_back, er.at[1, 0]))
            else:
                to = dev(ii, half * PR + pp)
                moved.append(rcopy(win.at[them], to_in, es.at[0, k], er.at[0, k], to))
                moved.append(rcopy(wback.at[them], to_back, es.at[1, k], er.at[1, k], to))
    for c in moved[: 2 * PR]:
        c.start()

    xr, gr, gater = ref["xr"], ref["gr"], ref["gater"]
    ds, dr = ref["ds"], ref["dr"]

    def spread(src, dst, row, whole):
        made = []
        for di in range(I):
            for dt in range(T):
                kk = di * T + dt
                ii, tt = lax.rem(i + di, I), lax.rem(t + dt, T)
                pp = lax.rem(tt, PR)
                if whole:
                    s, d = src.at[ii * PR + pp], dst.at[mine]
                else:
                    s, d = src.at[pl.ds((ii * PR + pp) * ED, ED)], dst.at[:, mine]
                if kk == 0:
                    made.append(lcopy(s, d, dr.at[row, 0]))
                else:
                    made.append(rcopy(s, d, ds.at[row, kk], dr.at[row, kk], dev(ii, tt)))
        for c in made:
            c.start()
        return made

    xn2a, cota, rp = ref["xn2a"], ref["cota"], ref["rp"]
    xn2a[...] = jnp.zeros_like(xn2a)
    cota[...] = jnp.zeros_like(cota)
    rp[...] = jnp.full_like(rp, -1.0)
    xs = ref["xs"]
    xs[...] = jnp.zeros_like(xs)
    for m in range(z.images):
        cota[pl.ds(m * RP, L), :] = cot[m]
        rp[pl.ds(m * RP, L), 0:2] = rt[m].astype(F32)
    for m in range(z.own_img):
        xs[pl.ds(m * RP, L), :] = tok[h * z.own_img + m].astype(F32)

    lane_all = iota((ROWS, LANES), 1)
    r0, r1 = rp[:, 0:1], rp[:, 1:2]
    oh0 = jnp.where(r0 == lane_all, 1.0, 0.0)
    oh1 = jnp.where(r1 == lane_all, 1.0, 0.0)
    both = ref["both"]
    both[...] = (oh0 + oh1).astype(BF16)
    idc = ref["idc"]

    def count(c, _):
        at = pl.ds(al(c * LANES, LANES), LANES)
        before = iota((LANES, ROWS), 1) < iota((LANES, ROWS), 0) + (c * LANES).astype(F32)
        counted = mm(jnp.where(before, 1.0, 0.0).astype(BF16), both[...])
        lane = iota((LANES, LANES), 1)
        q0, q1 = rp[at, 0:1], rp[at, 1:2]
        number = counted + lane * CAP
        n0 = jnp.sum(jnp.where(q0 == lane, number, 0.0), axis=1, keepdims=True)
        n1 = jnp.sum(jnp.where(q1 == lane, number, 0.0), axis=1, keepdims=True)
        n0 = jnp.where(q0 < 0.0, -1.0, n0)
        n1 = jnp.where(q1 < 0.0, -1.0, n1)
        idc[at, :] = jnp.where(lane == 0.0, n0, jnp.where(lane == 1.0, n1, -1.0))
        return 0

    lax.fori_loop(0, ROWS // LANES, count, 0)
    idr = ref["idr"]
    idr[...] = jnp.transpose(idc[...])

    gs, xsl = ref["gs"], ref["xsl"]

    gsend = ref["gsend"]

    def dispatch(source, target, gates=None):
        def one(c, _):
            slot = iota((LANES, ROWS), 0) + (c * LANES + h * z.slots).astype(F32)
            in0, in1 = idr[0:1, :] == slot, idr[1:2, :] == slot
            pick = jnp.where(in0, 1.0, 0.0) + jnp.where(in1, 1.0, 0.0)
            got = mm(pick.astype(BF16), source[...]).astype(BF16)
            per = LANES // CAP
            target[pl.ds(c * per, per)] = got.reshape(per, CAP, D)
            if gates is not None:
                w = jnp.where(in0, gates[0:1, :], 0.0) + jnp.where(in1, gates[1:2, :], 0.0)
                col = jnp.broadcast_to(jnp.sum(w, axis=1, keepdims=True), (LANES, LANES))
                sub, lane = iota((LANES, LANES), 0), iota((LANES, LANES), 1)
                for q in range(LANES // z.lw):
                    here = jnp.logical_and(lane < z.lw, lane == sub - q * z.lw)
                    line = jnp.sum(jnp.where(here, col, 0.0), axis=0, keepdims=True)
                    gsend[c * (LANES // z.lw) + q] = jnp.broadcast_to(line, (8, LANES))
            return 0

        lax.fori_loop(0, z.slots // LANES, one, 0)

    for c in first:
        c.wait_recv()
    for c in own_w:
        c.wait()
    b_x = rcopy(block(wall, i, h), block(wall, i, h), ws.at[2, 0], wr.at[2, 0], dev(i, t, oh))
    b_y = rcopy(block(wall, i, h), block(wall, i, h), ws.at[2, 1], wr.at[2, 1], dev(i_far, t))
    b_ys = rcopy(srows(i), srows(i), ws.at[2, 2], wr.at[2, 2], dev(i_far, t))
    b_c = rcopy(block(wall, i, h), block(wall, i, h), ws.at[2, 3], wr.at[2, 3], dev(i_core, t))
    b_cs = rcopy(srows(i), srows(i), ws.at[3, 0], wr.at[3, 0], dev(i_core, t))
    for c in (b_y, b_x, b_ys, b_c, b_cs):
        c.start()
    for c in moved[2 * PR :]:
        c.start()
    dispatch(cota, gs)
    g_moved = spread(gs, gr, 0, False)
    b_y.wait_recv()
    f_x = rcopy(block(wall, i_far, h), block(wall, i_far, h), ws.at[3, 1], wr.at[3, 1], dev(i, t, oh))
    f_x.start()
    f_c = rcopy(block(wall, i_far, h), block(wall, i_far, h), ws.at[3, 2], wr.at[3, 2], dev(i_core, t))
    f_c.start()
    b_ys.wait_recv()
    f_cs = rcopy(srows(i_far), srows(i_far), ws.at[3, 3], wr.at[3, 3], dev(i_core, t))
    f_cs.start()
    b_x.wait_recv()
    f_c2 = rcopy(block(wall, i, oh), block(wall, i, oh), ws.at[4, 0], wr.at[4, 0], dev(i_core, t))
    f_c2.start()

    f_x.wait_recv()
    f_c3 = rcopy(block(wall, i_far, oh), block(wall, i_far, oh), ws.at[4, 1], wr.at[4, 1], dev(i_core, t))
    f_c3.start()
    for c in (b_c, b_cs, f_c, f_cs, f_c2, f_c3):
        c.wait_recv()

    sall_t = jnp.transpose(sall[...].astype(F32))
    gains = ref["gains"]
    gains[...] = sall_t[EXPERTS : EXPERTS + 8, :]
    xn1, qkv, mixed, probs = ref["xn1"], ref["qkv"], ref["mixed"], ref["probs"]
    normed, _ = norm_of(xs[...])
    xn1[...] = (normed * gains[0:1, :]).astype(BF16)

    def project(j, _):
        qkv[j] = mm(xn1[...], wall[j]).astype(BF16)
        return 0

    lax.fori_loop(0, 3, project, 0)
    groups = D // LANES
    scale = HD ** (-0.5)

    def attend(n, _):
        rows = pl.ds(al((n // groups) * RP, 16), RP)
        cols = pl.ds(al(lax.rem(n, groups) * LANES, LANES), LANES)
        q, kk, v = qkv[0, rows, cols], qkv[1, rows, cols], qkv[2, rows, cols]
        low = iota((RP, LANES), 1) < HD
        key = iota((RP, RP), 1)
        outs = []
        for s in range(2):
            sel = low if s == 0 else jnp.logical_not(low)
            score = mm_nt(jnp.where(sel, q, jnp.zeros_like(q)), kk) * scale
            score = jnp.where(key < L, score, -1e30)
            e = jnp.exp(score - jnp.max(score, axis=-1, keepdims=True))
            p = e / jnp.sum(e, axis=-1, keepdims=True)
            p = p.astype(BF16)
            probs[n * 2 + s] = p
            outs.append(mm(p, v))
        mixed[rows, cols] = jnp.where(low, outs[0], outs[1]).astype(BF16)
        return 0

    lax.fori_loop(0, z.own_img * groups, attend, 0)
    resid = ref["resid"]
    resid[...] = xs[...] + mm_nt(mixed[...], wall[3])
    normed, _ = norm_of(resid[...])
    mine_rows = pl.ds(al(h * OWN, 16), OWN)
    other_rows = pl.ds(al(oh * OWN, 16), OWN)
    xn2a[mine_rows, :] = (normed * gains[1:2, :]).astype(BF16)

    xsm, xrm = ref["xsm"], ref["xrm"]
    x_swap = rcopy(xn2a.at[mine_rows], xn2a.at[mine_rows], xsm.at[0], xrm.at[0], dev(i, t, oh))
    x_swap.start()
    x_swap.wait_recv()
    logits = mm(xn2a[...], sall[...])
    logits = jnp.where(lane_all < EXPERTS, logits, -1e30)
    e = jnp.exp(logits - jnp.max(logits, axis=-1, keepdims=True))
    router = ref["router"]
    router[...] = e / jnp.sum(e, axis=-1, keepdims=True)
    gcol = ref["gcol"]
    g0 = jnp.sum(jnp.where(rp[:, 0:1] == lane_all, router[...], 0.0), axis=1, keepdims=True)
    g1 = jnp.sum(jnp.where(rp[:, 1:2] == lane_all, router[...], 0.0), axis=1, keepdims=True)
    gcol[...] = jnp.where(lane_all == 0.0, g0, g1)
    grow = ref["grow"]
    grow[...] = jnp.transpose(gcol[...])
    dispatch(xn2a, xsl, grow)
    gate_moved = spread(gsend, gater, 2, True)
    x_moved = spread(xsl, xr, 1, False)

    hid, igs, gtile = ref["hid"], ref["igs"], ref["gtile"]
    eoa, sia = ref["eoa"], ref["sia"]
    eos, sis, ggs = ref["eos"], ref["sis"], ref["ggs"]
    eor, sir, ggr = ref["eor"], ref["sir"], ref["ggr"]
    rs, rr = ref["rs"], ref["rr"]
    gcols = ref["gcols"]
    ggs[...] = jnp.zeros_like(ggs)
    for c in moved:
        c.wait()
    TR = T * CAP
    eye = iota((LANES, LANES), 0) == iota((LANES, LANES), 1)

    def wait_role(row, kk, dst):
        pltpu.make_async_copy(dst, dst, dr.at[row, kk]).wait()

    def tile(n, _):
        gi = lax.rem(i - n + I, I)
        grp = pl.ds(gi * T, T)
        for dt in range(T):
            src = gi * T + lax.rem(t - dt + T, T)
            wait_role(0, n * T + dt, gr.at[:, src])
            wait_role(1, n * T + dt, xr.at[:, src])
            wait_role(2, n * T + dt, gater.at[src])
        for dt in range(T):
            row = gater[gi * T + dt][0:1, :]
            col = jnp.sum(jnp.where(eye, jnp.broadcast_to(row, (LANES, LANES)), 0.0), axis=1, keepdims=True)
            gcols[dt] = jnp.broadcast_to(col, (LANES, LANES))

        def part(ep, _):
            e, p = ep // PR, lax.rem(ep, PR)
            cols = pl.ds(al(p * FS, FS), FS)
            trow = pl.ds(al(gi * TR, TR), TR)
            x = xr[e, grp].reshape(TR, D)

            @pl.when(p == 0)
            def _():
                g = gr[e, grp].reshape(TR, D)
                gtile[...] = g
                gate = gcols[:, pl.ds(al(e * CAP, CAP), CAP), :].reshape(TR, LANES)[:, 0:1]
                gr[e, grp] = (g.astype(F32) * gate).astype(BF16).reshape(T, CAP, D)
                eoa[...] = jnp.zeros_like(eoa)
                sia[...] = jnp.zeros_like(sia)

            inner = mm(x, vin[e, :, cols])
            erf = lax.erf(inner * (0.5**0.5))
            cdf = 0.5 * (1.0 + erf)
            hidden = (inner * cdf).astype(BF16)
            slope = cdf + inner * (jnp.exp(-0.5 * inner * inner) * 0.3989422804014327)
            hid[e, trow, cols] = hidden
            eoa[...] += mm(hidden, vback[e, cols, :])
            back = mm_nt(gr[e, grp].reshape(TR, D), vback[e, cols, :])
            inner_grad = (back * slope).astype(BF16)
            igs[e, trow, cols] = inner_grad
            sia[...] += mm_nt(inner_grad, vin[e, :, cols])

            @pl.when(p == PR - 1)
            def _():
                eo = eoa[...]
                eos[e, grp] = eo.astype(BF16).reshape(T, CAP, D)
                sis[e, grp] = sia[...].astype(BF16).reshape(T, CAP, D)
                gg = jnp.sum(eo * gtile[...].astype(F32), axis=1, keepdims=True)
                there = iota((CAP, LANES), 1) == iota((CAP, LANES), 0) + (e * CAP).astype(F32)
                for dt in range(T):
                    piece = jnp.broadcast_to(gg[dt * CAP : (dt + 1) * CAP], (CAP, LANES))
                    line = jnp.sum(jnp.where(there, piece, 0.0), axis=0, keepdims=True)
                    ggs[gi * T + dt] = ggs[gi * T + dt] + jnp.broadcast_to(line, (8, LANES))

            return 0

        lax.fori_loop(0, ED * PR, part, 0)
        give_back(n, 2, ggs, ggr, True)
        give_back(n, 0, sis, sir, False)
        return 0

    def give_back(n, row, src, dst, whole):
        gi = lax.rem(i - n + I, I)
        for dt in range(T):
            tt = lax.rem(t + dt, T)
            kk = n * T + dt
            if whole:
                s, d = src.at[gi * T + tt], dst.at[mine]
            else:
                s, d = src.at[:, gi * T + tt], dst.at[half, pl.ds(e0, ED)]
            if dt == 0:

                @pl.when(n == 0)
                def _():
                    lcopy(s, d, rr.at[row, kk]).start()

                @pl.when(n > 0)
                def _():
                    rcopy(s, d, rs.at[row, kk], rr.at[row, kk], dev(gi, tt)).start()

            else:
                rcopy(s, d, rs.at[row, kk], rr.at[row, kk], dev(gi, tt)).start()

    lax.fori_loop(0, I, tile, 0)

    ing, backg = ref["ing"], ref["backg"]
    vs, vr = ref["vs"], ref["vr"]

    def weight_grad(ep, _):
        e, p = ep // PR, lax.rem(ep, PR)
        cols = pl.ds(al(p * FS, FS), FS)
        vin[e, :, cols] = mm_tn(xr[e].reshape(z.team * CAP, D), igs[e, :, cols]).astype(BF16)
        vback[e, cols, :] = mm_tn(hid[e, :, cols], gr[e].reshape(z.team * CAP, D)).astype(BF16)
        return 0

    def give_grad(ep, _):
        e, p = ep // PR, lax.rem(ep, PR)
        cols = pl.ds(al(p * FS, FS), FS)
        for di in range(I):
            ii = lax.rem(i + di, I)
            part_in = vin.at[e, pl.ds(al(ii * DQ, DQ), DQ), cols]
            part_back = vback.at[e, cols, pl.ds(al(ii * DQ, DQ), DQ)]
            to_in, to_back = ing.at[e0 + e], backg.at[e0 + e]
            if di == 0:

                @pl.when(p == pos)
                def _():
                    lcopy(part_in, to_in, vr.at[0, e0 + e]).start()
                    lcopy(part_back, to_back, vr.at[1, e0 + e]).start()

                @pl.when(p != pos)
                def _():
                    rcopy(part_in, to_in, vs.at[0, ep * I], vr.at[0, e0 + e], dev(ii, half * PR + p)).start()
                    rcopy(part_back, to_back, vs.at[1, ep * I], vr.at[1, e0 + e], dev(ii, half * PR + p)).start()

            else:
                to = dev(ii, half * PR + p)
                rcopy(part_in, to_in, vs.at[0, ep * I + di], vr.at[0, e0 + e], to).start()
                rcopy(part_back, to_back, vs.at[1, ep * I + di], vr.at[1, e0 + e], to).start()
        return 0


    early = ED * PR * EARLY // 4
    lax.fori_loop(0, early, weight_grad, 0)
    lax.fori_loop(0, early, give_grad, 0)
    lax.fori_loop(early, ED * PR, weight_grad, 0)

    def back_gone(row, buf, n):
        for dt in range(T):

            def one():
                pltpu.make_async_copy(buf, buf, rs.at[row, n * T + dt]).wait()

            if dt == 0:
                pl.when(n > 0)(one)
            else:
                one()

    ggx = ref["ggx"]
    cacc = ref["cacc"]

    def from_of(n, dt):
        return lax.rem(i + n, I), lax.rem(t - dt + T, T)

    def wait_home(row, view):
        def one(n, _):
            for dt in range(T):
                fi, ft = from_of(n, dt)
                d = view(fi, ft)
                pltpu.make_async_copy(d, d, rr.at[row, n * T + dt]).wait()
            return 0

        lax.fori_loop(0, I, one, 0)

    def slot_view(buf):
        return lambda fi, ft: buf.at[ft // PR, pl.ds((fi * PR + lax.rem(ft, PR)) * ED, ED)]

    wait_home(2, lambda fi, ft: ggr.at[fi * T + ft])
    gg_swap = rcopy(ggr, ggx, xsm.at[1], xrm.at[1], dev(i, t, oh))
    gg_swap.start()
    wait_home(0, slot_view(sir))

    def give_eo(n, _):
        give_back(n, 1, eos, eor, False)
        return 0

    lax.fori_loop(0, I, give_eo, 0)


    CH = 256

    def combine(rows, src, weighted):
        c0, c1 = idc[rows, 0:1], idc[rows, 1:2]
        w0 = gcol[rows, 0:1] if weighted else 1.0
        w1 = gcol[rows, 1:2] if weighted else 1.0
        cacc[...] = jnp.zeros_like(cacc)

        def one(c, _):
            lane = iota((OWN, CH), 1) + (c * CH + h * z.slots).astype(F32)
            w = jnp.where(c0 == lane, w0, 0.0) + jnp.where(c1 == lane, w1, 0.0)
            w = w.astype(BF16)
            for a in range(A):
                cacc[...] += mm(w, src[a, pl.ds(c * (CH // CAP), CH // CAP)].reshape(CH, D))
            return 0

        lax.fori_loop(0, z.slots // CH, one, 0)

    dbs, dbr = ref["dbs"], ref["dbr"]
    combine(other_rows, sir, False)
    dbs[...] = cacc[...].astype(BF16)
    db_swap = rcopy(dbs, dbr, xsm.at[2], xrm.at[2], dev(i, t, oh))
    db_swap.start()
    combine(mine_rows, sir, False)

    lane_own = iota((OWN, LANES), 1)
    m0, m1 = rp[mine_rows, 0:1], rp[mine_rows, 1:2]
    gg_swap.wait_recv()
    ggacc = ref["ggacc"]
    ggacc[...] = jnp.zeros_like(ggacc)

    def gate_back(q, _):
        fi, pp = q // PR, lax.rem(q, PR)
        k0, k1 = idc[mine_rows, 0:1], idc[mine_rows, 1:2]
        for buf, hh in ((ggr, h), (ggx, oh)):
            line = buf[fi * T + pp][0:1, :]
            for a in range(1, A):
                line = line + buf[fi * T + a * PR + pp][0:1, :]
            lane = lane_own + (q * z.lw + hh * z.slots).astype(F32)
            keep = lane_own < z.lw
            ggacc[0] += jnp.where(jnp.logical_and(keep, k0 == lane), line, 0.0)
            ggacc[1] += jnp.where(jnp.logical_and(keep, k1 == lane), line, 0.0)
        return 0

    lax.fori_loop(0, z.home // ED, gate_back, 0)
    gg0 = jnp.sum(ggacc[0], axis=1, keepdims=True)
    gg1 = jnp.sum(ggacc[1], axis=1, keepdims=True)
    mrouter = router[mine_rows, :]
    pgrad = jnp.where(m0 == lane_own, gg0, 0.0) + jnp.where(m1 == lane_own, gg1, 0.0)
    lgrad = (mrouter * (pgrad - jnp.sum(pgrad * mrouter, axis=1, keepdims=True))).astype(BF16)
    xn2 = xn2a[mine_rows, :]
    small = ref["small"]
    small[...] = jnp.where(iota((D, LANES), 1) < EXPERTS, mm_tn(xn2, lgrad), 0.0)
    through = mm_nt(lgrad, sall[...])
    db_swap.wait_recv()
    xgrad = cacc[...] + dbr[...].astype(F32) + through
    normed, spread_two = norm_of(resid[...])
    nrows = ref["nrows"]
    nrows[...] = jnp.zeros_like(nrows)
    nrows[EXPERTS + 1 : EXPERTS + 2, :] = jnp.sum(xgrad * normed, axis=0, keepdims=True)
    rgrad = ref["rgrad"]
    rgrad[...] = cota[mine_rows, :].astype(F32) + norm_back(xgrad * gains[1:2, :], normed, spread_two)

    agrad = rgrad[...].astype(BF16)

    def gw(j, row, count):
        return (0, pl.ds(al((j // 2) * D + row, LANES), count), pl.ds(al(lax.rem(j, 2) * D, LANES), D))

    hid[gw(jnp.int32(3), 0, D)] = mm_tn(agrad, mixed[...]).astype(BF16)
    mg = ref["mg"]
    mg[...] = mm(agrad, wall[3]).astype(BF16)
    pg = ref["pg"]

    def attend_back(n, _):
        rows = pl.ds(al((n // groups) * RP, 16), RP)
        cols = pl.ds(al(lax.rem(n, groups) * LANES, LANES), LANES)
        q, kk, v = qkv[0, rows, cols], qkv[1, rows, cols], qkv[2, rows, cols]
        m = mg[rows, cols]
        low = iota((RP, LANES), 1) < HD
        dq, dk, dv = [], [], []
        for s in range(2):
            sel = low if s == 0 else jnp.logical_not(low)
            low_p = probs[n * 2 + s]
            p = low_p.astype(F32)
            dp = mm_nt(jnp.where(sel, m, jnp.zeros_like(m)), v)
            dv.append(mm_tn(low_p, m))
            sg = (p * (dp - jnp.sum(dp * p, axis=-1, keepdims=True))).astype(BF16)
            dq.append(mm(sg, kk))
            dk.append(mm_tn(sg, q))
        pg[0, rows, cols] = (jnp.where(low, dq[0], dq[1]) * scale).astype(BF16)
        pg[1, rows, cols] = (jnp.where(low, dk[0], dk[1]) * scale).astype(BF16)
        pg[2, rows, cols] = jnp.where(low, dv[0], dv[1]).astype(BF16)
        return 0

    lax.fori_loop(0, z.own_img * groups, attend_back, 0)
    cacc[...] = jnp.zeros_like(cacc)

    def project_back(j, _):
        hid[gw(j, 0, D)] = mm_tn(xn1[...], pg[j]).astype(BF16)
        cacc[...] += mm_nt(pg[j], wall[j])
        return 0

    lax.fori_loop(0, 3, project_back, 0)

    s1r, s2s, s2r, s3s, s3r, s4s, s4r = (ref[n] for n in ("s1r", "s2s", "s2r", "s3s", "s3r", "s4s", "s4r"))
    u1s, u1r, u3s, u3r, u4s, u4r, u5s, u5r = (ref[n] for n in ("u1s", "u1r", "u3s", "u3r", "u4s", "u4r", "u5s", "u5r"))
    qs, qr = ref["qs"], ref["qr"]

    def quarter(ii):
        return pl.ds(al(ii * DQ, DQ), DQ)

    sw1 = []
    for b, ii in enumerate((i_core, i_diag)):
        for jr in range(2):
            src = hid.at[0, pl.ds(al(jr * D + ii * DQ, LANES), DQ), pl.ds(0, 2 * D)]
            sw1.append(rcopy(src, s1r.at[jr, b], qs.at[13 + 2 * b + jr], qr.at[13 + 2 * b + jr], dev(i_core, t)))
    for c in sw1:
        c.start()

    normed, spread_one = norm_of(xs[...])
    nrows[EXPERTS : EXPERTS + 1, :] = jnp.sum(cacc[...] * normed, axis=0, keepdims=True)
    tgrad = rgrad[...] + norm_back(cacc[...] * gains[0:1, :], normed, spread_one)
    tgs, tgr = ref["tgs"], ref["tgr"]
    tgs[...] = tgrad.astype(BF16)
    small[...] = small[...] + jnp.transpose(nrows[...])
    for b, ii in enumerate((i_core, i_diag)):
        u1s[b] = small[quarter(ii), :]
    sv1 = rcopy(u1s, u1r, qs.at[1], qr.at[1], dev(i_core, t))
    sv1.start()
    for c in sw1:
        c.wait_recv()
    sv1.wait_recv()
    accu, acc2 = ref["accu"], ref["acc2"]
    for b, ii in enumerate((i, i_far)):
        for j in range(4):
            for hh, keep in ((oh, False), (h, True)):
                cols = pl.ds(al((j % 2) * D + hh * EC, LANES), EC)
                here = hid[0, pl.ds(al((j // 2) * D + ii * DQ, LANES), DQ), cols].astype(F32)
                here = here + s1r[j // 2, b, :, cols].astype(F32)
                if keep:
                    acc2[j, b] = here
                else:
                    s2s[j, b] = here.astype(BF16)
        accu[b] = small[quarter(ii), :] + u1r[b]
    sw2 = rcopy(s2s, s2r, qs.at[2], qr.at[2], dev(i, t, oh))
    sw2.start()
    t_swap = rcopy(tgs, tgr, xsm.at[3], xrm.at[3], dev(i, t, oh))
    t_swap.start()
    u3s[...] = accu[1]
    sv3 = rcopy(u3s, u3r, qs.at[3], qr.at[3], dev(i_far, t))
    sv3.start()

    sw2.wait_recv()
    acc2[...] = acc2[...] + s2r[...].astype(F32)
    s3s[...] = acc2[:, 1].astype(BF16)
    sw3 = rcopy(s3s, s3r, qs.at[4], qr.at[4], dev(i_far, t))
    sw3.start()
    sw3.wait_recv()
    sv3.wait_recv()
    accu[0] = accu[0] + u3r[...]
    u4s[...] = accu[0]
    acc2[:, 0] = acc2[:, 0] + s3r[...].astype(F32)
    s4s[...] = acc2[:, 0].astype(BF16)
    last = []
    for dt in range(1, T):
        tt = lax.rem(t + dt, T)
        rows = pl.ds(al(tt * WR, WR), WR)
        last.append(rcopy(s4s.at[:, rows, :], s4r.at[dt], qs.at[4 + 2 * dt], qr.at[4 + 2 * dt], dev(i, tt)))
        last.append(rcopy(u4s.at[rows, :], u4r.at[dt], qs.at[5 + 2 * dt], qr.at[5 + 2 * dt], dev(i, tt)))
    for c in last:
        c.start()
    lax.fori_loop(early, ED * PR, give_grad, 0)

    out_o, tg_o = ref["out_o"], ref["tg_o"]
    mos, mor, outs, outr = ref["mos"], ref["mor"], ref["outs"], ref["outr"]
    wait_home(1, slot_view(eor))
    combine(other_rows, eor, True)
    mos[...] = cacc[...].astype(BF16)
    m_swap = rcopy(mos, mor, xsm.at[4], xrm.at[4], dev(i, t, oh))
    m_swap.start()
    combine(mine_rows, eor, True)
    m_swap.wait_recv()
    outs[...] = (resid[...] + cacc[...] + mor[...].astype(F32)).astype(BF16)
    o_swap = rcopy(outs, outr, xsm.at[5], xrm.at[5], dev(i, t, oh))
    o_swap.start()
    for m in range(z.own_img):
        out_o[h * z.own_img + m] = outs[pl.ds(m * RP, L), :]
        tg_o[h * z.own_img + m] = tgs[pl.ds(m * RP, L), :]
    for c in last:
        c.wait_recv()
    wfin, sfin = ref["wfin"], ref["sfin"]
    my_rows = pl.ds(al(t * WR, WR), WR)
    total = acc2[:, 0, my_rows, :]
    part = accu[0, my_rows, :]
    for dt in range(1, T):
        total = total + s4r[dt].astype(F32)
        part = part + u4r[dt]
    wfin[...] = total
    u5s[...] = part
    sv5 = rcopy(u5s, u5r, qs.at[12], qr.at[12], dev(i, t, oh))
    sv5.start()
    t_swap.wait_recv()
    o_swap.wait_recv()
    for m in range(z.own_img):
        out_o[oh * z.own_img + m] = outr[pl.ds(m * RP, L), :]
        tg_o[oh * z.own_img + m] = tgr[pl.ds(m * RP, L), :]
    sv5.wait_recv()
    sfin[...] = u5s[...] + u5r[...]

    def grads_in(e, _):
        pltpu.make_async_copy(ing.at[e], ing.at[e], vr.at[0, e]).wait()
        pltpu.make_async_copy(backg.at[e], backg.at[e], vr.at[1, e]).wait()
        return 0

    lax.fori_loop(0, z.home, grads_in, 0)

    def grads_out(ep, _):
        p = lax.rem(ep, PR)
        for di in range(I):
            a_in = vin.at[0, pl.ds(0, DQ), pl.ds(0, FS)]
            a_back = vback.at[0, pl.ds(0, FS), pl.ds(0, DQ)]
            if di == 0:

                @pl.when(p != pos)
                def _():
                    pltpu.make_async_copy(a_in, a_in, vs.at[0, ep * I]).wait()
                    pltpu.make_async_copy(a_back, a_back, vs.at[1, ep * I]).wait()

            else:
                pltpu.make_async_copy(a_in, a_in, vs.at[0, ep * I + di]).wait()
                pltpu.make_async_copy(a_back, a_back, vs.at[1, ep * I + di]).wait()
        return 0

    lax.fori_loop(0, ED * PR, grads_out, 0)

    def back_out(n, _):
        back_gone(0, sis.at[:, 0], n)
        back_gone(1, eos.at[:, 0], n)
        back_gone(2, ggs.at[0], n)
        return 0

    lax.fori_loop(0, I, back_out, 0)
    for c in g_moved[1:] + x_moved[1:] + gate_moved[1:]:
        c.wait_send()
    for c in first + [b_x, b_y, b_ys, b_c, b_cs, f_x, f_c, f_cs, f_c2, f_c3]:
        c.wait_send()
    for c in (x_swap, gg_swap, db_swap, t_swap, m_swap, o_swap, *sw1, sv1, sw2, sv3, sw3, sv5, *last):
        c.wait_send()


def call(z, tok, cot, rt, wpack, spack, win, wback):
    T, I, PR, A, ED, D = z.tensor, z.team_i, z.pair, z.halves, z.own_e, z.width
    OWN, ROWS, EC, DQ, WR = z.own, z.rows, z.ecols, z.dq, z.wrow
    team = z.team
    V, S = pltpu.VMEM, pltpu.SemaphoreType.DMA
    ins = ["tok", "cot", "rt", "wpack", "spack", "win", "wback"]
    outs = {
        "out_o": jax.ShapeDtypeStruct(tok.shape, BF16),
        "tg_o": jax.ShapeDtypeStruct(tok.shape, BF16),
        "wfin": jax.ShapeDtypeStruct((4, WR, EC), F32),
        "sfin": jax.ShapeDtypeStruct((WR, LANES), F32),
        "ing": jax.ShapeDtypeStruct(win.shape, BF16),
        "backg": jax.ShapeDtypeStruct(wback.shape, BF16),
    }
    heads_own = z.own_img * z.nh
    scratch = {
        "wall": V((4, D, D), BF16), "sall": V((D, LANES), BF16), "gains": V((8, D), F32),
        "xn2a": V((ROWS, D), BF16), "cota": V((ROWS, D), BF16), "rp": V((ROWS, LANES), F32),
        "xs": V((OWN, D), F32), "both": V((ROWS, LANES), BF16), "idc": V((ROWS, LANES), F32),
        "idr": V((LANES, ROWS), F32), "grow": V((LANES, ROWS), F32), "gs": V((z.home, CAP, D), BF16), "xsl": V((z.home, CAP, D), BF16),
        "vin": V((ED, D, z.ff), BF16), "vback": V((ED, z.ff, D), BF16),
        "xr": V((ED, team, CAP, D), BF16), "gr": V((ED, team, CAP, D), BF16), "gater": V((team, 8, LANES), F32),
        "xn1": V((OWN, D), BF16), "qkv": V((3, OWN, D), BF16), "mixed": V((OWN, D), BF16),
        "probs": V((heads_own, z.pad, z.pad), BF16), "resid": V((OWN, D), F32), "router": V((ROWS, LANES), F32),
        "gcol": V((ROWS, LANES), F32), "gsend": V((z.home // ED, 8, LANES), F32),
        "hid": V((ED, team * CAP, z.ff), BF16), "igs": V((ED, team * CAP, z.ff), BF16),
        "eoa": V((T * CAP, D), F32), "sia": V((T * CAP, D), F32),
        "eos": V((ED, team, CAP, D), BF16), "sis": V((ED, team, CAP, D), BF16), "ggs": V((team, 8, LANES), F32),
        "eor": V((A, z.home, CAP, D), BF16), "sir": V((A, z.home, CAP, D), BF16), "ggr": V((team, 8, LANES), F32),
        "gcols": V((T, LANES, LANES), F32), "gtile": V((T * CAP, D), BF16),
        "ggx": V((team, 8, LANES), F32), "cacc": V((OWN, D), F32), "dbs": V((OWN, D), BF16), "dbr": V((OWN, D), BF16),
        "ggacc": V((2, OWN, LANES), F32), "small": V((D, LANES), F32), "nrows": V((LANES, D), F32),
        "rgrad": V((OWN, D), F32), "mg": V((OWN, D), BF16), "pg": V((3, OWN, D), BF16),
        "s1r": V((2, 2, DQ, 2 * D), BF16),
        "s2s": V((4, 2, DQ, EC), BF16), "s2r": V((4, 2, DQ, EC), BF16),
        "s3s": V((4, DQ, EC), BF16), "s3r": V((4, DQ, EC), BF16),
        "s4s": V((4, DQ, EC), BF16), "s4r": V((T, 4, WR, EC), BF16),
        "u1s": V((2, DQ, LANES), F32), "u1r": V((2, DQ, LANES), F32),
        "u3s": V((DQ, LANES), F32), "u3r": V((DQ, LANES), F32),
        "u4s": V((DQ, LANES), F32), "u4r": V((T, WR, LANES), F32),
        "u5s": V((WR, LANES), F32), "u5r": V((WR, LANES), F32),
        "accu": V((2, DQ, LANES), F32), "acc2": V((4, 2, DQ, EC), F32),
        "tgs": V((OWN, D), BF16), "tgr": V((OWN, D), BF16), "mos": V((OWN, D), BF16), "mor": V((OWN, D), BF16),
        "outs": V((OWN, D), BF16), "outr": V((OWN, D), BF16),
        "ws": S((5, 4)), "wr": S((5, 4)), "wl": S((2,)), "es": S((2, I * PR)), "er": S((2, I * PR)),
        "ds": S((3, team)), "dr": S((3, team)), "rs": S((3, team)), "rr": S((3, team)),
        "vs": S((2, ED * PR * I)), "vr": S((2, z.home)), "xsm": S((6,)), "xrm": S((6,)), "qs": S((20,)), "qr": S((20,)),
    }
    vmem = pl.BlockSpec(memory_space=pltpu.VMEM)
    anyw = pl.BlockSpec(memory_space=pl.ANY)
    names = ins + list(outs) + list(scratch)
    return pl.pallas_call(
        functools.partial(kernel, z, names),
        out_shape=tuple(outs.values()),
        in_specs=[vmem] * 5 + [anyw] * 2,
        out_specs=(vmem,) * 4 + (anyw,) * 2,
        scratch_shapes=list(scratch.values()),
        compiler_params=pltpu.CompilerParams(collective_id=0, has_side_effects=True, vmem_limit_bytes=64 * 1024 * 1024 - 65536),
        name="block",
    )(tok, cot, rt, wpack, spack, win, wback)


def solution(mesh):
    def local(tokens, cotangent, w_qkv, w_out, w_router, norm_one, norm_two, w_in, w_back, routes):
        images, length, width = tokens.shape
        z = Sizes(mesh.shape, images, length, width, w_in.shape[0], w_in.shape[2])
        R = z.reps
        wpack = jnp.concatenate([w_qkv, jnp.transpose(w_out)[None]], axis=0)
        fill = jnp.zeros((w_router.shape[0], LANES - EXPERTS - 2), BF16)
        spack = jnp.concatenate([w_router, norm_one[:, None], norm_two[:, None], fill], axis=1)
        sets = None
        if R > 1:
            sets = [[a * R + b for b in range(R)] for a in range(z.team_i)]
            w_in = lax.all_gather(w_in, "fsdp", axis=1, tiled=True, axis_index_groups=sets)
            w_back = lax.all_gather(w_back, "fsdp", axis=2, tiled=True, axis_index_groups=sets)
            place = lax.axis_index("tensor") * z.wrow

            def quarter(w, axis):
                w = lax.all_gather(w, "tensor", axis=axis, tiled=True)
                w = lax.all_gather(w, "fsdp", axis=axis, tiled=True, axis_index_groups=sets)
                return lax.dynamic_slice_in_dim(w, place, z.wrow, axis)

            wpack, spack = quarter(wpack, 1), quarter(spack, 0)
        out, tgrad, wfin, sfin, ing, backg = call(z, tokens, cotangent, routes, wpack, spack, w_in, w_back)
        if R > 1:
            ing = lax.psum_scatter(ing, "fsdp", scatter_dimension=1, tiled=True, axis_index_groups=sets)
            backg = lax.psum_scatter(backg, "fsdp", scatter_dimension=2, tiled=True, axis_index_groups=sets)

            def shard(w, axis):
                w = lax.all_gather(w, "tensor", axis=axis, tiled=True)
                w = lax.psum_scatter(w, "fsdp", scatter_dimension=axis, tiled=True, axis_index_groups=sets)
                rows = w.shape[axis] // z.tensor
                return lax.dynamic_slice_in_dim(w, lax.axis_index("tensor") * rows, rows, axis)

            wfin, sfin = shard(wfin, 1), shard(sfin, 0)
        return (
            out,
            tgrad.astype(F32),
            wfin[:3],
            jnp.transpose(wfin[3]),
            sfin[:, :EXPERTS],
            sfin[:, EXPERTS],
            sfin[:, EXPERTS + 1],
            ing.astype(F32),
            backg.astype(F32),
        )

    rows = P(("fsdp", "tensor"), None, None)
    qkv = P(None, ("fsdp", "tensor"), "heads")
    proj = P("heads", ("fsdp", "tensor"))
    table = P(("fsdp", "tensor"), None)
    gain = P(("fsdp", "tensor"))
    first = P("heads", "fsdp", "tensor")
    second = P("heads", "tensor", "fsdp")
    return jax.shard_map(
        local,
        mesh=mesh,
        in_specs=(rows, rows, qkv, proj, table, gain, gain, first, second, rows),
        out_specs=(rows, rows, qkv, proj, table, gain, gain, first, second),
        check_vma=False,
    )
```

```python
import functools

import jax
import jax.numpy as jnp
from jax import lax
from jax.experimental import pallas as pl
from jax.experimental.pallas import tpu as pltpu
from jax.sharding import PartitionSpec as P

HD = 64
EXPERTS = 32
CAP = 64
PAIR = 2
EARLY = 2
LANES = 128
MESH = pl.DeviceIdType.MESH
F32 = jnp.float32
BF16 = jnp.bfloat16


def mm(a, b):
    return lax.dot_general(a, b, (((1,), (0,)), ((), ())), preferred_element_type=F32)


def mm_nt(a, b):
    return lax.dot_general(a, b, (((1,), (1,)), ((), ())), preferred_element_type=F32)


def mm_tn(a, b):
    return lax.dot_general(a, b, (((0,), (0,)), ((), ())), preferred_element_type=F32)


def iota(shape, dim):
    return lax.broadcasted_iota(jnp.int32, shape, dim).astype(F32)


def norm_of(x):
    centre = x - jnp.mean(x, axis=-1, keepdims=True)
    spread = lax.rsqrt(jnp.mean(centre * centre, axis=-1, keepdims=True) + 1e-06)
    return centre * spread, spread


def norm_back(scaled, normed, spread):
    middle = jnp.mean(scaled, axis=-1, keepdims=True)
    along = jnp.mean(scaled * normed, axis=-1, keepdims=True)
    return spread * (scaled - middle - normed * along)


class Sizes:
    def __init__(self, mesh_shape, images, length, width, home, ff_shard):
        self.tensor = mesh_shape["tensor"]
        self.heads = mesh_shape["heads"]
        self.pair = PAIR if self.tensor % PAIR == 0 else 1
        self.halves = self.tensor // self.pair
        self.team_i = min(mesh_shape["fsdp"], max(1, home // self.tensor))
        self.reps = mesh_shape["fsdp"] // self.team_i
        self.team = self.team_i * self.tensor
        self.home = home
        self.own_e = home // (self.team_i * self.pair)
        self.images = images
        self.length = length
        self.width = width
        self.pad = -(-length // 16) * 16
        self.own_img = images // self.heads
        self.own = self.own_img * self.pad
        self.all = images * self.pad
        self.rows = -(-self.all // LANES) * LANES
        self.ffs = ff_shard
        self.ff = ff_shard * self.pair
        self.slots = home * CAP
        self.dq = width // self.team_i
        self.wrow = self.dq // self.tensor
        self.ecols = width // self.heads
        self.lw = self.own_e * CAP
        self.nh = width // HD


def kernel(z, names, *refs):
    ref = dict(zip(names, refs))
    tok, cot, rt, wqkv, wout = ref["tok"], ref["cot"], ref["rt"], ref["wqkv"], ref["wout"]
    spack = ref["spack"]
    win, wback = ref["win"], ref["wback"]
    T, I, R = z.tensor, z.team_i, z.reps
    D, L, RP = z.width, z.length, z.pad
    OWN, ALL, ROWS = z.own, z.all, z.rows
    PR, A, ED = z.pair, z.halves, z.own_e
    FS, DQ, WR, EC = z.ffs, z.dq, z.wrow, z.ecols

    fs, h, t = lax.axis_index("fsdp"), lax.axis_index("heads"), lax.axis_index("tensor")
    i, r = fs // R, lax.rem(fs, R)
    oh = 1 - h
    pos, half = lax.rem(t, PR), t // PR
    e0 = (i * PR + pos) * ED
    i_core = i + 1 - 2 * lax.rem(i, 2)
    i_far = lax.rem(i + 2, I)
    i_diag = lax.rem(i_core + 2, I)
    mine = i * T + t

    def dev(ii, tt, hh=None):
        return {"fsdp": ii * R + r, "heads": h if hh is None else hh, "tensor": tt}

    def rcopy(src, dst, ssem, rsem, target):
        return pltpu.make_async_remote_copy(
            src_ref=src, dst_ref=dst, send_sem=ssem, recv_sem=rsem, device_id=target, device_id_type=MESH
        )

    def lcopy(src, dst, sem):
        return pltpu.make_async_copy(src, dst, sem)

    def al(v, m):
        return pl.multiple_of(v, m)

    tokv, cotv, ls = ref["tokv"], ref["cotv"], ref["ls"]
    fetched = [lcopy(cot, cotv, ls.at[0]), lcopy(tok, tokv, ls.at[1])]
    for c in fetched:
        c.start()

    turn = iota((WR, WR), 0) == iota((WR, WR), 1)
    spack[...] = jnp.zeros_like(spack)
    spack[:, 0:EXPERTS] = ref["table"][...]
    for k, gain in enumerate((ref["one"], ref["two"])):
        col = jnp.sum(jnp.where(turn, gain[...].astype(F32), 0.0), axis=1, keepdims=True)
        spack[:, EXPERTS + k : EXPERTS + k + 1] = col.astype(BF16)

    bar = pltpu.get_barrier_semaphore()
    for di in range(I):
        for dt in range(T):
            if di or dt:
                pl.semaphore_signal(
                    bar, inc=1, device_id=dev(lax.rem(i + di, I), lax.rem(t + dt, T)), device_id_type=MESH
                )
    pl.semaphore_signal(bar, inc=1, device_id=dev(i, t, oh), device_id_type=MESH)
    pl.semaphore_wait(bar, I * T)

    wall, sall = ref["wall"], ref["sall"]
    ws, wr, wl = ref["ws"], ref["wr"], ref["wl"]

    shard = (pl.ds(al(mine * WR, WR), WR), pl.ds(al(h * EC, LANES), EC))
    qkv_shard, out_shard = wall.at[(pl.ds(0, 3), *shard)], wall.at[(3, *shard)]

    def block(buf, ii, hh):
        return buf.at[:, pl.ds(al(ii * DQ, DQ), DQ), pl.ds(al(hh * EC, LANES), EC)]

    def srows(ii):
        return sall.at[pl.ds(al(ii * DQ, DQ), DQ)]

    s_mine = sall.at[pl.ds(al(mine * WR, WR), WR)]
    first = []
    for dt in range(1, T):
        to = dev(i, lax.rem(t + dt, T))
        first.append(rcopy(wqkv, qkv_shard, ws.at[0, dt], wr.at[0, dt], to))
        first.append(rcopy(wout, out_shard, ws.at[5, dt], wr.at[5, dt], to))
        first.append(rcopy(spack, s_mine, ws.at[1, dt], wr.at[1, dt], to))
    for c in first:
        c.start()
    own_w = [lcopy(wqkv, qkv_shard, wl.at[0]), lcopy(spack, s_mine, wl.at[1]), lcopy(wout, out_shard, wl.at[2])]
    for c in own_w:
        c.start()

    vin, vback = ref["vin"], ref["vback"]
    es, er = ref["es"], ref["er"]
    moved = []
    for di in range(I):
        for dp in range(PR):
            k = di * PR + dp
            ii, pp = lax.rem(i + di, I), lax.rem(pos + dp, PR)
            them = pl.ds((ii * PR + pp) * ED, ED)
            to_in = vin.at[:, pl.ds(al(i * DQ, DQ), DQ), pl.ds(al(pos * FS, FS), FS)]
            to_back = vback.at[:, pl.ds(al(pos * FS, FS), FS), pl.ds(al(i * DQ, DQ), DQ)]
            if k == 0:
                moved.append(lcopy(win.at[them], to_in, er.at[0, 0]))
                moved.append(lcopy(wback.at[them], to_back, er.at[1, 0]))
            else:
                to = dev(ii, half * PR + pp)
                moved.append(rcopy(win.at[them], to_in, es.at[0, k], er.at[0, k], to))
                moved.append(rcopy(wback.at[them], to_back, es.at[1, k], er.at[1, k], to))
    for c in moved[: 2 * PR]:
        c.start()

    xr, gr, gater = ref["xr"], ref["gr"], ref["gater"]
    ds, dr = ref["ds"], ref["dr"]

    def spread(src, dst, row, whole):
        made = []
        for di in range(I):
            for dt in range(T):
                kk = di * T + dt
                ii, tt = lax.rem(i + di, I), lax.rem(t + dt, T)
                pp = lax.rem(tt, PR)
                if whole:
                    s, d = src.at[ii * PR + pp], dst.at[mine]
                else:
                    s, d = src.at[pl.ds((ii * PR + pp) * ED, ED)], dst.at[:, mine]
                if kk == 0:
                    made.append(lcopy(s, d, dr.at[row, 0]))
                else:
                    made.append(rcopy(s, d, ds.at[row, kk], dr.at[row, kk], dev(ii, tt)))
        for c in made:
            c.start()
        return made

    xn2a, cota, rp = ref["xn2a"], ref["cota"], ref["rp"]
    xn2a[...] = jnp.zeros_like(xn2a)
    cota[...] = jnp.zeros_like(cota)
    rp[...] = jnp.full_like(rp, -1.0)
    xs = ref["xs"]
    xs[...] = jnp.zeros_like(xs)
    rtt = ref["rtt"]
    for m in range(z.images):
        rtt[...] = jnp.full_like(rtt, -1.0)
        rtt[0:2, 0:L] = rt[m].astype(F32)
        rp[pl.ds(m * RP, L), :] = jnp.transpose(rtt[...])[:L, :]
    for c in fetched:
        c.wait()
    for m in range(z.images):
        cota[pl.ds(m * RP, L), :] = cotv[:, m, :]
    for m in range(z.own_img):
        row = tokv[:, m, :].astype(F32)
        for hh in range(1, z.heads):
            row = jnp.where(h == hh, tokv[:, hh * z.own_img + m, :].astype(F32), row)
        xs[pl.ds(m * RP, L), :] = row

    lane_all = iota((ROWS, LANES), 1)
    r0, r1 = rp[:, 0:1], rp[:, 1:2]
    oh0 = jnp.where(r0 == lane_all, 1.0, 0.0)
    oh1 = jnp.where(r1 == lane_all, 1.0, 0.0)
    both = ref["both"]
    both[...] = (oh0 + oh1).astype(BF16)
    idc = ref["idc"]

    def count(c, _):
        at = pl.ds(al(c * LANES, LANES), LANES)
        before = iota((LANES, ROWS), 1) < iota((LANES, ROWS), 0) + (c * LANES).astype(F32)
        counted = mm(jnp.where(before, 1.0, 0.0).astype(BF16), both[...])
        lane = iota((LANES, LANES), 1)
        q0, q1 = rp[at, 0:1], rp[at, 1:2]
        number = counted + lane * CAP
        n0 = jnp.sum(jnp.where(q0 == lane, number, 0.0), axis=1, keepdims=True)
        n1 = jnp.sum(jnp.where(q1 == lane, number, 0.0), axis=1, keepdims=True)
        n0 = jnp.where(q0 < 0.0, -1.0, n0)
        n1 = jnp.where(q1 < 0.0, -1.0, n1)
        idc[at, :] = jnp.where(lane == 0.0, n0, jnp.where(lane == 1.0, n1, -1.0))
        return 0

    lax.fori_loop(0, ROWS // LANES, count, 0)
    idr = ref["idr"]
    idr[...] = jnp.transpose(idc[...])

    gs, xsl = ref["gs"], ref["xsl"]

    gsend = ref["gsend"]

    def dispatch(source, target, gates=None):
        def one(c, _):
            slot = iota((LANES, ROWS), 0) + (c * LANES + h * z.slots).astype(F32)
            in0, in1 = idr[0:1, :] == slot, idr[1:2, :] == slot
            pick = jnp.where(in0, 1.0, 0.0) + jnp.where(in1, 1.0, 0.0)
            got = mm(pick.astype(BF16), source[...]).astype(BF16)
            per = LANES // CAP
            target[pl.ds(c * per, per)] = got.reshape(per, CAP, D)
            if gates is not None:
                w = jnp.where(in0, gates[0:1, :], 0.0) + jnp.where(in1, gates[1:2, :], 0.0)
                col = jnp.broadcast_to(jnp.sum(w, axis=1, keepdims=True), (LANES, LANES))
                sub, lane = iota((LANES, LANES), 0), iota((LANES, LANES), 1)
                for q in range(LANES // z.lw):
                    here = jnp.logical_and(lane < z.lw, lane == sub - q * z.lw)
                    line = jnp.sum(jnp.where(here, col, 0.0), axis=0, keepdims=True)
                    gsend[c * (LANES // z.lw) + q] = jnp.broadcast_to(line, (8, LANES))
            return 0

        lax.fori_loop(0, z.slots // LANES, one, 0)

    for c in first:
        c.wait_recv()
    for c in own_w:
        c.wait()
    b_x = rcopy(block(wall, i, h), block(wall, i, h), ws.at[2, 0], wr.at[2, 0], dev(i, t, oh))
    b_y = rcopy(block(wall, i, h), block(wall, i, h), ws.at[2, 1], wr.at[2, 1], dev(i_far, t))
    b_ys = rcopy(srows(i), srows(i), ws.at[2, 2], wr.at[2, 2], dev(i_far, t))
    b_c = rcopy(block(wall, i, h), block(wall, i, h), ws.at[2, 3], wr.at[2, 3], dev(i_core, t))
    b_cs = rcopy(srows(i), srows(i), ws.at[3, 0], wr.at[3, 0], dev(i_core, t))
    for c in (b_y, b_x, b_ys, b_c, b_cs):
        c.start()
    for c in moved[2 * PR :]:
        c.start()
    dispatch(cota, gs)
    g_moved = spread(gs, gr, 0, False)
    b_y.wait_recv()
    f_x = rcopy(block(wall, i_far, h), block(wall, i_far, h), ws.at[3, 1], wr.at[3, 1], dev(i, t, oh))
    f_x.start()
    f_c = rcopy(block(wall, i_far, h), block(wall, i_far, h), ws.at[3, 2], wr.at[3, 2], dev(i_core, t))
    f_c.start()
    b_ys.wait_recv()
    f_cs = rcopy(srows(i_far), srows(i_far), ws.at[3, 3], wr.at[3, 3], dev(i_core, t))
    f_cs.start()
    b_x.wait_recv()
    f_c2 = rcopy(block(wall, i, oh), block(wall, i, oh), ws.at[4, 0], wr.at[4, 0], dev(i_core, t))
    f_c2.start()

    f_x.wait_recv()
    f_c3 = rcopy(block(wall, i_far, oh), block(wall, i_far, oh), ws.at[4, 1], wr.at[4, 1], dev(i_core, t))
    f_c3.start()
    for c in (b_c, b_cs, f_c, f_cs, f_c2, f_c3):
        c.wait_recv()

    sall_t = jnp.transpose(sall[...].astype(F32))
    gains = ref["gains"]
    gains[...] = sall_t[EXPERTS : EXPERTS + 8, :]
    xn1, qkv, mixed, probs = ref["xn1"], ref["qkv"], ref["mixed"], ref["probs"]
    normed, _ = norm_of(xs[...])
    xn1[...] = (normed * gains[0:1, :]).astype(BF16)

    def project(j, _):
        qkv[j] = mm(xn1[...], wall[j]).astype(BF16)
        return 0

    lax.fori_loop(0, 3, project, 0)
    groups = D // LANES
    scale = HD ** (-0.5)

    def attend(n, _):
        rows = pl.ds(al((n // groups) * RP, 16), RP)
        cols = pl.ds(al(lax.rem(n, groups) * LANES, LANES), LANES)
        q, kk, v = qkv[0, rows, cols], qkv[1, rows, cols], qkv[2, rows, cols]
        low = iota((RP, LANES), 1) < HD
        key = iota((RP, RP), 1)
        outs = []
        for s in range(2):
            sel = low if s == 0 else jnp.logical_not(low)
            score = mm_nt(jnp.where(sel, q, jnp.zeros_like(q)), kk) * scale
            score = jnp.where(key < L, score, -1e30)
            e = jnp.exp(score - jnp.max(score, axis=-1, keepdims=True))
            p = e / jnp.sum(e, axis=-1, keepdims=True)
            p = p.astype(BF16)
            probs[n * 2 + s] = p
            outs.append(mm(p, v))
        mixed[rows, cols] = jnp.where(low, outs[0], outs[1]).astype(BF16)
        return 0

    lax.fori_loop(0, z.own_img * groups, attend, 0)
    resid = ref["resid"]
    resid[...] = xs[...] + mm_nt(mixed[...], wall[3])
    normed, _ = norm_of(resid[...])
    mine_rows = pl.ds(al(h * OWN, 16), OWN)
    other_rows = pl.ds(al(oh * OWN, 16), OWN)
    xn2a[mine_rows, :] = (normed * gains[1:2, :]).astype(BF16)

    xsm, xrm = ref["xsm"], ref["xrm"]
    x_swap = rcopy(xn2a.at[mine_rows], xn2a.at[mine_rows], xsm.at[0], xrm.at[0], dev(i, t, oh))
    x_swap.start()
    x_swap.wait_recv()
    logits = mm(xn2a[...], sall[...])
    logits = jnp.where(lane_all < EXPERTS, logits, -1e30)
    e = jnp.exp(logits - jnp.max(logits, axis=-1, keepdims=True))
    router = ref["router"]
    router[...] = e / jnp.sum(e, axis=-1, keepdims=True)
    gcol = ref["gcol"]
    g0 = jnp.sum(jnp.where(rp[:, 0:1] == lane_all, router[...], 0.0), axis=1, keepdims=True)
    g1 = jnp.sum(jnp.where(rp[:, 1:2] == lane_all, router[...], 0.0), axis=1, keepdims=True)
    gcol[...] = jnp.where(lane_all == 0.0, g0, g1)
    grow = ref["grow"]
    grow[...] = jnp.transpose(gcol[...])
    dispatch(xn2a, xsl, grow)
    gate_moved = spread(gsend, gater, 2, True)
    x_moved = spread(xsl, xr, 1, False)

    hid, igs, gtile = ref["hid"], ref["igs"], ref["gtile"]
    eoa, sia = ref["eoa"], ref["sia"]
    eos, sis, ggs = ref["eos"], ref["sis"], ref["ggs"]
    eor, sir, ggr = ref["eor"], ref["sir"], ref["ggr"]
    rs, rr = ref["rs"], ref["rr"]
    gcols = ref["gcols"]
    ggs[...] = jnp.zeros_like(ggs)
    for c in moved:
        c.wait()
    TR = T * CAP
    eye = iota((LANES, LANES), 0) == iota((LANES, LANES), 1)

    def wait_role(row, kk, dst):
        pltpu.make_async_copy(dst, dst, dr.at[row, kk]).wait()

    def tile(n, _):
        gi = lax.rem(i - n + I, I)
        grp = pl.ds(gi * T, T)
        for dt in range(T):
            src = gi * T + lax.rem(t - dt + T, T)
            wait_role(0, n * T + dt, gr.at[:, src])
            wait_role(1, n * T + dt, xr.at[:, src])
            wait_role(2, n * T + dt, gater.at[src])
        for dt in range(T):
            row = gater[gi * T + dt][0:1, :]
            col = jnp.sum(jnp.where(eye, jnp.broadcast_to(row, (LANES, LANES)), 0.0), axis=1, keepdims=True)
            gcols[dt] = jnp.broadcast_to(col, (LANES, LANES))

        def part(ep, _):
            e, p = ep // PR, lax.rem(ep, PR)
            cols = pl.ds(al(p * FS, FS), FS)
            trow = pl.ds(al(gi * TR, TR), TR)
            x = xr[e, grp].reshape(TR, D)

            @pl.when(p == 0)
            def _():
                g = gr[e, grp].reshape(TR, D)
                gtile[...] = g
                gate = gcols[:, pl.ds(al(e * CAP, CAP), CAP), :].reshape(TR, LANES)[:, 0:1]
                gr[e, grp] = (g.astype(F32) * gate).astype(BF16).reshape(T, CAP, D)
                eoa[...] = jnp.zeros_like(eoa)
                sia[...] = jnp.zeros_like(sia)

            inner = mm(x, vin[e, :, cols])
            erf = lax.erf(inner * (0.5**0.5))
            cdf = 0.5 * (1.0 + erf)
            hidden = (inner * cdf).astype(BF16)
            slope = cdf + inner * (jnp.exp(-0.5 * inner * inner) * 0.3989422804014327)
            hid[e, trow, cols] = hidden
            eoa[...] += mm(hidden, vback[e, cols, :])
            back = mm_nt(gr[e, grp].reshape(TR, D), vback[e, cols, :])
            inner_grad = (back * slope).astype(BF16)
            igs[e, trow, cols] = inner_grad
            sia[...] += mm_nt(inner_grad, vin[e, :, cols])

            @pl.when(p == PR - 1)
            def _():
                eo = eoa[...]
                eos[e, grp] = eo.astype(BF16).reshape(T, CAP, D)
                sis[e, grp] = sia[...].astype(BF16).reshape(T, CAP, D)
                gg = jnp.sum(eo * gtile[...].astype(F32), axis=1, keepdims=True)
                there = iota((CAP, LANES), 1) == iota((CAP, LANES), 0) + (e * CAP).astype(F32)
                for dt in range(T):
                    piece = jnp.broadcast_to(gg[dt * CAP : (dt + 1) * CAP], (CAP, LANES))
                    line = jnp.sum(jnp.where(there, piece, 0.0), axis=0, keepdims=True)
                    ggs[gi * T + dt] = ggs[gi * T + dt] + jnp.broadcast_to(line, (8, LANES))

            return 0

        lax.fori_loop(0, ED * PR, part, 0)
        give_back(n, 2, ggs, ggr, True)
        give_back(n, 0, sis, sir, False)
        return 0

    def give_back(n, row, src, dst, whole):
        gi = lax.rem(i - n + I, I)
        for dt in range(T):
            tt = lax.rem(t + dt, T)
            kk = n * T + dt
            if whole:
                s, d = src.at[gi * T + tt], dst.at[mine]
            else:
                s, d = src.at[:, gi * T + tt], dst.at[half, pl.ds(e0, ED)]
            if dt == 0:

                @pl.when(n == 0)
                def _():
                    lcopy(s, d, rr.at[row, kk]).start()

                @pl.when(n > 0)
                def _():
                    rcopy(s, d, rs.at[row, kk], rr.at[row, kk], dev(gi, tt)).start()

            else:
                rcopy(s, d, rs.at[row, kk], rr.at[row, kk], dev(gi, tt)).start()

    lax.fori_loop(0, I, tile, 0)

    ing, backg = ref["ing"], ref["backg"]
    vs, vr = ref["vs"], ref["vr"]

    def weight_grad(ep, _):
        e, p = ep // PR, lax.rem(ep, PR)
        cols = pl.ds(al(p * FS, FS), FS)
        vin[e, :, cols] = mm_tn(xr[e].reshape(z.team * CAP, D), igs[e, :, cols]).astype(BF16)
        vback[e, cols, :] = mm_tn(hid[e, :, cols], gr[e].reshape(z.team * CAP, D)).astype(BF16)
        return 0

    def give_grad(ep, _):
        e, p = ep // PR, lax.rem(ep, PR)
        cols = pl.ds(al(p * FS, FS), FS)
        for di in range(I):
            ii = lax.rem(i + di, I)
            part_in = vin.at[e, pl.ds(al(ii * DQ, DQ), DQ), cols]
            part_back = vback.at[e, cols, pl.ds(al(ii * DQ, DQ), DQ)]
            to_in, to_back = ing.at[e0 + e], backg.at[e0 + e]
            if di == 0:

                @pl.when(p == pos)
                def _():
                    lcopy(part_in, to_in, vr.at[0, e0 + e]).start()
                    lcopy(part_back, to_back, vr.at[1, e0 + e]).start()

                @pl.when(p != pos)
                def _():
                    rcopy(part_in, to_in, vs.at[0, ep * I], vr.at[0, e0 + e], dev(ii, half * PR + p)).start()
                    rcopy(part_back, to_back, vs.at[1, ep * I], vr.at[1, e0 + e], dev(ii, half * PR + p)).start()

            else:
                to = dev(ii, half * PR + p)
                rcopy(part_in, to_in, vs.at[0, ep * I + di], vr.at[0, e0 + e], to).start()
                rcopy(part_back, to_back, vs.at[1, ep * I + di], vr.at[1, e0 + e], to).start()
        return 0


    early = ED * PR * EARLY // 4
    lax.fori_loop(0, early, weight_grad, 0)
    lax.fori_loop(0, early, give_grad, 0)
    lax.fori_loop(early, ED * PR, weight_grad, 0)

    def back_gone(row, buf, n):
        for dt in range(T):

            def one():
                pltpu.make_async_copy(buf, buf, rs.at[row, n * T + dt]).wait()

            if dt == 0:
                pl.when(n > 0)(one)
            else:
                one()

    ggx = ref["ggx"]
    cacc = ref["cacc"]

    def from_of(n, dt):
        return lax.rem(i + n, I), lax.rem(t - dt + T, T)

    def wait_home(row, view):
        def one(n, _):
            for dt in range(T):
                fi, ft = from_of(n, dt)
                d = view(fi, ft)
                pltpu.make_async_copy(d, d, rr.at[row, n * T + dt]).wait()
            return 0

        lax.fori_loop(0, I, one, 0)

    def slot_view(buf):
        return lambda fi, ft: buf.at[ft // PR, pl.ds((fi * PR + lax.rem(ft, PR)) * ED, ED)]

    wait_home(2, lambda fi, ft: ggr.at[fi * T + ft])
    gg_swap = rcopy(ggr, ggx, xsm.at[1], xrm.at[1], dev(i, t, oh))
    gg_swap.start()
    wait_home(0, slot_view(sir))

    def give_eo(n, _):
        give_back(n, 1, eos, eor, False)
        return 0

    lax.fori_loop(0, I, give_eo, 0)


    CH = 256

    def combine(rows, src, weighted):
        c0, c1 = idc[rows, 0:1], idc[rows, 1:2]
        w0 = gcol[rows, 0:1] if weighted else 1.0
        w1 = gcol[rows, 1:2] if weighted else 1.0
        cacc[...] = jnp.zeros_like(cacc)

        def one(c, _):
            lane = iota((OWN, CH), 1) + (c * CH + h * z.slots).astype(F32)
            w = jnp.where(c0 == lane, w0, 0.0) + jnp.where(c1 == lane, w1, 0.0)
            w = w.astype(BF16)
            for a in range(A):
                cacc[...] += mm(w, src[a, pl.ds(c * (CH // CAP), CH // CAP)].reshape(CH, D))
            return 0

        lax.fori_loop(0, z.slots // CH, one, 0)

    dbs, dbr = ref["dbs"], ref["dbr"]
    combine(other_rows, sir, False)
    dbs[...] = cacc[...].astype(BF16)
    db_swap = rcopy(dbs, dbr, xsm.at[2], xrm.at[2], dev(i, t, oh))
    db_swap.start()
    combine(mine_rows, sir, False)

    lane_own = iota((OWN, LANES), 1)
    m0, m1 = rp[mine_rows, 0:1], rp[mine_rows, 1:2]
    gg_swap.wait_recv()
    ggacc = ref["ggacc"]
    ggacc[...] = jnp.zeros_like(ggacc)

    def gate_back(q, _):
        fi, pp = q // PR, lax.rem(q, PR)
        k0, k1 = idc[mine_rows, 0:1], idc[mine_rows, 1:2]
        for buf, hh in ((ggr, h), (ggx, oh)):
            line = buf[fi * T + pp][0:1, :]
            for a in range(1, A):
                line = line + buf[fi * T + a * PR + pp][0:1, :]
            lane = lane_own + (q * z.lw + hh * z.slots).astype(F32)
            keep = lane_own < z.lw
            ggacc[0] += jnp.where(jnp.logical_and(keep, k0 == lane), line, 0.0)
            ggacc[1] += jnp.where(jnp.logical_and(keep, k1 == lane), line, 0.0)
        return 0

    lax.fori_loop(0, z.home // ED, gate_back, 0)
    gg0 = jnp.sum(ggacc[0], axis=1, keepdims=True)
    gg1 = jnp.sum(ggacc[1], axis=1, keepdims=True)
    mrouter = router[mine_rows, :]
    pgrad = jnp.where(m0 == lane_own, gg0, 0.0) + jnp.where(m1 == lane_own, gg1, 0.0)
    lgrad = (mrouter * (pgrad - jnp.sum(pgrad * mrouter, axis=1, keepdims=True))).astype(BF16)
    xn2 = xn2a[mine_rows, :]
    small = ref["small"]
    small[...] = jnp.where(iota((D, LANES), 1) < EXPERTS, mm_tn(xn2, lgrad), 0.0)
    through = mm_nt(lgrad, sall[...])
    db_swap.wait_recv()
    xgrad = cacc[...] + dbr[...].astype(F32) + through
    normed, spread_two = norm_of(resid[...])
    nrows = ref["nrows"]
    nrows[...] = jnp.zeros_like(nrows)
    nrows[EXPERTS + 1 : EXPERTS + 2, :] = jnp.sum(xgrad * normed, axis=0, keepdims=True)
    rgrad = ref["rgrad"]
    rgrad[...] = cota[mine_rows, :].astype(F32) + norm_back(xgrad * gains[1:2, :], normed, spread_two)

    agrad = rgrad[...].astype(BF16)

    def gw(j, row, count):
        return (0, pl.ds(al((j // 2) * D + row, LANES), count), pl.ds(al(lax.rem(j, 2) * D, LANES), D))

    hid[gw(jnp.int32(3), 0, D)] = mm_tn(agrad, mixed[...]).astype(BF16)
    mg = ref["mg"]
    mg[...] = mm(agrad, wall[3]).astype(BF16)
    pg = ref["pg"]

    def attend_back(n, _):
        rows = pl.ds(al((n // groups) * RP, 16), RP)
        cols = pl.ds(al(lax.rem(n, groups) * LANES, LANES), LANES)
        q, kk, v = qkv[0, rows, cols], qkv[1, rows, cols], qkv[2, rows, cols]
        m = mg[rows, cols]
        low = iota((RP, LANES), 1) < HD
        dq, dk, dv = [], [], []
        for s in range(2):
            sel = low if s == 0 else jnp.logical_not(low)
            low_p = probs[n * 2 + s]
            p = low_p.astype(F32)
            dp = mm_nt(jnp.where(sel, m, jnp.zeros_like(m)), v)
            dv.append(mm_tn(low_p, m))
            sg = (p * (dp - jnp.sum(dp * p, axis=-1, keepdims=True))).astype(BF16)
            dq.append(mm(sg, kk))
            dk.append(mm_tn(sg, q))
        pg[0, rows, cols] = (jnp.where(low, dq[0], dq[1]) * scale).astype(BF16)
        pg[1, rows, cols] = (jnp.where(low, dk[0], dk[1]) * scale).astype(BF16)
        pg[2, rows, cols] = jnp.where(low, dv[0], dv[1]).astype(BF16)
        return 0

    lax.fori_loop(0, z.own_img * groups, attend_back, 0)
    cacc[...] = jnp.zeros_like(cacc)

    def project_back(j, _):
        hid[gw(j, 0, D)] = mm_tn(xn1[...], pg[j]).astype(BF16)
        cacc[...] += mm_nt(pg[j], wall[j])
        return 0

    lax.fori_loop(0, 3, project_back, 0)

    s1r, s2s, s2r, s3s, s3r, s4s, s4r = (ref[n] for n in ("s1r", "s2s", "s2r", "s3s", "s3r", "s4s", "s4r"))
    u1s, u1r, u3s, u3r, u4s, u4r, u5s, u5r = (ref[n] for n in ("u1s", "u1r", "u3s", "u3r", "u4s", "u4r", "u5s", "u5r"))
    qs, qr = ref["qs"], ref["qr"]

    def quarter(ii):
        return pl.ds(al(ii * DQ, DQ), DQ)

    sw1 = []
    for b, ii in enumerate((i_core, i_diag)):
        for jr in range(2):
            src = hid.at[0, pl.ds(al(jr * D + ii * DQ, LANES), DQ), pl.ds(0, 2 * D)]
            sw1.append(rcopy(src, s1r.at[jr, b], qs.at[13 + 2 * b + jr], qr.at[13 + 2 * b + jr], dev(i_core, t)))
    for c in sw1:
        c.start()

    normed, spread_one = norm_of(xs[...])
    nrows[EXPERTS : EXPERTS + 1, :] = jnp.sum(cacc[...] * normed, axis=0, keepdims=True)
    tgrad = rgrad[...] + norm_back(cacc[...] * gains[0:1, :], normed, spread_one)
    tgs, tg_p, out_p = ref["tgs"], ref["tg_p"], ref["out_p"]
    tgs[...] = tgrad.astype(BF16)
    small[...] = small[...] + jnp.transpose(nrows[...])
    for b, ii in enumerate((i_core, i_diag)):
        u1s[b] = small[quarter(ii), :]
    sv1 = rcopy(u1s, u1r, qs.at[1], qr.at[1], dev(i_core, t))
    sv1.start()
    for c in sw1:
        c.wait_recv()
    sv1.wait_recv()
    accu, acc2 = ref["accu"], ref["acc2"]
    for b, ii in enumerate((i, i_far)):
        for j in range(4):
            for hh, keep in ((oh, False), (h, True)):
                cols = pl.ds(al((j % 2) * D + hh * EC, LANES), EC)
                here = hid[0, pl.ds(al((j // 2) * D + ii * DQ, LANES), DQ), cols].astype(F32)
                here = here + s1r[j // 2, b, :, cols].astype(F32)
                if keep:
                    acc2[j, b] = here
                else:
                    s2s[j, b] = here.astype(BF16)
        accu[b] = small[quarter(ii), :] + u1r[b]
    sw2 = rcopy(s2s, s2r, qs.at[2], qr.at[2], dev(i, t, oh))
    sw2.start()
    t_swap = rcopy(tgs, tg_p.at[mine_rows], xsm.at[3], xrm.at[3], dev(i, t, oh))
    t_own = lcopy(tgs, tg_p.at[mine_rows], ls.at[2])
    t_swap.start()
    t_own.start()
    u3s[...] = accu[1]
    sv3 = rcopy(u3s, u3r, qs.at[3], qr.at[3], dev(i_far, t))
    sv3.start()

    sw2.wait_recv()
    acc2[...] = acc2[...] + s2r[...].astype(F32)
    s3s[...] = acc2[:, 1].astype(BF16)
    sw3 = rcopy(s3s, s3r, qs.at[4], qr.at[4], dev(i_far, t))
    sw3.start()
    sw3.wait_recv()
    sv3.wait_recv()
    accu[0] = accu[0] + u3r[...]
    u4s[...] = accu[0]
    acc2[:, 0] = acc2[:, 0] + s3r[...].astype(F32)
    s4s[...] = acc2[:, 0].astype(BF16)
    last = []
    for dt in range(1, T):
        tt = lax.rem(t + dt, T)
        rows = pl.ds(al(tt * WR, WR), WR)
        last.append(rcopy(s4s.at[:, rows, :], s4r.at[dt], qs.at[4 + 2 * dt], qr.at[4 + 2 * dt], dev(i, tt)))
        last.append(rcopy(u4s.at[rows, :], u4r.at[dt], qs.at[5 + 2 * dt], qr.at[5 + 2 * dt], dev(i, tt)))
    for c in last:
        c.start()
    lax.fori_loop(early, ED * PR, give_grad, 0)

    mos, mor, outs = ref["mos"], ref["mor"], ref["outs"]
    wait_home(1, slot_view(eor))
    combine(other_rows, eor, True)
    mos[...] = cacc[...].astype(BF16)
    m_swap = rcopy(mos, mor, xsm.at[4], xrm.at[4], dev(i, t, oh))
    m_swap.start()
    combine(mine_rows, eor, True)
    m_swap.wait_recv()
    outs[...] = (resid[...] + cacc[...] + mor[...].astype(F32)).astype(BF16)
    o_swap = rcopy(outs, out_p.at[mine_rows], xsm.at[5], xrm.at[5], dev(i, t, oh))
    o_own = lcopy(outs, out_p.at[mine_rows], ls.at[3])
    o_swap.start()
    o_own.start()
    for c in last:
        c.wait_recv()
    wfin, sfin = ref["wfin"], ref["sfin"]
    my_rows = pl.ds(al(t * WR, WR), WR)
    total = acc2[:, 0, my_rows, :]
    part = accu[0, my_rows, :]
    for dt in range(1, T):
        total = total + s4r[dt].astype(F32)
        part = part + u4r[dt]
    wfs, sfs = ref["wfs"], ref["sfs"]
    wfs[...] = total
    w_own = lcopy(wfs, wfin, ls.at[4])
    w_own.start()
    u5s[...] = part
    sv5 = rcopy(u5s, u5r, qs.at[12], qr.at[12], dev(i, t, oh))
    sv5.start()
    t_swap.wait_recv()
    o_swap.wait_recv()
    t_own.wait()
    o_own.wait()
    sv5.wait_recv()
    sfs[...] = u5s[...] + u5r[...]
    s_own = lcopy(sfs, sfin, ls.at[5])
    s_own.start()

    def grads_in(e, _):
        pltpu.make_async_copy(ing.at[e], ing.at[e], vr.at[0, e]).wait()
        pltpu.make_async_copy(backg.at[e], backg.at[e], vr.at[1, e]).wait()
        return 0

    lax.fori_loop(0, z.home, grads_in, 0)

    def grads_out(ep, _):
        p = lax.rem(ep, PR)
        for di in range(I):
            a_in = vin.at[0, pl.ds(0, DQ), pl.ds(0, FS)]
            a_back = vback.at[0, pl.ds(0, FS), pl.ds(0, DQ)]
            if di == 0:

                @pl.when(p != pos)
                def _():
                    pltpu.make_async_copy(a_in, a_in, vs.at[0, ep * I]).wait()
                    pltpu.make_async_copy(a_back, a_back, vs.at[1, ep * I]).wait()

            else:
                pltpu.make_async_copy(a_in, a_in, vs.at[0, ep * I + di]).wait()
                pltpu.make_async_copy(a_back, a_back, vs.at[1, ep * I + di]).wait()
        return 0

    lax.fori_loop(0, ED * PR, grads_out, 0)

    def back_out(n, _):
        back_gone(0, sis.at[:, 0], n)
        back_gone(1, eos.at[:, 0], n)
        back_gone(2, ggs.at[0], n)
        return 0

    lax.fori_loop(0, I, back_out, 0)
    w_own.wait()
    s_own.wait()
    for c in g_moved[1:] + x_moved[1:] + gate_moved[1:]:
        c.wait_send()
    for c in first + [b_x, b_y, b_ys, b_c, b_cs, f_x, f_c, f_cs, f_c2, f_c3]:
        c.wait_send()
    for c in (x_swap, gg_swap, db_swap, t_swap, m_swap, o_swap, *sw1, sv1, sw2, sv3, sw3, sv5, *last):
        c.wait_send()


def call(z, tok, cot, rt, wqkv, wout, table, one, two, win, wback):
    T, I, PR, A, ED, D = z.tensor, z.team_i, z.pair, z.halves, z.own_e, z.width
    OWN, ROWS, EC, DQ, WR = z.own, z.rows, z.ecols, z.dq, z.wrow
    team = z.team
    V, S = pltpu.VMEM, pltpu.SemaphoreType.DMA
    ins = ["tok", "cot", "rt", "wqkv", "wout", "table", "one", "two", "win", "wback"]
    outs = {
        "out_p": jax.ShapeDtypeStruct((z.all, D), BF16),
        "tg_p": jax.ShapeDtypeStruct((z.all, D), BF16),
        "wfin": jax.ShapeDtypeStruct((4, WR, EC), F32),
        "sfin": jax.ShapeDtypeStruct((WR, LANES), F32),
        "ing": jax.ShapeDtypeStruct(win.shape, BF16),
        "backg": jax.ShapeDtypeStruct(wback.shape, BF16),
    }
    heads_own = z.own_img * z.nh
    wide = -(-z.length // LANES) * LANES
    scratch = {
        "spack": V((WR, LANES), BF16),
        "wfs": V((4, WR, EC), F32),
        "sfs": V((WR, LANES), F32),
        "tokv": V(tok.shape, BF16),
        "cotv": V(cot.shape, BF16),
        "rtt": V((LANES, wide), F32),
        "ls": S((6,)),
        "wall": V((4, D, D), BF16), "sall": V((D, LANES), BF16), "gains": V((8, D), F32),
        "xn2a": V((ROWS, D), BF16), "cota": V((ROWS, D), BF16), "rp": V((ROWS, LANES), F32),
        "xs": V((OWN, D), F32), "both": V((ROWS, LANES), BF16), "idc": V((ROWS, LANES), F32),
        "idr": V((LANES, ROWS), F32), "grow": V((LANES, ROWS), F32), "gs": V((z.home, CAP, D), BF16), "xsl": V((z.home, CAP, D), BF16),
        "vin": V((ED, D, z.ff), BF16), "vback": V((ED, z.ff, D), BF16),
        "xr": V((ED, team, CAP, D), BF16), "gr": V((ED, team, CAP, D), BF16), "gater": V((team, 8, LANES), F32),
        "xn1": V((OWN, D), BF16), "qkv": V((3, OWN, D), BF16), "mixed": V((OWN, D), BF16),
        "probs": V((heads_own, z.pad, z.pad), BF16), "resid": V((OWN, D), F32), "router": V((ROWS, LANES), F32),
        "gcol": V((ROWS, LANES), F32), "gsend": V((z.home // ED, 8, LANES), F32),
        "hid": V((ED, team * CAP, z.ff), BF16), "igs": V((ED, team * CAP, z.ff), BF16),
        "eoa": V((T * CAP, D), F32), "sia": V((T * CAP, D), F32),
        "eos": V((ED, team, CAP, D), BF16), "sis": V((ED, team, CAP, D), BF16), "ggs": V((team, 8, LANES), F32),
        "eor": V((A, z.home, CAP, D), BF16), "sir": V((A, z.home, CAP, D), BF16), "ggr": V((team, 8, LANES), F32),
        "gcols": V((T, LANES, LANES), F32), "gtile": V((T * CAP, D), BF16),
        "ggx": V((team, 8, LANES), F32), "cacc": V((OWN, D), F32), "dbs": V((OWN, D), BF16), "dbr": V((OWN, D), BF16),
        "ggacc": V((2, OWN, LANES), F32), "small": V((D, LANES), F32), "nrows": V((LANES, D), F32),
        "rgrad": V((OWN, D), F32), "mg": V((OWN, D), BF16), "pg": V((3, OWN, D), BF16),
        "s1r": V((2, 2, DQ, 2 * D), BF16),
        "s2s": V((4, 2, DQ, EC), BF16), "s2r": V((4, 2, DQ, EC), BF16),
        "s3s": V((4, DQ, EC), BF16), "s3r": V((4, DQ, EC), BF16),
        "s4s": V((4, DQ, EC), BF16), "s4r": V((T, 4, WR, EC), BF16),
        "u1s": V((2, DQ, LANES), F32), "u1r": V((2, DQ, LANES), F32),
        "u3s": V((DQ, LANES), F32), "u3r": V((DQ, LANES), F32),
        "u4s": V((DQ, LANES), F32), "u4r": V((T, WR, LANES), F32),
        "u5s": V((WR, LANES), F32), "u5r": V((WR, LANES), F32),
        "accu": V((2, DQ, LANES), F32), "acc2": V((4, 2, DQ, EC), F32),
        "tgs": V((OWN, D), BF16),  "mos": V((OWN, D), BF16), "mor": V((OWN, D), BF16),
        "outs": V((OWN, D), BF16),
        "ws": S((6, 4)), "wr": S((6, 4)), "wl": S((3,)), "es": S((2, I * PR)), "er": S((2, I * PR)),
        "ds": S((3, team)), "dr": S((3, team)), "rs": S((3, team)), "rr": S((3, team)),
        "vs": S((2, ED * PR * I)), "vr": S((2, z.home)), "xsm": S((6,)), "xrm": S((6,)), "qs": S((20,)), "qr": S((20,)),
    }
    vmem = pl.BlockSpec(memory_space=pltpu.VMEM)
    anyw = pl.BlockSpec(memory_space=pl.ANY)
    names = ins + list(outs) + list(scratch)
    return pl.pallas_call(
        functools.partial(kernel, z, names),
        out_shape=tuple(outs.values()),
        in_specs=[anyw] * 2 + [vmem] * 6 + [anyw] * 2,
        out_specs=(anyw,) * 6,
        scratch_shapes=list(scratch.values()),
        compiler_params=pltpu.CompilerParams(collective_id=0, has_side_effects=True, vmem_limit_bytes=64 * 1024 * 1024 - 65536),
        name="block",
    )(tok, cot, rt, wqkv, wout, table, one, two, win, wback)


def finish_kernel(z, out_p, tg_p, wfin, sfin, ing, backg, out, tgrad, qkv, proj, table, one, two, gin, gback, mix):
    gin[...] = ing[...].astype(F32)
    gback[...] = backg[...].astype(F32)

    @pl.when(pl.program_id(0) == 0)
    def _():
        for m in range(z.images):
            mix[:, m, :] = out_p[pl.ds(m * z.pad, z.length), :].astype(F32)
        out[...] = mix[...].astype(BF16)
        qkv[...] = wfin[0:3]
        proj[...] = wfin[3]

    @pl.when(pl.program_id(0) == 1)
    def _():
        for m in range(z.images):
            tgrad[:, m, :] = tg_p[pl.ds(m * z.pad, z.length), :].astype(F32)
        table[...] = sfin[:, 0:EXPERTS]
        n = sfin.shape[0]
        eye = iota((n, n), 0) == iota((n, n), 1)
        for k, target in enumerate((one, two)):
            col = sfin[:, EXPERTS + k : EXPERTS + k + 1]
            target[...] = jnp.sum(jnp.where(eye, col, 0.0), axis=0, keepdims=True)


def finish(z, out_p, tg_p, wfin, sfin, ing, backg):
    steps = 4
    part = z.home // steps
    whole = pl.BlockSpec(memory_space=pltpu.VMEM)

    def cut(a):
        return pl.BlockSpec((part, *a.shape[1:]), lambda n: (n, 0, 0))

    mixed = (z.length, z.images, z.width)
    n = sfin.shape[0]
    outs = (
        jax.ShapeDtypeStruct(mixed, BF16),
        jax.ShapeDtypeStruct(mixed, F32),
        jax.ShapeDtypeStruct((3, *wfin.shape[1:]), F32),
        jax.ShapeDtypeStruct(wfin.shape[1:], F32),
        jax.ShapeDtypeStruct((n, EXPERTS), F32),
        jax.ShapeDtypeStruct((1, n), F32),
        jax.ShapeDtypeStruct((1, n), F32),
        jax.ShapeDtypeStruct(ing.shape, F32),
        jax.ShapeDtypeStruct(backg.shape, F32),
    )
    return pl.pallas_call(
        functools.partial(finish_kernel, z),
        grid=(steps,),
        out_shape=outs,
        in_specs=[whole] * 4 + [cut(ing), cut(backg)],
        out_specs=(whole,) * 7 + (cut(ing), cut(backg)),
        scratch_shapes=[pltpu.VMEM(mixed, F32)],
        compiler_params=pltpu.CompilerParams(vmem_limit_bytes=64 * 1024 * 1024 - 65536),
        name="finish",
    )(out_p, tg_p, wfin, sfin, ing, backg)


def solution(mesh):
    def local(tokens, cotangent, w_qkv, w_out, w_router, norm_one, norm_two, w_in, w_back, routes):
        images, length, width = tokens.shape
        z = Sizes(mesh.shape, images, length, width, w_in.shape[0], w_in.shape[2])
        R = z.reps
        wqkv, wout, table = w_qkv, jnp.transpose(w_out), w_router
        one, two = norm_one, norm_two
        sets = None
        if R > 1:
            sets = [[a * R + b for b in range(R)] for a in range(z.team_i)]
            w_in = lax.all_gather(w_in, "fsdp", axis=1, tiled=True, axis_index_groups=sets)
            w_back = lax.all_gather(w_back, "fsdp", axis=2, tiled=True, axis_index_groups=sets)
            place = lax.axis_index("tensor") * z.wrow

            def quarter(w, axis):
                w = lax.all_gather(w, "tensor", axis=axis, tiled=True)
                w = lax.all_gather(w, "fsdp", axis=axis, tiled=True, axis_index_groups=sets)
                return lax.dynamic_slice_in_dim(w, place, z.wrow, axis)

            wqkv, wout, table = quarter(wqkv, 1), quarter(wout, 0), quarter(table, 0)
            one, two = quarter(one, 0), quarter(two, 0)
        tok, cot = jnp.transpose(tokens, (1, 0, 2)), jnp.transpose(cotangent, (1, 0, 2))
        rt = jnp.transpose(routes, (0, 2, 1))
        out_p, tg_p, wfin, sfin, ing, backg = call(z, tok, cot, rt, wqkv, wout, table, one[None], two[None], w_in, w_back)
        if R > 1:
            ing = lax.psum_scatter(ing, "fsdp", scatter_dimension=1, tiled=True, axis_index_groups=sets)
            backg = lax.psum_scatter(backg, "fsdp", scatter_dimension=2, tiled=True, axis_index_groups=sets)

            def shard(w, axis):
                w = lax.all_gather(w, "tensor", axis=axis, tiled=True)
                w = lax.psum_scatter(w, "fsdp", scatter_dimension=axis, tiled=True, axis_index_groups=sets)
                rows = w.shape[axis] // z.tensor
                return lax.dynamic_slice_in_dim(w, lax.axis_index("tensor") * rows, rows, axis)

            wfin, sfin = shard(wfin, 1), shard(sfin, 0)
        out, tgrad, qkv, proj, table, one, two, gin, gback = finish(z, out_p, tg_p, wfin, sfin, ing, backg)
        return (
            jnp.transpose(out, (1, 0, 2)),
            jnp.transpose(tgrad, (1, 0, 2)),
            qkv,
            jnp.transpose(proj),
            table,
            one.reshape(-1),
            two.reshape(-1),
            gin,
            gback,
        )

    rows = P(("fsdp", "tensor"), None, None)
    qkv = P(None, ("fsdp", "tensor"), "heads")
    proj = P("heads", ("fsdp", "tensor"))
    table = P(("fsdp", "tensor"), None)
    gain = P(("fsdp", "tensor"))
    first = P("heads", "fsdp", "tensor")
    second = P("heads", "tensor", "fsdp")
    return jax.shard_map(
        local,
        mesh=mesh,
        in_specs=(rows, rows, qkv, proj, table, gain, gain, first, second, rows),
        out_specs=(rows, rows, qkv, proj, table, gain, gain, first, second),
        check_vma=False,
    )
```

```python
import functools

import jax
import jax.numpy as jnp
from jax import lax
from jax.experimental import pallas as pl
from jax.experimental.pallas import tpu as pltpu
from jax.sharding import PartitionSpec as P

HD = 64
EXPERTS = 32
CAP = 64
PAIR = 2
EARLY = 2
LANES = 128
MESH = pl.DeviceIdType.MESH
F32 = jnp.float32
BF16 = jnp.bfloat16


def mm(a, b):
    return lax.dot_general(a, b, (((1,), (0,)), ((), ())), preferred_element_type=F32)


def mm_nt(a, b):
    return lax.dot_general(a, b, (((1,), (1,)), ((), ())), preferred_element_type=F32)


def mm_tn(a, b):
    return lax.dot_general(a, b, (((0,), (0,)), ((), ())), preferred_element_type=F32)


def iota(shape, dim):
    return lax.broadcasted_iota(jnp.int32, shape, dim).astype(F32)


def norm_of(x):
    centre = x - jnp.mean(x, axis=-1, keepdims=True)
    spread = lax.rsqrt(jnp.mean(centre * centre, axis=-1, keepdims=True) + 1e-06)
    return centre * spread, spread


def norm_back(scaled, normed, spread):
    middle = jnp.mean(scaled, axis=-1, keepdims=True)
    along = jnp.mean(scaled * normed, axis=-1, keepdims=True)
    return spread * (scaled - middle - normed * along)


class Sizes:
    def __init__(self, mesh_shape, images, length, width, home, ff_shard):
        self.tensor = mesh_shape["tensor"]
        self.heads = mesh_shape["heads"]
        self.pair = PAIR if self.tensor % PAIR == 0 else 1
        self.halves = self.tensor // self.pair
        self.team_i = min(mesh_shape["fsdp"], max(1, home // self.tensor))
        self.reps = mesh_shape["fsdp"] // self.team_i
        self.team = self.team_i * self.tensor
        self.home = home
        self.own_e = home // (self.team_i * self.pair)
        self.images = images
        self.length = length
        self.width = width
        self.pad = -(-length // 16) * 16
        self.own_img = images // self.heads
        self.own = self.own_img * self.pad
        self.all = images * self.pad
        self.rows = -(-self.all // LANES) * LANES
        self.ffs = ff_shard
        self.ff = ff_shard * self.pair
        self.slots = home * CAP
        self.dq = width // self.team_i
        self.wrow = self.dq // self.tensor
        self.ecols = width // self.heads
        self.lw = self.own_e * CAP
        self.nh = width // HD


def kernel(z, names, *refs):
    ref = dict(zip(names, refs))
    tok, cot, rt, wqkv, wout = ref["tok"], ref["cot"], ref["rt"], ref["wqkv"], ref["wout"]
    spack = ref["spack"]
    win, wback = ref["win"], ref["wback"]
    T, I, R = z.tensor, z.team_i, z.reps
    D, L, RP = z.width, z.length, z.pad
    OWN, ALL, ROWS = z.own, z.all, z.rows
    PR, A, ED = z.pair, z.halves, z.own_e
    FS, DQ, WR, EC = z.ffs, z.dq, z.wrow, z.ecols

    fs, h, t = lax.axis_index("fsdp"), lax.axis_index("heads"), lax.axis_index("tensor")
    i, r = fs // R, lax.rem(fs, R)
    oh = 1 - h
    pos, half = lax.rem(t, PR), t // PR
    e0 = (i * PR + pos) * ED
    CROSS, SAME = tuple(range(PR, T)), tuple(range(PR - 1, -1, -1))
    i_core = i + 1 - 2 * lax.rem(i, 2)
    i_far = lax.rem(i + 2, I)
    i_diag = lax.rem(i_core + 2, I)
    mine = i * T + t

    def dev(ii, tt, hh=None):
        return {"fsdp": ii * R + r, "heads": h if hh is None else hh, "tensor": tt}

    def onto(dt):
        return lax.rem(half + dt // PR, A) * PR + lax.rem(pos + dt % PR, PR)

    def whence(dt):
        return lax.rem(half - dt // PR + A, A) * PR + lax.rem(pos - dt % PR + PR, PR)

    def rcopy(src, dst, ssem, rsem, target):
        return pltpu.make_async_remote_copy(
            src_ref=src, dst_ref=dst, send_sem=ssem, recv_sem=rsem, device_id=target, device_id_type=MESH
        )

    def lcopy(src, dst, sem):
        return pltpu.make_async_copy(src, dst, sem)

    def al(v, m):
        return pl.multiple_of(v, m)

    tokv, cotv, ls = ref["tokv"], ref["cotv"], ref["ls"]
    fetched = [lcopy(cot, cotv, ls.at[0]), lcopy(tok, tokv, ls.at[1])]
    for c in fetched:
        c.start()

    turn = iota((WR, WR), 0) == iota((WR, WR), 1)
    spack[...] = jnp.zeros_like(spack)
    spack[:, 0:EXPERTS] = ref["table"][...]
    for k, gain in enumerate((ref["one"], ref["two"])):
        col = jnp.sum(jnp.where(turn, gain[...].astype(F32), 0.0), axis=1, keepdims=True)
        spack[:, EXPERTS + k : EXPERTS + k + 1] = col.astype(BF16)

    bar = pltpu.get_barrier_semaphore()
    for di in range(I):
        for dt in range(T):
            if di or dt:
                pl.semaphore_signal(
                    bar, inc=1, device_id=dev(lax.rem(i + di, I), lax.rem(t + dt, T)), device_id_type=MESH
                )
    pl.semaphore_signal(bar, inc=1, device_id=dev(i, t, oh), device_id_type=MESH)
    pl.semaphore_wait(bar, I * T)

    wall, sall = ref["wall"], ref["sall"]
    ws, wr, wl = ref["ws"], ref["wr"], ref["wl"]

    shard = (pl.ds(al(mine * WR, WR), WR), pl.ds(al(h * EC, LANES), EC))
    qkv_shard, out_shard = wall.at[(pl.ds(0, 3), *shard)], wall.at[(3, *shard)]

    def block(buf, ii, hh):
        return buf.at[:, pl.ds(al(ii * DQ, DQ), DQ), pl.ds(al(hh * EC, LANES), EC)]

    def srows(ii):
        return sall.at[pl.ds(al(ii * DQ, DQ), DQ)]

    s_mine = sall.at[pl.ds(al(mine * WR, WR), WR)]
    first = []
    for dt in range(1, T):
        to = dev(i, lax.rem(t + dt, T))
        first.append(rcopy(wqkv, qkv_shard, ws.at[0, dt], wr.at[0, dt], to))
        first.append(rcopy(wout, out_shard, ws.at[5, dt], wr.at[5, dt], to))
        first.append(rcopy(spack, s_mine, ws.at[1, dt], wr.at[1, dt], to))
    for c in first:
        c.start()
    own_w = [lcopy(wqkv, qkv_shard, wl.at[0]), lcopy(spack, s_mine, wl.at[1]), lcopy(wout, out_shard, wl.at[2])]
    for c in own_w:
        c.start()

    vin, vback = ref["vin"], ref["vback"]
    es, er = ref["es"], ref["er"]
    moved = []
    for di in range(I):
        for dp in range(PR):
            k = di * PR + dp
            ii, pp = lax.rem(i + di, I), lax.rem(pos + dp, PR)
            them = pl.ds((ii * PR + pp) * ED, ED)
            to_in = vin.at[:, pl.ds(al(i * DQ, DQ), DQ), pl.ds(al(pos * FS, FS), FS)]
            to_back = vback.at[:, pl.ds(al(pos * FS, FS), FS), pl.ds(al(i * DQ, DQ), DQ)]
            if k == 0:
                moved.append(lcopy(win.at[them], to_in, er.at[0, 0]))
                moved.append(lcopy(wback.at[them], to_back, er.at[1, 0]))
            else:
                to = dev(ii, half * PR + pp)
                moved.append(rcopy(win.at[them], to_in, es.at[0, k], er.at[0, k], to))
                moved.append(rcopy(wback.at[them], to_back, es.at[1, k], er.at[1, k], to))
    for c in moved[: 2 * PR]:
        c.start()

    xr, gr, gater = ref["xr"], ref["gr"], ref["gater"]
    ds, dr = ref["ds"], ref["dr"]

    def spread(src, dst, row, whole, dts):
        made = []
        for di in range(I):
            for dt in dts:
                kk = di * T + dt
                ii, tt = lax.rem(i + di, I), onto(dt)
                pp = lax.rem(tt, PR)
                if whole:
                    s, d = src.at[ii * PR + pp], dst.at[mine]
                else:
                    s, d = src.at[pl.ds((ii * PR + pp) * ED, ED)], dst.at[:, mine]
                if kk == 0:
                    made.append(lcopy(s, d, dr.at[row, 0]))
                else:
                    made.append(rcopy(s, d, ds.at[row, kk], dr.at[row, kk], dev(ii, tt)))
        for c in made:
            c.start()
        return made

    xn2a, cota, rp = ref["xn2a"], ref["cota"], ref["rp"]
    xn2a[...] = jnp.zeros_like(xn2a)
    cota[...] = jnp.zeros_like(cota)
    rp[...] = jnp.full_like(rp, -1.0)
    xs = ref["xs"]
    xs[...] = jnp.zeros_like(xs)
    rtt = ref["rtt"]
    for m in range(z.images):
        rtt[...] = jnp.full_like(rtt, -1.0)
        rtt[0:2, 0:L] = rt[m].astype(F32)
        rp[pl.ds(m * RP, L), :] = jnp.transpose(rtt[...])[:L, :]
    for c in fetched:
        c.wait()
    for m in range(z.images):
        cota[pl.ds(m * RP, L), :] = cotv[:, m, :]
    for m in range(z.own_img):
        row = tokv[:, m, :].astype(F32)
        for hh in range(1, z.heads):
            row = jnp.where(h == hh, tokv[:, hh * z.own_img + m, :].astype(F32), row)
        xs[pl.ds(m * RP, L), :] = row

    lane_all = iota((ROWS, LANES), 1)
    r0, r1 = rp[:, 0:1], rp[:, 1:2]
    oh0 = jnp.where(r0 == lane_all, 1.0, 0.0)
    oh1 = jnp.where(r1 == lane_all, 1.0, 0.0)
    both = ref["both"]
    both[...] = (oh0 + oh1).astype(BF16)
    idc = ref["idc"]

    def count(c, _):
        at = pl.ds(al(c * LANES, LANES), LANES)
        before = iota((LANES, ROWS), 1) < iota((LANES, ROWS), 0) + (c * LANES).astype(F32)
        counted = mm(jnp.where(before, 1.0, 0.0).astype(BF16), both[...])
        lane = iota((LANES, LANES), 1)
        q0, q1 = rp[at, 0:1], rp[at, 1:2]
        number = counted + lane * CAP
        n0 = jnp.sum(jnp.where(q0 == lane, number, 0.0), axis=1, keepdims=True)
        n1 = jnp.sum(jnp.where(q1 == lane, number, 0.0), axis=1, keepdims=True)
        n0 = jnp.where(q0 < 0.0, -1.0, n0)
        n1 = jnp.where(q1 < 0.0, -1.0, n1)
        idc[at, :] = jnp.where(lane == 0.0, n0, jnp.where(lane == 1.0, n1, -1.0))
        return 0

    lax.fori_loop(0, ROWS // LANES, count, 0)
    idr = ref["idr"]
    idr[...] = jnp.transpose(idc[...])

    gs, xsl = ref["gs"], ref["xsl"]

    gsend = ref["gsend"]

    def dispatch(source, target, gates=None):
        def one(c, _):
            slot = iota((LANES, ROWS), 0) + (c * LANES + h * z.slots).astype(F32)
            in0, in1 = idr[0:1, :] == slot, idr[1:2, :] == slot
            pick = jnp.where(in0, 1.0, 0.0) + jnp.where(in1, 1.0, 0.0)
            got = mm(pick.astype(BF16), source[...]).astype(BF16)
            per = LANES // CAP
            target[pl.ds(c * per, per)] = got.reshape(per, CAP, D)
            if gates is not None:
                w = jnp.where(in0, gates[0:1, :], 0.0) + jnp.where(in1, gates[1:2, :], 0.0)
                col = jnp.broadcast_to(jnp.sum(w, axis=1, keepdims=True), (LANES, LANES))
                sub, lane = iota((LANES, LANES), 0), iota((LANES, LANES), 1)
                for q in range(LANES // z.lw):
                    here = jnp.logical_and(lane < z.lw, lane == sub - q * z.lw)
                    line = jnp.sum(jnp.where(here, col, 0.0), axis=0, keepdims=True)
                    gsend[c * (LANES // z.lw) + q] = jnp.broadcast_to(line, (8, LANES))
            return 0

        lax.fori_loop(0, z.slots // LANES, one, 0)

    for c in first:
        c.wait_recv()
    for c in own_w:
        c.wait()
    b_x = rcopy(block(wall, i, h), block(wall, i, h), ws.at[2, 0], wr.at[2, 0], dev(i, t, oh))
    b_y = rcopy(block(wall, i, h), block(wall, i, h), ws.at[2, 1], wr.at[2, 1], dev(i_far, t))
    b_ys = rcopy(srows(i), srows(i), ws.at[2, 2], wr.at[2, 2], dev(i_far, t))
    b_c = rcopy(block(wall, i, h), block(wall, i, h), ws.at[2, 3], wr.at[2, 3], dev(i_core, t))
    b_cs = rcopy(srows(i), srows(i), ws.at[3, 0], wr.at[3, 0], dev(i_core, t))
    for c in (b_y, b_x, b_ys, b_c, b_cs):
        c.start()
    dispatch(cota, gs)
    g_moved = spread(gs, gr, 0, False, CROSS)
    for c in moved[2 * PR :]:
        c.start()
    g_moved += spread(gs, gr, 0, False, SAME)
    b_y.wait_recv()
    f_x = rcopy(block(wall, i_far, h), block(wall, i_far, h), ws.at[3, 1], wr.at[3, 1], dev(i, t, oh))
    f_x.start()
    f_c = rcopy(block(wall, i_far, h), block(wall, i_far, h), ws.at[3, 2], wr.at[3, 2], dev(i_core, t))
    f_c.start()
    b_ys.wait_recv()
    f_cs = rcopy(srows(i_far), srows(i_far), ws.at[3, 3], wr.at[3, 3], dev(i_core, t))
    f_cs.start()
    b_x.wait_recv()
    f_c2 = rcopy(block(wall, i, oh), block(wall, i, oh), ws.at[4, 0], wr.at[4, 0], dev(i_core, t))
    f_c2.start()

    f_x.wait_recv()
    f_c3 = rcopy(block(wall, i_far, oh), block(wall, i_far, oh), ws.at[4, 1], wr.at[4, 1], dev(i_core, t))
    f_c3.start()
    for c in (b_c, b_cs, f_c, f_cs, f_c2, f_c3):
        c.wait_recv()

    sall_t = jnp.transpose(sall[...].astype(F32))
    gains = ref["gains"]
    gains[...] = sall_t[EXPERTS : EXPERTS + 8, :]
    xn1, qkv, mixed, probs = ref["xn1"], ref["qkv"], ref["mixed"], ref["probs"]
    normed, _ = norm_of(xs[...])
    xn1[...] = (normed * gains[0:1, :]).astype(BF16)

    def project(j, _):
        qkv[j] = mm(xn1[...], wall[j]).astype(BF16)
        return 0

    lax.fori_loop(0, 3, project, 0)
    groups = D // LANES
    scale = HD ** (-0.5)

    def attend(n, _):
        rows = pl.ds(al((n // groups) * RP, 16), RP)
        cols = pl.ds(al(lax.rem(n, groups) * LANES, LANES), LANES)
        q, kk, v = qkv[0, rows, cols], qkv[1, rows, cols], qkv[2, rows, cols]
        low = iota((RP, LANES), 1) < HD
        key = iota((RP, RP), 1)
        outs = []
        for s in range(2):
            sel = low if s == 0 else jnp.logical_not(low)
            score = mm_nt(jnp.where(sel, q, jnp.zeros_like(q)), kk) * scale
            score = jnp.where(key < L, score, -1e30)
            e = jnp.exp(score - jnp.max(score, axis=-1, keepdims=True))
            p = e / jnp.sum(e, axis=-1, keepdims=True)
            p = p.astype(BF16)
            probs[n * 2 + s] = p
            outs.append(mm(p, v))
        mixed[rows, cols] = jnp.where(low, outs[0], outs[1]).astype(BF16)
        return 0

    lax.fori_loop(0, z.own_img * groups, attend, 0)
    resid = ref["resid"]
    resid[...] = xs[...] + mm_nt(mixed[...], wall[3])
    normed, _ = norm_of(resid[...])
    mine_rows = pl.ds(al(h * OWN, 16), OWN)
    other_rows = pl.ds(al(oh * OWN, 16), OWN)
    xn2a[mine_rows, :] = (normed * gains[1:2, :]).astype(BF16)

    xsm, xrm = ref["xsm"], ref["xrm"]
    x_swap = rcopy(xn2a.at[mine_rows], xn2a.at[mine_rows], xsm.at[0], xrm.at[0], dev(i, t, oh))
    x_swap.start()
    x_swap.wait_recv()
    logits = mm(xn2a[...], sall[...])
    logits = jnp.where(lane_all < EXPERTS, logits, -1e30)
    e = jnp.exp(logits - jnp.max(logits, axis=-1, keepdims=True))
    router = ref["router"]
    router[...] = e / jnp.sum(e, axis=-1, keepdims=True)
    gcol = ref["gcol"]
    g0 = jnp.sum(jnp.where(rp[:, 0:1] == lane_all, router[...], 0.0), axis=1, keepdims=True)
    g1 = jnp.sum(jnp.where(rp[:, 1:2] == lane_all, router[...], 0.0), axis=1, keepdims=True)
    gcol[...] = jnp.where(lane_all == 0.0, g0, g1)
    grow = ref["grow"]
    grow[...] = jnp.transpose(gcol[...])
    dispatch(xn2a, xsl, grow)
    gate_moved = spread(gsend, gater, 2, True, CROSS + SAME)
    x_moved = spread(xsl, xr, 1, False, CROSS + SAME)

    hid, igs, gtile = ref["hid"], ref["igs"], ref["gtile"]
    eoa, sia = ref["eoa"], ref["sia"]
    eos, sis, ggs = ref["eos"], ref["sis"], ref["ggs"]
    eor, sir, ggr = ref["eor"], ref["sir"], ref["ggr"]
    rs, rr = ref["rs"], ref["rr"]
    gcols = ref["gcols"]
    ggs[...] = jnp.zeros_like(ggs)
    for c in moved:
        c.wait()
    TR = T * CAP
    eye = iota((LANES, LANES), 0) == iota((LANES, LANES), 1)

    def wait_role(row, kk, dst):
        pltpu.make_async_copy(dst, dst, dr.at[row, kk]).wait()

    def tile(n, _):
        gi = lax.rem(i - n + I, I)
        grp = pl.ds(gi * T, T)
        for dt in range(T):
            src = gi * T + whence(dt)
            wait_role(0, n * T + dt, gr.at[:, src])
            wait_role(1, n * T + dt, xr.at[:, src])
            wait_role(2, n * T + dt, gater.at[src])
        for dt in range(T):
            row = gater[gi * T + dt][0:1, :]
            col = jnp.sum(jnp.where(eye, jnp.broadcast_to(row, (LANES, LANES)), 0.0), axis=1, keepdims=True)
            gcols[dt] = jnp.broadcast_to(col, (LANES, LANES))

        def part(ep, _):
            e, p = ep // PR, lax.rem(ep, PR)
            cols = pl.ds(al(p * FS, FS), FS)
            trow = pl.ds(al(gi * TR, TR), TR)
            x = xr[e, grp].reshape(TR, D)

            @pl.when(p == 0)
            def _():
                g = gr[e, grp].reshape(TR, D)
                gtile[...] = g
                gate = gcols[:, pl.ds(al(e * CAP, CAP), CAP), :].reshape(TR, LANES)[:, 0:1]
                gr[e, grp] = (g.astype(F32) * gate).astype(BF16).reshape(T, CAP, D)
                eoa[...] = jnp.zeros_like(eoa)
                sia[...] = jnp.zeros_like(sia)

            inner = mm(x, vin[e, :, cols])
            erf = lax.erf(inner * (0.5**0.5))
            cdf = 0.5 * (1.0 + erf)
            hidden = (inner * cdf).astype(BF16)
            slope = cdf + inner * (jnp.exp(-0.5 * inner * inner) * 0.3989422804014327)
            hid[e, trow, cols] = hidden
            eoa[...] += mm(hidden, vback[e, cols, :])
            back = mm_nt(gr[e, grp].reshape(TR, D), vback[e, cols, :])
            inner_grad = (back * slope).astype(BF16)
            igs[e, trow, cols] = inner_grad
            sia[...] += mm_nt(inner_grad, vin[e, :, cols])

            @pl.when(p == PR - 1)
            def _():
                eo = eoa[...]
                eos[e, grp] = eo.astype(BF16).reshape(T, CAP, D)
                sis[e, grp] = sia[...].astype(BF16).reshape(T, CAP, D)
                gg = jnp.sum(eo * gtile[...].astype(F32), axis=1, keepdims=True)
                there = iota((CAP, LANES), 1) == iota((CAP, LANES), 0) + (e * CAP).astype(F32)
                for dt in range(T):
                    piece = jnp.broadcast_to(gg[dt * CAP : (dt + 1) * CAP], (CAP, LANES))
                    line = jnp.sum(jnp.where(there, piece, 0.0), axis=0, keepdims=True)
                    ggs[gi * T + dt] = ggs[gi * T + dt] + jnp.broadcast_to(line, (8, LANES))

            return 0

        lax.fori_loop(0, ED * PR, part, 0)
        give_back(n, 2, ggs, ggr, True)
        give_back(n, 0, sis, sir, False)
        return 0

    def give_back(n, row, src, dst, whole):
        gi = lax.rem(i - n + I, I)
        for dt in CROSS + SAME:
            tt = onto(dt)
            kk = n * T + dt
            if whole:
                s, d = src.at[gi * T + tt], dst.at[mine]
            else:
                s, d = src.at[:, gi * T + tt], dst.at[half, pl.ds(e0, ED)]
            if dt == 0:

                @pl.when(n == 0)
                def _():
                    lcopy(s, d, rr.at[row, kk]).start()

                @pl.when(n > 0)
                def _():
                    rcopy(s, d, rs.at[row, kk], rr.at[row, kk], dev(gi, tt)).start()

            else:
                rcopy(s, d, rs.at[row, kk], rr.at[row, kk], dev(gi, tt)).start()

    lax.fori_loop(0, I, tile, 0)

    ing, backg = ref["ing"], ref["backg"]
    vs, vr = ref["vs"], ref["vr"]

    def weight_grad(ep, _):
        e, p = ep // PR, lax.rem(ep, PR)
        cols = pl.ds(al(p * FS, FS), FS)
        vin[e, :, cols] = mm_tn(xr[e].reshape(z.team * CAP, D), igs[e, :, cols]).astype(BF16)
        vback[e, cols, :] = mm_tn(hid[e, :, cols], gr[e].reshape(z.team * CAP, D)).astype(BF16)
        return 0

    def give_grad(ep, _):
        e, p = ep // PR, lax.rem(ep, PR)
        cols = pl.ds(al(p * FS, FS), FS)
        for di in range(I):
            ii = lax.rem(i + di, I)
            part_in = vin.at[e, pl.ds(al(ii * DQ, DQ), DQ), cols]
            part_back = vback.at[e, cols, pl.ds(al(ii * DQ, DQ), DQ)]
            to_in, to_back = ing.at[e0 + e], backg.at[e0 + e]
            if di == 0:

                @pl.when(p == pos)
                def _():
                    lcopy(part_in, to_in, vr.at[0, e0 + e]).start()
                    lcopy(part_back, to_back, vr.at[1, e0 + e]).start()

                @pl.when(p != pos)
                def _():
                    rcopy(part_in, to_in, vs.at[0, ep * I], vr.at[0, e0 + e], dev(ii, half * PR + p)).start()
                    rcopy(part_back, to_back, vs.at[1, ep * I], vr.at[1, e0 + e], dev(ii, half * PR + p)).start()

            else:
                to = dev(ii, half * PR + p)
                rcopy(part_in, to_in, vs.at[0, ep * I + di], vr.at[0, e0 + e], to).start()
                rcopy(part_back, to_back, vs.at[1, ep * I + di], vr.at[1, e0 + e], to).start()
        return 0


    early = ED * PR * EARLY // 4
    lax.fori_loop(0, early, weight_grad, 0)
    lax.fori_loop(0, early, give_grad, 0)
    lax.fori_loop(early, ED * PR, weight_grad, 0)

    def back_gone(row, buf, n):
        for dt in range(T):

            def one():
                pltpu.make_async_copy(buf, buf, rs.at[row, n * T + dt]).wait()

            if dt == 0:
                pl.when(n > 0)(one)
            else:
                one()

    ggx = ref["ggx"]
    cacc = ref["cacc"]

    def from_of(n, dt):
        return lax.rem(i + n, I), whence(dt)

    def wait_home(row, view):
        def one(n, _):
            for dt in range(T):
                fi, ft = from_of(n, dt)
                d = view(fi, ft)
                pltpu.make_async_copy(d, d, rr.at[row, n * T + dt]).wait()
            return 0

        lax.fori_loop(0, I, one, 0)

    def slot_view(buf):
        return lambda fi, ft: buf.at[ft // PR, pl.ds((fi * PR + lax.rem(ft, PR)) * ED, ED)]

    wait_home(2, lambda fi, ft: ggr.at[fi * T + ft])
    gg_swap = rcopy(ggr, ggx, xsm.at[1], xrm.at[1], dev(i, t, oh))
    gg_swap.start()
    wait_home(0, slot_view(sir))

    def give_eo(n, _):
        give_back(n, 1, eos, eor, False)
        return 0

    lax.fori_loop(0, I, give_eo, 0)


    CH = 256

    def combine(rows, src, weighted):
        c0, c1 = idc[rows, 0:1], idc[rows, 1:2]
        w0 = gcol[rows, 0:1] if weighted else 1.0
        w1 = gcol[rows, 1:2] if weighted else 1.0
        cacc[...] = jnp.zeros_like(cacc)

        def one(c, _):
            lane = iota((OWN, CH), 1) + (c * CH + h * z.slots).astype(F32)
            w = jnp.where(c0 == lane, w0, 0.0) + jnp.where(c1 == lane, w1, 0.0)
            w = w.astype(BF16)
            for a in range(A):
                cacc[...] += mm(w, src[a, pl.ds(c * (CH // CAP), CH // CAP)].reshape(CH, D))
            return 0

        lax.fori_loop(0, z.slots // CH, one, 0)

    dbs, dbr = ref["dbs"], ref["dbr"]
    combine(other_rows, sir, False)
    dbs[...] = cacc[...].astype(BF16)
    db_swap = rcopy(dbs, dbr, xsm.at[2], xrm.at[2], dev(i, t, oh))
    db_swap.start()
    combine(mine_rows, sir, False)

    lane_own = iota((OWN, LANES), 1)
    m0, m1 = rp[mine_rows, 0:1], rp[mine_rows, 1:2]
    gg_swap.wait_recv()
    ggacc = ref["ggacc"]
    ggacc[...] = jnp.zeros_like(ggacc)

    def gate_back(q, _):
        fi, pp = q // PR, lax.rem(q, PR)
        k0, k1 = idc[mine_rows, 0:1], idc[mine_rows, 1:2]
        for buf, hh in ((ggr, h), (ggx, oh)):
            line = buf[fi * T + pp][0:1, :]
            for a in range(1, A):
                line = line + buf[fi * T + a * PR + pp][0:1, :]
            lane = lane_own + (q * z.lw + hh * z.slots).astype(F32)
            keep = lane_own < z.lw
            ggacc[0] += jnp.where(jnp.logical_and(keep, k0 == lane), line, 0.0)
            ggacc[1] += jnp.where(jnp.logical_and(keep, k1 == lane), line, 0.0)
        return 0

    lax.fori_loop(0, z.home // ED, gate_back, 0)
    gg0 = jnp.sum(ggacc[0], axis=1, keepdims=True)
    gg1 = jnp.sum(ggacc[1], axis=1, keepdims=True)
    mrouter = router[mine_rows, :]
    pgrad = jnp.where(m0 == lane_own, gg0, 0.0) + jnp.where(m1 == lane_own, gg1, 0.0)
    lgrad = (mrouter * (pgrad - jnp.sum(pgrad * mrouter, axis=1, keepdims=True))).astype(BF16)
    xn2 = xn2a[mine_rows, :]
    small = ref["small"]
    small[...] = jnp.where(iota((D, LANES), 1) < EXPERTS, mm_tn(xn2, lgrad), 0.0)
    through = mm_nt(lgrad, sall[...])
    db_swap.wait_recv()
    xgrad = cacc[...] + dbr[...].astype(F32) + through
    normed, spread_two = norm_of(resid[...])
    nrows = ref["nrows"]
    nrows[...] = jnp.zeros_like(nrows)
    nrows[EXPERTS + 1 : EXPERTS + 2, :] = jnp.sum(xgrad * normed, axis=0, keepdims=True)
    rgrad = ref["rgrad"]
    rgrad[...] = cota[mine_rows, :].astype(F32) + norm_back(xgrad * gains[1:2, :], normed, spread_two)

    agrad = rgrad[...].astype(BF16)

    def gw(j, row, count):
        return (0, pl.ds(al((j // 2) * D + row, LANES), count), pl.ds(al(lax.rem(j, 2) * D, LANES), D))

    hid[gw(jnp.int32(3), 0, D)] = mm_tn(agrad, mixed[...]).astype(BF16)
    mg = ref["mg"]
    mg[...] = mm(agrad, wall[3]).astype(BF16)
    pg = ref["pg"]

    def attend_back(n, _):
        rows = pl.ds(al((n // groups) * RP, 16), RP)
        cols = pl.ds(al(lax.rem(n, groups) * LANES, LANES), LANES)
        q, kk, v = qkv[0, rows, cols], qkv[1, rows, cols], qkv[2, rows, cols]
        m = mg[rows, cols]
        low = iota((RP, LANES), 1) < HD
        dq, dk, dv = [], [], []
        for s in range(2):
            sel = low if s == 0 else jnp.logical_not(low)
            low_p = probs[n * 2 + s]
            p = low_p.astype(F32)
            dp = mm_nt(jnp.where(sel, m, jnp.zeros_like(m)), v)
            dv.append(mm_tn(low_p, m))
            sg = (p * (dp - jnp.sum(dp * p, axis=-1, keepdims=True))).astype(BF16)
            dq.append(mm(sg, kk))
            dk.append(mm_tn(sg, q))
        pg[0, rows, cols] = (jnp.where(low, dq[0], dq[1]) * scale).astype(BF16)
        pg[1, rows, cols] = (jnp.where(low, dk[0], dk[1]) * scale).astype(BF16)
        pg[2, rows, cols] = jnp.where(low, dv[0], dv[1]).astype(BF16)
        return 0

    lax.fori_loop(0, z.own_img * groups, attend_back, 0)
    cacc[...] = jnp.zeros_like(cacc)

    def project_back(j, _):
        hid[gw(j, 0, D)] = mm_tn(xn1[...], pg[j]).astype(BF16)
        cacc[...] += mm_nt(pg[j], wall[j])
        return 0

    lax.fori_loop(0, 3, project_back, 0)

    s1r, s2s, s2r, s3s, s3r, s4s, s4r = (ref[n] for n in ("s1r", "s2s", "s2r", "s3s", "s3r", "s4s", "s4r"))
    u1s, u1r, u3s, u3r, u4s, u4r, u5s, u5r = (ref[n] for n in ("u1s", "u1r", "u3s", "u3r", "u4s", "u4r", "u5s", "u5r"))
    qs, qr = ref["qs"], ref["qr"]

    def quarter(ii):
        return pl.ds(al(ii * DQ, DQ), DQ)

    sw1 = []
    for b, ii in enumerate((i_core, i_diag)):
        for jr in range(2):
            src = hid.at[0, pl.ds(al(jr * D + ii * DQ, LANES), DQ), pl.ds(0, 2 * D)]
            sw1.append(rcopy(src, s1r.at[jr, b], qs.at[13 + 2 * b + jr], qr.at[13 + 2 * b + jr], dev(i_core, t)))
    for c in sw1:
        c.start()

    normed, spread_one = norm_of(xs[...])
    nrows[EXPERTS : EXPERTS + 1, :] = jnp.sum(cacc[...] * normed, axis=0, keepdims=True)
    tgrad = rgrad[...] + norm_back(cacc[...] * gains[0:1, :], normed, spread_one)
    tgs, tg_p, out_p = ref["tgs"], ref["tg_p"], ref["out_p"]
    tgs[...] = tgrad.astype(BF16)
    small[...] = small[...] + jnp.transpose(nrows[...])
    for b, ii in enumerate((i_core, i_diag)):
        u1s[b] = small[quarter(ii), :]
    sv1 = rcopy(u1s, u1r, qs.at[1], qr.at[1], dev(i_core, t))
    sv1.start()
    for c in sw1:
        c.wait_recv()
    sv1.wait_recv()
    accu, acc2 = ref["accu"], ref["acc2"]
    for b, ii in enumerate((i, i_far)):
        for j in range(4):
            for hh, keep in ((oh, False), (h, True)):
                cols = pl.ds(al((j % 2) * D + hh * EC, LANES), EC)
                here = hid[0, pl.ds(al((j // 2) * D + ii * DQ, LANES), DQ), cols].astype(F32)
                here = here + s1r[j // 2, b, :, cols].astype(F32)
                if keep:
                    acc2[j, b] = here
                else:
                    s2s[j, b] = here.astype(BF16)
        accu[b] = small[quarter(ii), :] + u1r[b]
    sw2 = rcopy(s2s, s2r, qs.at[2], qr.at[2], dev(i, t, oh))
    sw2.start()
    t_swap = rcopy(tgs, tg_p.at[mine_rows], xsm.at[3], xrm.at[3], dev(i, t, oh))
    t_own = lcopy(tgs, tg_p.at[mine_rows], ls.at[2])
    t_swap.start()
    t_own.start()
    u3s[...] = accu[1]
    sv3 = rcopy(u3s, u3r, qs.at[3], qr.at[3], dev(i_far, t))
    sv3.start()

    sw2.wait_recv()
    acc2[...] = acc2[...] + s2r[...].astype(F32)
    s3s[...] = acc2[:, 1].astype(BF16)
    sw3 = rcopy(s3s, s3r, qs.at[4], qr.at[4], dev(i_far, t))
    sw3.start()
    sw3.wait_recv()
    sv3.wait_recv()
    accu[0] = accu[0] + u3r[...]
    u4s[...] = accu[0]
    acc2[:, 0] = acc2[:, 0] + s3r[...].astype(F32)
    s4s[...] = acc2[:, 0].astype(BF16)
    last = []
    for dt in range(1, T):
        tt = lax.rem(t + dt, T)
        rows = pl.ds(al(tt * WR, WR), WR)
        last.append(rcopy(s4s.at[:, rows, :], s4r.at[dt], qs.at[4 + 2 * dt], qr.at[4 + 2 * dt], dev(i, tt)))
        last.append(rcopy(u4s.at[rows, :], u4r.at[dt], qs.at[5 + 2 * dt], qr.at[5 + 2 * dt], dev(i, tt)))
    for c in last:
        c.start()
    lax.fori_loop(early, ED * PR, give_grad, 0)

    mos, mor, outs = ref["mos"], ref["mor"], ref["outs"]
    wait_home(1, slot_view(eor))
    combine(other_rows, eor, True)
    mos[...] = cacc[...].astype(BF16)
    pieces = [pl.ds(m * RP, RP) for m in range(z.own_img)]
    m_swap = []
    for m, rows in enumerate(pieces):
        m_swap.append(rcopy(mos.at[rows], mor.at[rows], xsm.at[4 + 2 * m], xrm.at[4 + 2 * m], dev(i, t, oh)))
        m_swap[m].start()
    combine(mine_rows, eor, True)
    o_swap = []
    for m, rows in enumerate(pieces):
        m_swap[m].wait_recv()
        outs[rows, :] = (resid[rows, :] + cacc[rows, :] + mor[rows, :].astype(F32)).astype(BF16)
        there = out_p.at[pl.ds(al(h * OWN + m * RP, 16), RP)]
        o_swap.append(rcopy(outs.at[rows], there, xsm.at[5 + 2 * m], xrm.at[5 + 2 * m], dev(i, t, oh)))
        o_swap[m].start()
    o_own = lcopy(outs, out_p.at[mine_rows], ls.at[3])
    o_own.start()
    for c in last:
        c.wait_recv()
    wfin, sfin = ref["wfin"], ref["sfin"]
    my_rows = pl.ds(al(t * WR, WR), WR)
    total = acc2[:, 0, my_rows, :]
    part = accu[0, my_rows, :]
    for dt in range(1, T):
        total = total + s4r[dt].astype(F32)
        part = part + u4r[dt]
    wfs, sfs = ref["wfs"], ref["sfs"]
    wfs[...] = total
    w_own = lcopy(wfs, wfin, ls.at[4])
    w_own.start()
    u5s[...] = part
    sv5 = rcopy(u5s, u5r, qs.at[12], qr.at[12], dev(i, t, oh))
    sv5.start()
    t_swap.wait_recv()
    for c in o_swap:
        c.wait_recv()
    t_own.wait()
    o_own.wait()
    sv5.wait_recv()
    sfs[...] = u5s[...] + u5r[...]
    s_own = lcopy(sfs, sfin, ls.at[5])
    s_own.start()

    def grads_in(e, _):
        pltpu.make_async_copy(ing.at[e], ing.at[e], vr.at[0, e]).wait()
        pltpu.make_async_copy(backg.at[e], backg.at[e], vr.at[1, e]).wait()
        return 0

    lax.fori_loop(0, z.home, grads_in, 0)

    def grads_out(ep, _):
        p = lax.rem(ep, PR)
        for di in range(I):
            a_in = vin.at[0, pl.ds(0, DQ), pl.ds(0, FS)]
            a_back = vback.at[0, pl.ds(0, FS), pl.ds(0, DQ)]
            if di == 0:

                @pl.when(p != pos)
                def _():
                    pltpu.make_async_copy(a_in, a_in, vs.at[0, ep * I]).wait()
                    pltpu.make_async_copy(a_back, a_back, vs.at[1, ep * I]).wait()

            else:
                pltpu.make_async_copy(a_in, a_in, vs.at[0, ep * I + di]).wait()
                pltpu.make_async_copy(a_back, a_back, vs.at[1, ep * I + di]).wait()
        return 0

    lax.fori_loop(0, ED * PR, grads_out, 0)

    def back_out(n, _):
        back_gone(0, sis.at[:, 0], n)
        back_gone(1, eos.at[:, 0], n)
        back_gone(2, ggs.at[0], n)
        return 0

    lax.fori_loop(0, I, back_out, 0)
    w_own.wait()
    s_own.wait()
    for c in g_moved + x_moved + gate_moved:
        if c.is_remote:
            c.wait_send()
    for c in first + [b_x, b_y, b_ys, b_c, b_cs, f_x, f_c, f_cs, f_c2, f_c3]:
        c.wait_send()
    for c in (x_swap, gg_swap, db_swap, t_swap, *m_swap, *o_swap, *sw1, sv1, sw2, sv3, sw3, sv5, *last):
        c.wait_send()


def call(z, tok, cot, rt, wqkv, wout, table, one, two, win, wback):
    T, I, PR, A, ED, D = z.tensor, z.team_i, z.pair, z.halves, z.own_e, z.width
    OWN, ROWS, EC, DQ, WR = z.own, z.rows, z.ecols, z.dq, z.wrow
    team = z.team
    V, S = pltpu.VMEM, pltpu.SemaphoreType.DMA
    ins = ["tok", "cot", "rt", "wqkv", "wout", "table", "one", "two", "win", "wback"]
    outs = {
        "out_p": jax.ShapeDtypeStruct((z.all, D), BF16),
        "tg_p": jax.ShapeDtypeStruct((z.all, D), BF16),
        "wfin": jax.ShapeDtypeStruct((4, WR, EC), F32),
        "sfin": jax.ShapeDtypeStruct((WR, LANES), F32),
        "ing": jax.ShapeDtypeStruct(win.shape, BF16),
        "backg": jax.ShapeDtypeStruct(wback.shape, BF16),
    }
    heads_own = z.own_img * z.nh
    wide = -(-z.length // LANES) * LANES
    scratch = {
        "spack": V((WR, LANES), BF16),
        "wfs": V((4, WR, EC), F32),
        "sfs": V((WR, LANES), F32),
        "tokv": V(tok.shape, BF16),
        "cotv": V(cot.shape, BF16),
        "rtt": V((LANES, wide), F32),
        "ls": S((6,)),
        "wall": V((4, D, D), BF16), "sall": V((D, LANES), BF16), "gains": V((8, D), F32),
        "xn2a": V((ROWS, D), BF16), "cota": V((ROWS, D), BF16), "rp": V((ROWS, LANES), F32),
        "xs": V((OWN, D), F32), "both": V((ROWS, LANES), BF16), "idc": V((ROWS, LANES), F32),
        "idr": V((LANES, ROWS), F32), "grow": V((LANES, ROWS), F32), "gs": V((z.home, CAP, D), BF16), "xsl": V((z.home, CAP, D), BF16),
        "vin": V((ED, D, z.ff), BF16), "vback": V((ED, z.ff, D), BF16),
        "xr": V((ED, team, CAP, D), BF16), "gr": V((ED, team, CAP, D), BF16), "gater": V((team, 8, LANES), F32),
        "xn1": V((OWN, D), BF16), "qkv": V((3, OWN, D), BF16), "mixed": V((OWN, D), BF16),
        "probs": V((heads_own, z.pad, z.pad), BF16), "resid": V((OWN, D), F32), "router": V((ROWS, LANES), F32),
        "gcol": V((ROWS, LANES), F32), "gsend": V((z.home // ED, 8, LANES), F32),
        "hid": V((ED, team * CAP, z.ff), BF16), "igs": V((ED, team * CAP, z.ff), BF16),
        "eoa": V((T * CAP, D), F32), "sia": V((T * CAP, D), F32),
        "eos": V((ED, team, CAP, D), BF16), "sis": V((ED, team, CAP, D), BF16), "ggs": V((team, 8, LANES), F32),
        "eor": V((A, z.home, CAP, D), BF16), "sir": V((A, z.home, CAP, D), BF16), "ggr": V((team, 8, LANES), F32),
        "gcols": V((T, LANES, LANES), F32), "gtile": V((T * CAP, D), BF16),
        "ggx": V((team, 8, LANES), F32), "cacc": V((OWN, D), F32), "dbs": V((OWN, D), BF16), "dbr": V((OWN, D), BF16),
        "ggacc": V((2, OWN, LANES), F32), "small": V((D, LANES), F32), "nrows": V((LANES, D), F32),
        "rgrad": V((OWN, D), F32), "mg": V((OWN, D), BF16), "pg": V((3, OWN, D), BF16),
        "s1r": V((2, 2, DQ, 2 * D), BF16),
        "s2s": V((4, 2, DQ, EC), BF16), "s2r": V((4, 2, DQ, EC), BF16),
        "s3s": V((4, DQ, EC), BF16), "s3r": V((4, DQ, EC), BF16),
        "s4s": V((4, DQ, EC), BF16), "s4r": V((T, 4, WR, EC), BF16),
        "u1s": V((2, DQ, LANES), F32), "u1r": V((2, DQ, LANES), F32),
        "u3s": V((DQ, LANES), F32), "u3r": V((DQ, LANES), F32),
        "u4s": V((DQ, LANES), F32), "u4r": V((T, WR, LANES), F32),
        "u5s": V((WR, LANES), F32), "u5r": V((WR, LANES), F32),
        "accu": V((2, DQ, LANES), F32), "acc2": V((4, 2, DQ, EC), F32),
        "tgs": V((OWN, D), BF16),  "mos": V((OWN, D), BF16), "mor": V((OWN, D), BF16),
        "outs": V((OWN, D), BF16),
        "ws": S((6, 4)), "wr": S((6, 4)), "wl": S((3,)), "es": S((2, I * PR)), "er": S((2, I * PR)),
        "ds": S((3, team)), "dr": S((3, team)), "rs": S((3, team)), "rr": S((3, team)),
        "vs": S((2, ED * PR * I)), "vr": S((2, z.home)), "xsm": S((4 + 2 * z.own_img,)), "xrm": S((4 + 2 * z.own_img,)), "qs": S((20,)), "qr": S((20,)),
    }
    vmem = pl.BlockSpec(memory_space=pltpu.VMEM)
    anyw = pl.BlockSpec(memory_space=pl.ANY)
    names = ins + list(outs) + list(scratch)
    return pl.pallas_call(
        functools.partial(kernel, z, names),
        out_shape=tuple(outs.values()),
        in_specs=[anyw] * 2 + [vmem] * 6 + [anyw] * 2,
        out_specs=(anyw,) * 6,
        scratch_shapes=list(scratch.values()),
        compiler_params=pltpu.CompilerParams(collective_id=0, has_side_effects=True, vmem_limit_bytes=64 * 1024 * 1024 - 65536),
        name="block",
    )(tok, cot, rt, wqkv, wout, table, one, two, win, wback)


def finish_kernel(z, parts, out_p, tg_p, wfin, sfin, ing, backg, out, tgrad, qkv, proj, table, one, two, gin, gback, *work):
    half_in, half_back, full_in, full_back, outl, tgl, outv, tgv, mix, got, put = work
    step = z.home // parts
    cuts = [pl.ds(p * step, step) for p in range(parts)]
    tasks = [(ing, half_in, full_in, gin), (backg, half_back, full_back, gback)]
    reads, writes = [], []
    for p, cut in enumerate(cuts):
        for k, (src, low, full, dst) in enumerate(tasks):
            reads.append(pltpu.make_async_copy(src.at[cut], low.at[cut], got.at[k, p]))
            writes.append(pltpu.make_async_copy(full.at[cut], dst.at[cut], put.at[k, p]))
    rows = [pltpu.make_async_copy(out_p, outl, got.at[0, parts]), pltpu.make_async_copy(tg_p, tgl, got.at[1, parts])]
    for c in reads[:2] + rows + reads[2:]:
        c.start()

    def convert(p):
        for k, (_, low, full, _) in enumerate(tasks):
            reads[2 * p + k].wait()
            full[cuts[p]] = low[cuts[p]].astype(F32)
            writes[2 * p + k].start()

    last = [
        pltpu.make_async_copy(outv, out, put.at[0, parts]),
        pltpu.make_async_copy(tgv, tgrad, put.at[1, parts]),
    ]
    convert(0)
    rows[0].wait()
    for m in range(z.images):
        mix[:, m, :] = outl[pl.ds(m * z.pad, z.length), :].astype(F32)
    outv[...] = mix[...].astype(BF16)
    last[0].start()
    convert(1)
    rows[1].wait()
    for m in range(z.images):
        tgv[:, m, :] = tgl[pl.ds(m * z.pad, z.length), :].astype(F32)
    last[1].start()
    for p in range(2, parts):
        convert(p)
    qkv[...] = wfin[0:3]
    proj[...] = wfin[3]
    table[...] = sfin[:, 0:EXPERTS]
    n = sfin.shape[0]
    eye = iota((n, n), 0) == iota((n, n), 1)
    for k, target in enumerate((one, two)):
        col = sfin[:, EXPERTS + k : EXPERTS + k + 1]
        target[...] = jnp.sum(jnp.where(eye, col, 0.0), axis=0, keepdims=True)
    for c in writes + last:
        c.wait()


def finish(z, out_p, tg_p, wfin, sfin, ing, backg):
    parts = 4
    V, S = pltpu.VMEM, pltpu.SemaphoreType.DMA
    whole = pl.BlockSpec(memory_space=pltpu.VMEM)
    anyw = pl.BlockSpec(memory_space=pl.ANY)
    mixed = (z.length, z.images, z.width)
    n = sfin.shape[0]
    outs = (
        jax.ShapeDtypeStruct(mixed, BF16),
        jax.ShapeDtypeStruct(mixed, F32),
        jax.ShapeDtypeStruct((3, *wfin.shape[1:]), F32),
        jax.ShapeDtypeStruct(wfin.shape[1:], F32),
        jax.ShapeDtypeStruct((n, EXPERTS), F32),
        jax.ShapeDtypeStruct((1, n), F32),
        jax.ShapeDtypeStruct((1, n), F32),
        jax.ShapeDtypeStruct(ing.shape, F32),
        jax.ShapeDtypeStruct(backg.shape, F32),
    )
    scratch = [V(ing.shape, BF16), V(backg.shape, BF16), V(ing.shape, F32), V(backg.shape, F32)]
    scratch += [V(out_p.shape, BF16), V(tg_p.shape, BF16), V(mixed, BF16), V(mixed, F32), V(mixed, F32)]
    scratch += [S((2, parts + 1)), S((2, parts + 1))]
    return pl.pallas_call(
        functools.partial(finish_kernel, z, parts),
        out_shape=outs,
        in_specs=[anyw] * 2 + [whole] * 2 + [anyw] * 2,
        out_specs=(anyw,) * 2 + (whole,) * 5 + (anyw,) * 2,
        scratch_shapes=scratch,
        compiler_params=pltpu.CompilerParams(vmem_limit_bytes=64 * 1024 * 1024 - 65536),
        name="finish",
    )(out_p, tg_p, wfin, sfin, ing, backg)


def solution(mesh):
    def local(tokens, cotangent, w_qkv, w_out, w_router, norm_one, norm_two, w_in, w_back, routes):
        images, length, width = tokens.shape
        z = Sizes(mesh.shape, images, length, width, w_in.shape[0], w_in.shape[2])
        R = z.reps
        wqkv, wout, table = w_qkv, jnp.transpose(w_out), w_router
        one, two = norm_one, norm_two
        sets = None
        if R > 1:
            sets = [[a * R + b for b in range(R)] for a in range(z.team_i)]
            w_in = lax.all_gather(w_in, "fsdp", axis=1, tiled=True, axis_index_groups=sets)
            w_back = lax.all_gather(w_back, "fsdp", axis=2, tiled=True, axis_index_groups=sets)
            place = lax.axis_index("tensor") * z.wrow

            def quarter(w, axis):
                w = lax.all_gather(w, "tensor", axis=axis, tiled=True)
                w = lax.all_gather(w, "fsdp", axis=axis, tiled=True, axis_index_groups=sets)
                return lax.dynamic_slice_in_dim(w, place, z.wrow, axis)

            wqkv, wout, table = quarter(wqkv, 1), quarter(wout, 0), quarter(table, 0)
            one, two = quarter(one, 0), quarter(two, 0)
        tok, cot = jnp.transpose(tokens, (1, 0, 2)), jnp.transpose(cotangent, (1, 0, 2))
        rt = jnp.transpose(routes, (0, 2, 1))
        out_p, tg_p, wfin, sfin, ing, backg = call(z, tok, cot, rt, wqkv, wout, table, one[None], two[None], w_in, w_back)
        if R > 1:
            ing = lax.psum_scatter(ing, "fsdp", scatter_dimension=1, tiled=True, axis_index_groups=sets)
            backg = lax.psum_scatter(backg, "fsdp", scatter_dimension=2, tiled=True, axis_index_groups=sets)

            def shard(w, axis):
                w = lax.all_gather(w, "tensor", axis=axis, tiled=True)
                w = lax.psum_scatter(w, "fsdp", scatter_dimension=axis, tiled=True, axis_index_groups=sets)
                rows = w.shape[axis] // z.tensor
                return lax.dynamic_slice_in_dim(w, lax.axis_index("tensor") * rows, rows, axis)

            wfin, sfin = shard(wfin, 1), shard(sfin, 0)
        out, tgrad, qkv, proj, table, one, two, gin, gback = finish(z, out_p, tg_p, wfin, sfin, ing, backg)
        return (
            jnp.transpose(out, (1, 0, 2)),
            jnp.transpose(tgrad, (1, 0, 2)),
            qkv,
            jnp.transpose(proj),
            table,
            one.reshape(-1),
            two.reshape(-1),
            gin,
            gback,
        )

    rows = P(("fsdp", "tensor"), None, None)
    qkv = P(None, ("fsdp", "tensor"), "heads")
    proj = P("heads", ("fsdp", "tensor"))
    table = P(("fsdp", "tensor"), None)
    gain = P(("fsdp", "tensor"))
    first = P("heads", "fsdp", "tensor")
    second = P("heads", "tensor", "fsdp")
    return jax.shard_map(
        local,
        mesh=mesh,
        in_specs=(rows, rows, qkv, proj, table, gain, gain, first, second, rows),
        out_specs=(rows, rows, qkv, proj, table, gain, gain, first, second),
        check_vma=False,
    )
```
